32 devices in a mesh: dp: 8 (over z, x), mp: 4 (over y, core).
Axes of the slice: x: 2, y: 2, z: 4, core: 2. Of those that a mesh axis runs over, the one named last changes fastest.
Arguments:
- text_in: bfloat16 [7680, 768], P(('dp', 'mp')), may hold values from -6 to 6
- caption_ids: int32 [480, 16], P('dp'), may hold values from 0 to 31999, as said below
- pairing: int32 [480], replicated, may hold values from 0 to 479, each once
- image_low: bfloat16 [19200, 768], P(('dp', 'mp')), may hold values from -6 to 6
- image_high: bfloat16 [13920, 768], P(('dp', 'mp')), may hold values from -6 to 6
- img_gains: float32 [2, 768], replicated, may hold values from 0.5 to 1.5
- img_qkv: bfloat16 [3, 768, 768], P(None, None, 'mp'), may hold values from -0.21875 to 0.21875
- img_out: bfloat16 [768, 768], P('mp'), may hold values from -0.625 to 0.625
- img_fc1: bfloat16 [768, 3072], P(None, 'mp'), may hold values from -0.21875 to 0.21875
- img_fc2: bfloat16 [3072, 768], P('mp'), may hold values from -0.109375 to 0.109375
- txt_qkv: bfloat16 [3, 768, 768], P(None, None, 'mp'), may hold values from -0.21875 to 0.21875
- txt_qv_bias: float32 [2, 768], P(None, 'mp'), may hold values from -3 to 3
- txt_out: bfloat16 [768, 768], P('mp'), may hold values from -0.4375 to 0.4375
- txt_fc1: bfloat16 [768, 3072], P(None, 'mp'), may hold values from -0.21875 to 0.21875
- txt_fc1_bias: float32 [3072], P('mp'), may hold values from -3 to 3
- txt_fc2: bfloat16 [3072, 768], P('mp'), may hold values from -0.109375 to 0.109375
- txt_gains: float32 [2, 768], replicated, may hold values from 0.5 to 1.5
- txt_shifts: float32 [2, 768], replicated, may hold values from -2 to 2
- txt_biases: float32 [2, 768], replicated, may hold values from -2 to 2
Outputs:
- loss: float32 [], replicated
- grad_text_in: float32 [7680, 768], P(('dp', 'mp'))
- grad_qkv: float32 [3, 768, 768], P(None, None, 'mp')
- grad_qv_bias: float32 [2, 768], P(None, 'mp')
- grad_out: float32 [768, 768], P('mp')
- grad_fc1: float32 [768, 3072], P(None, 'mp')
- grad_fc1_bias: float32 [3072], P('mp')
- grad_fc2: float32 [3072, 768], P('mp')
- grad_gains: float32 [2, 768], replicated
- grad_shifts: float32 [2, 768], replicated
- grad_biases: float32 [2, 768], replicated
The draws below stay inside these ranges and needn't reach their ends.
Inputs may be any that keep to these rules, and one draw needn't show every extreme that they name: `caption_ids`: in each caption the nonzero ids come first and the zeros after; each caption has 4 to 16 nonzero ids. Image i is paired with caption pairing[i]; each caption is paired once.
All inputs are finite; a program needn't handle non-finite values.
Results may differ from the reference program's by a relative error of at most 0.017.
Values may be sent and summed in bfloat16 or wider, within the bound.
A program may use at most 192 MiB of HBM per device.

```python
import jax
import jax.numpy as jnp
from jax import lax

D = 768
HEADS = 12
HEAD = 64
FF = 3072
L = 16
P_LOW = 50
P_HIGH = 145
HIGH_DEV = 3
LOW_DEV = 12
PAIRS_DEV = 15
PAIRS = 480
IMG_LOW = 384
IMG_HIGH = 96
N_DP = 8
N_MP = 4


def draw_caption_ids(key, part):
    first, second = jax.random.split(key)
    rows = jnp.arange(PAIRS)
    lengths = jax.random.randint(first, (PAIRS,), L // 4, L + 1)
    lengths = jnp.where(rows % 8 == 0, L, jnp.where(rows % 8 == 1, L // 4, lengths))
    tokens = jax.random.randint(second, (PAIRS, L), 1, 32000)
    places = jnp.arange(L)[None, :]
    return jnp.where(places < lengths[:, None], tokens, 0).astype(jnp.int32)


def block_levels(rng, dims, shards, least, largest):
    loudness, own = 1.0, jax.random.fold_in(rng, 6)
    for position, shards_of in shards:
        steps = jnp.exp(jax.random.uniform(jax.random.fold_in(own, position), (shards_of,), jnp.float32, least / len(shards), largest / len(shards)))
        loudness = loudness * jnp.repeat(steps, dims[position] // shards_of).reshape([-1 if axis == position else 1 for axis in range(len(dims))])
    return loudness


def centred(rng, dims, width, bound, shards=(), held_as=jnp.bfloat16):
    level = block_levels(rng, dims, shards, -0.22, 0.18) if shards else 1.0
    array = jax.random.normal(rng, dims, jnp.float32) * width * level
    return jnp.minimum(jnp.maximum(array, -bound), bound).astype(held_as)


def setup_inputs(seed: int = 0) -> dict:
    key_list = jax.random.split(jax.random.key(seed), 20)
    text_in = centred(key_list[0], (PAIRS * L, D), 1.0, 6.0, ((0, 32),))
    caption_ids = draw_caption_ids(jax.random.fold_in(key_list[19], 71), 0)
    pairing = jax.random.permutation(key_list[2], PAIRS).astype(jnp.int32)
    image_low = centred(key_list[3], (IMG_LOW * P_LOW, D), 1.0, 6.0, ((0, 32),))
    image_high = centred(key_list[4], (IMG_HIGH * P_HIGH, D), 1.0, 6.0, ((0, 32),))
    img_gains = jnp.clip(1.0 + 0.1 * jax.random.normal(key_list[5], (2, D), jnp.float32), 0.5, 1.5)
    img_qkv = centred(key_list[6], (3, D, D), D ** -0.5, 0.21875, ((2, 4),))
    img_out = centred(key_list[7], (D, D), (D // 8) ** -0.5, 0.625, ((0, 4),))
    img_fc1 = centred(key_list[8], (D, FF), D ** -0.5, 0.21875, ((1, 4),))
    img_fc2 = centred(key_list[9], (FF, D), FF ** -0.5, 0.109375, ((0, 4),))
    txt_qkv = centred(key_list[10], (3, D, D), D ** -0.5, 0.21875, ((2, 4),))
    txt_qv_bias = centred(key_list[11], (2, D), 0.5, 3.0, ((1, 4),), jnp.float32)
    txt_out = centred(key_list[12], (D, D), (D // 4) ** -0.5, 0.4375, ((0, 4),))
    txt_fc1 = centred(key_list[13], (D, FF), D ** -0.5, 0.21875, ((1, 4),))
    txt_fc1_bias = centred(key_list[14], (FF,), 0.5, 3.0, ((0, 4),), jnp.float32)
    txt_fc2 = centred(key_list[15], (FF, D), FF ** -0.5, 0.109375, ((0, 4),))
    txt_gains = jnp.clip(1.0 + 0.1 * jax.random.normal(key_list[16], (2, D), jnp.float32), 0.5, 1.5)
    txt_shifts = centred(key_list[17], (2, D), 0.3, 2.0, (), jnp.float32)
    txt_biases = centred(key_list[18], (2, D), 0.3, 2.0, (), jnp.float32)
    return {"text_in": text_in, "caption_ids": caption_ids, "pairing": pairing, "image_low": image_low, "image_high": image_high, "img_gains": img_gains, "img_qkv": img_qkv, "img_out": img_out, "img_fc1": img_fc1, "img_fc2": img_fc2, "txt_qkv": txt_qkv, "txt_qv_bias": txt_qv_bias, "txt_out": txt_out, "txt_fc1": txt_fc1, "txt_fc1_bias": txt_fc1_bias, "txt_fc2": txt_fc2, "txt_gains": txt_gains, "txt_shifts": txt_shifts, "txt_biases": txt_biases}


EPS = 1e-06
SCALE = 40.0
LOSS_SCALE = 16.0
MASKED = -1e+30

@jax.custom_vjp
def low(v):
    return lax.optimization_barrier(v.astype(jnp.bfloat16)).astype(jnp.float32)

@jax.custom_vjp
def low_back(v):
    return v

def low_keep(v):
    return (low(v), None)

def low_pass(kept, grad):
    return (grad,)

def back_keep(v):
    return (v, None)

def back_low(kept, grad):
    return (low(grad),)
low.defvjp(low_keep, low_pass)
low_back.defvjp(back_keep, back_low)

def dense(values, matrix):
    return jnp.dot(values, matrix, precision=lax.Precision.HIGHEST)

def layer_norm(values, gain, shift):
    center = values - lax.optimization_barrier(jnp.mean(values, -1, keepdims=True))
    return center * lax.rsqrt(lax.optimization_barrier(jnp.mean(center * center, -1, keepdims=True)) + EPS) * gain + shift

def attend(queries, keys, values, keep):
    scores = low_back(jnp.einsum('nqhe,nkhe->nhqk', queries, keys, precision=lax.Precision.HIGHEST) * 0.125)
    if keep is not None:
        scores = jnp.where(keep, scores, MASKED)
    shares = low(jax.nn.softmax(scores, -1))
    context = jnp.einsum('nhqk,nkhe->nqhe', shares, values, precision=lax.Precision.HIGHEST)
    return low(low_back(context))

def gelu_exact(values):
    return jax.nn.gelu(values, approximate=False)

def image_tower(tokens, gains, frozen):
    w_qkv, w_out, w_fc1, w_fc2 = frozen
    count = tokens.shape[0]
    length = tokens.shape[1]
    flat = tokens.reshape(count * length, D)
    normed = low(layer_norm(flat, gains[0], 0.0))
    shaped = [low(dense(normed, w_qkv[j])).reshape(count, length, HEADS, HEAD) for j in range(3)]
    context = attend(shaped[0], shaped[1], shaped[2], None).reshape(count * length, D)
    middle = flat + dense(context, w_out)
    normed2 = low(layer_norm(middle, gains[1], 0.0))
    result = middle + dense(low(gelu_exact(dense(normed2, w_fc1))), w_fc2)
    pooled = lax.optimization_barrier(jnp.mean(result.reshape(count, length, D), 1))
    return low(pooled * lax.rsqrt(lax.optimization_barrier(jnp.sum(pooled * pooled, -1, keepdims=True)) + EPS))

def text_block(tokens, ids, params):
    w_qkv, qv_bias, w_out, w_fc1, fc1_bias, w_fc2, gains, shifts, biases = params
    count = tokens.shape[0]
    flat = tokens.reshape(count * L, D)
    normed = low(layer_norm(flat, gains[0], shifts[0]))
    queries = low(low_back(dense(normed, w_qkv[0]) + qv_bias[0]))
    keys = low(low_back(dense(normed, w_qkv[1])))
    values = low(low_back(dense(normed, w_qkv[2]) + qv_bias[1]))
    keep = (ids > 0)[:, None, None, :]
    form = (count, L, HEADS, HEAD)
    context = attend(queries.reshape(form), keys.reshape(form), values.reshape(form), keep).reshape(count * L, D)
    middle = flat + (low_back(dense(context, w_out)) + biases[0])
    normed2 = low(layer_norm(middle, gains[1], shifts[1]))
    hidden = low_back(dense(normed2, w_fc1) + fc1_bias)
    result = middle + (low_back(dense(low(gelu_exact(hidden)), w_fc2)) + biases[1])
    present = (ids > 0).astype(jnp.float32)
    return lax.optimization_barrier(jnp.sum(result.reshape(count, L, D) * present[:, :, None], 1)) / lax.optimization_barrier(jnp.sum(present, 1, keepdims=True))

def reference(text_in, caption_ids, pairing, image_low, image_high, img_gains, img_qkv, img_out, img_fc1, img_fc2, txt_qkv, txt_qv_bias, txt_out, txt_fc1, txt_fc1_bias, txt_fc2, txt_gains, txt_shifts, txt_biases):
    blocks_all = N_DP * N_MP
    frozen = (img_qkv.astype(jnp.float32), img_out.astype(jnp.float32), img_fc1.astype(jnp.float32), img_fc2.astype(jnp.float32))

    def tower_block(block):
        return image_tower(block, img_gains, frozen)
    low_embeds = lax.map(tower_block, image_low.astype(jnp.float32).reshape(blocks_all, LOW_DEV, P_LOW, D))
    high_embeds = lax.map(tower_block, image_high.astype(jnp.float32).reshape(blocks_all, HIGH_DEV, P_HIGH, D))
    images = jnp.concatenate([low_embeds, high_embeds], 1).reshape(PAIRS, D)

    def objective(text_f, params):
        blocks = text_f.reshape(N_DP, PAIRS_DEV * N_MP, L, D)
        id_blocks = caption_ids.reshape(N_DP, PAIRS_DEV * N_MP, L)

        def one_block(member):
            return text_block(member[0], member[1], params)
        pooled = lax.map(jax.checkpoint(one_block), (blocks, id_blocks)).reshape(PAIRS, D)
        captions = low(pooled * lax.rsqrt(lax.optimization_barrier(jnp.sum(pooled * pooled, -1, keepdims=True)) + EPS))
        logits = low_back(SCALE * dense(images, captions.T))
        raised = jnp.exp(logits - SCALE)
        row_lse = SCALE + jnp.log(lax.optimization_barrier(jnp.sum(raised, 1)))
        col_lse = SCALE + jnp.log(lax.optimization_barrier(jnp.sum(raised, 0)))
        positive = jnp.sum(jnp.take_along_axis(logits, pairing[:, None], 1))
        total = 0.5 * jnp.sum(row_lse) + 0.5 * jnp.sum(col_lse) - positive
        return (LOSS_SCALE * total, total)
    params = (txt_qkv.astype(jnp.float32), txt_qv_bias.astype(jnp.float32), txt_out.astype(jnp.float32), txt_fc1.astype(jnp.float32), txt_fc1_bias.astype(jnp.float32), txt_fc2.astype(jnp.float32), txt_gains.astype(jnp.float32), txt_shifts.astype(jnp.float32), txt_biases.astype(jnp.float32))
    scaled, pullback, total = jax.vjp(objective, text_in.astype(jnp.float32), params, has_aux=True)
    grad_text, grads = pullback(jnp.ones_like(scaled))
    return (total / PAIRS, grad_text, grads[0], grads[1], grads[2], grads[3], grads[4], grads[5], grads[6], grads[7], grads[8])
```

```python
import jax
import jax.numpy as jnp
from jax import lax
from jax.sharding import PartitionSpec as P

D = 768
HEAD = 64
L = 16
P_LOW = 50
P_HIGH = 145


EPS = 1e-06
SCALE = 40.0
LOSS_SCALE = 16.0
MASKED = -1e30


def layer_stats(values):
    center = values - jnp.mean(values, -1, keepdims=True)
    inverse = lax.rsqrt(jnp.mean(center * center, -1, keepdims=True) + EPS)
    return (center * inverse, inverse)


def norm_back(grad_out, unit, inverse, gain):
    scaled = grad_out * gain
    return inverse * (
        scaled
        - jnp.mean(scaled, -1, keepdims=True)
        - unit * jnp.mean(scaled * unit, -1, keepdims=True)
    )


def gelu_exact(values):
    return jax.nn.gelu(values, approximate=False)


def score_rows(queries, keys_all, keep):
    scores = (
        jnp.einsum("nqhe,nkhe->nhqk", queries, keys_all, preferred_element_type=jnp.float32) * 0.125
    )
    if keep is not None:
        scores = jnp.where(keep, scores, MASKED)
    return scores


def attention_shares(queries, keys_all, keep):
    scores = score_rows(queries, keys_all, keep)
    highest = jnp.max(scores, -1, keepdims=True)
    raised = jnp.exp(scores - highest)
    totals = jnp.sum(raised, -1, keepdims=True)
    return (raised / totals, highest + jnp.log(totals))


def image_tower(tokens, count, length, gains, weights):
    w_qkv, w_out, w_fc1, w_fc2 = weights
    head_count = D // HEAD
    inputs = tokens.astype(jnp.float32)
    unit, spare = layer_stats(inputs)
    normed = (unit * gains[0]).astype(jnp.bfloat16)
    projected = jnp.einsum("rd,jdw->jrw", normed, w_qkv, preferred_element_type=jnp.float32).astype(
        jnp.bfloat16
    )
    shaped = projected.reshape(3, count, length, head_count, HEAD)
    shares, spare_lse = attention_shares(shaped[0], shaped[1], None)
    context = jnp.einsum(
        "nhqk,nkhe->nqhe",
        shares.astype(jnp.bfloat16),
        shaped[2],
        preferred_element_type=jnp.float32,
    )
    context = context.astype(jnp.bfloat16).reshape(count * length, D)
    middle = inputs + jnp.dot(context, w_out, preferred_element_type=jnp.float32)
    unit2, spare2 = layer_stats(middle)
    normed2 = (unit2 * gains[1]).astype(jnp.bfloat16)
    active = gelu_exact(jnp.dot(normed2, w_fc1, preferred_element_type=jnp.float32)).astype(
        jnp.bfloat16
    )
    result = middle + jnp.dot(active, w_fc2, preferred_element_type=jnp.float32)
    pooled = jnp.mean(result.reshape(count, length, D), 1)
    return (pooled * lax.rsqrt(jnp.sum(pooled * pooled, -1, keepdims=True) + EPS)).astype(
        jnp.bfloat16
    )


def local(
    text_in,
    caption_ids,
    pairing,
    image_low,
    image_high,
    img_gains,
    img_qkv,
    img_out,
    img_fc1,
    img_fc2,
    txt_qkv,
    txt_qv_bias,
    txt_out,
    txt_fc1,
    txt_fc1_bias,
    txt_fc2,
    txt_gains,
    txt_shifts,
    txt_biases,
):
    weights = (
        lax.all_gather(img_qkv, "mp", axis=2, tiled=True),
        lax.all_gather(img_out, "mp", axis=0, tiled=True),
        lax.all_gather(img_fc1, "mp", axis=1, tiled=True),
        lax.all_gather(img_fc2, "mp", axis=0, tiled=True),
    )
    low_count = image_low.shape[0] // P_LOW
    high_count = image_high.shape[0] // P_HIGH
    images16 = jnp.concatenate(
        [
            image_tower(image_low, low_count, P_LOW, img_gains, weights),
            image_tower(image_high, high_count, P_HIGH, img_gains, weights),
        ],
        0,
    )
    images_all = lax.all_gather(images16, ("dp", "mp"), axis=0, tiled=True)
    width = txt_qkv.shape[2]
    head_count = width // HEAD
    own_rows = text_in.shape[0]
    own_caps = own_rows // L
    group_caps = caption_ids.shape[0]
    group_rows = group_caps * L
    own_ids = lax.dynamic_slice_in_dim(caption_ids, lax.axis_index("mp") * own_caps, own_caps, 0)
    keep = (caption_ids > 0)[:, None, None, :]
    inputs = text_in.astype(jnp.float32)
    unit1, inverse1 = layer_stats(inputs)
    normed1 = (unit1 * txt_gains[0] + txt_shifts[0]).astype(jnp.bfloat16)
    bias_rows = jnp.stack([txt_qv_bias[0], jnp.zeros_like(txt_qv_bias[0]), txt_qv_bias[1]])
    piece = lax.all_gather(normed1, "mp", axis=0, tiled=True)
    made = jnp.einsum("rd,jdw->rjw", piece, txt_qkv, preferred_element_type=jnp.float32) + bias_rows
    joined = jnp.concatenate(
        [piece, made.astype(jnp.bfloat16).reshape(piece.shape[0], 3 * width)], 1
    )
    normed1_all = joined[:, :D]
    triple = joined[:, D:].reshape(group_caps, L, 3, head_count, HEAD)
    queries = triple[:, :, 0]
    keys_all = triple[:, :, 1]
    values_all = triple[:, :, 2]
    shares, log_totals = attention_shares(queries, keys_all, keep)
    context = jnp.einsum(
        "nhqk,nkhe->nqhe",
        shares.astype(jnp.bfloat16),
        values_all,
        preferred_element_type=jnp.float32,
    )
    context = context.astype(jnp.bfloat16).reshape(group_rows, width)
    middle = inputs + (
        lax.psum_scatter(
            jnp.dot(context, txt_out, preferred_element_type=jnp.float32).astype(jnp.bfloat16),
            "mp",
            scatter_dimension=0,
            tiled=True,
        ).astype(jnp.float32)
        + txt_biases[0]
    )
    unit2, inverse2 = layer_stats(middle)
    normed2 = (unit2 * txt_gains[1] + txt_shifts[1]).astype(jnp.bfloat16)
    piece = lax.all_gather(normed2, "mp", axis=0, tiled=True)
    hidden_piece = jnp.dot(piece, txt_fc1, preferred_element_type=jnp.float32) + txt_fc1_bias
    spread = jnp.concatenate([piece.astype(jnp.float32), hidden_piece], 1)
    normed2_all = spread[:, :D].astype(jnp.bfloat16)
    hidden = spread[:, D:]
    active, gelu_pull = jax.vjp(gelu_exact, hidden)
    active16 = active.astype(jnp.bfloat16)
    result = middle + (
        lax.psum_scatter(
            jnp.dot(active16, txt_fc2, preferred_element_type=jnp.float32).astype(jnp.bfloat16),
            "mp",
            scatter_dimension=0,
            tiled=True,
        ).astype(jnp.float32)
        + txt_biases[1]
    )
    present = (own_ids > 0).astype(jnp.float32)
    counts = jnp.sum(present, 1, keepdims=True)
    pooled = jnp.sum(result.reshape(own_caps, L, D) * present[:, :, None], 1) / counts
    inverse_len = lax.rsqrt(jnp.sum(pooled * pooled, -1, keepdims=True) + EPS)
    captions_unit = pooled * inverse_len
    captions16 = captions_unit.astype(jnp.bfloat16)
    total_pairs = pairing.shape[0]
    first_pair = lax.axis_index(("dp", "mp")) * own_caps
    arrived = lax.all_gather(captions16, ("dp", "mp"), axis=0, tiled=True)
    logits = SCALE * jnp.einsum("id,jd->ij", images_all, arrived, preferred_element_type=jnp.float32)
    matched = (pairing[:, None] == jnp.arange(total_pairs)[None, :]).astype(jnp.float32)
    raised = jnp.exp(logits - SCALE)
    row_lse = SCALE + jnp.log(jnp.sum(raised, 1))
    col_lse = SCALE + jnp.log(jnp.sum(raised, 0))
    total = 0.5 * jnp.sum(row_lse) + 0.5 * jnp.sum(col_lse) - jnp.sum(matched * logits)
    loss = total / total_pairs
    own_logits = lax.dynamic_slice_in_dim(logits, first_pair, own_caps, 1)
    own_col_lse = lax.dynamic_slice_in_dim(col_lse, first_pair, own_caps, 0)
    own_matched = lax.dynamic_slice_in_dim(matched, first_pair, own_caps, 1)
    grads16 = (
        LOSS_SCALE
        * (
            0.5 * jnp.exp(own_logits - row_lse[:, None])
            + 0.5 * jnp.exp(own_logits - own_col_lse[None, :])
            - own_matched
        )
    ).astype(jnp.bfloat16)
    grad_caps = SCALE * jnp.einsum(
        "ic,id->cd", grads16, images_all, preferred_element_type=jnp.float32
    )
    grad_pooled = inverse_len * (
        grad_caps - captions_unit * jnp.sum(captions_unit * grad_caps, -1, keepdims=True)
    )
    grad_result = (grad_pooled[:, None, :] * (present / counts)[:, :, None]).reshape(own_rows, D)
    grad_all = lax.all_gather(grad_result.astype(jnp.bfloat16), "mp", axis=0, tiled=True)
    grad_fc2 = jnp.einsum("gf,gd->fd", active16, grad_all, preferred_element_type=jnp.float32)
    grad_active = jnp.einsum("gd,fd->gf", grad_all, txt_fc2, preferred_element_type=jnp.float32)
    grad_hidden16 = gelu_pull(grad_active)[0].astype(jnp.bfloat16)
    grad_fc1 = jnp.einsum(
        "gd,gf->df", normed2_all, grad_hidden16, preferred_element_type=jnp.float32
    )
    grad_fc1_bias = jnp.sum(grad_hidden16.astype(jnp.float32), 0)
    grad_normed2 = lax.psum_scatter(
        jnp.einsum("gf,df->gd", grad_hidden16, txt_fc1, preferred_element_type=jnp.float32).astype(
            jnp.bfloat16
        ),
        "mp",
        scatter_dimension=0,
        tiled=True,
    ).astype(jnp.float32)
    grad_middle = grad_result + norm_back(grad_normed2, unit2, inverse2, txt_gains[1])
    grad_mid_all = lax.all_gather(grad_middle.astype(jnp.bfloat16), "mp", axis=0, tiled=True)
    grad_out = jnp.einsum("gw,gd->wd", context, grad_mid_all, preferred_element_type=jnp.float32)
    grad_context = jnp.einsum(
        "gd,wd->gw", grad_mid_all, txt_out, preferred_element_type=jnp.float32
    )
    grad_context = grad_context.astype(jnp.bfloat16).reshape(group_caps, L, head_count, HEAD)
    shares_again = jnp.exp(score_rows(queries, keys_all, keep) - log_totals)
    grad_shares = jnp.einsum(
        "nqhe,nkhe->nhqk", grad_context, values_all, preferred_element_type=jnp.float32
    )
    grad_values = jnp.einsum(
        "nhqk,nqhe->nkhe",
        shares_again.astype(jnp.bfloat16),
        grad_context,
        preferred_element_type=jnp.float32,
    ).astype(jnp.bfloat16)
    grad_scores = (
        shares_again * (grad_shares - jnp.sum(grad_shares * shares_again, -1, keepdims=True))
    ).astype(jnp.bfloat16)
    grad_queries = (
        jnp.einsum("nhqk,nkhe->nqhe", grad_scores, keys_all, preferred_element_type=jnp.float32)
        * 0.125
    ).astype(jnp.bfloat16)
    grad_keys = (
        jnp.einsum("nhqk,nqhe->nkhe", grad_scores, queries, preferred_element_type=jnp.float32)
        * 0.125
    ).astype(jnp.bfloat16)
    grad_triple = jnp.stack([grad_queries, grad_keys, grad_values], 0).reshape(3, group_rows, width)
    grad_qkv = jnp.einsum(
        "gd,jgw->jdw", normed1_all, grad_triple, preferred_element_type=jnp.float32
    )
    grad_qv_bias = jnp.stack(
        [
            jnp.sum(grad_triple[0].astype(jnp.float32), 0),
            jnp.sum(grad_triple[2].astype(jnp.float32), 0),
        ]
    )
    grad_normed1 = lax.psum_scatter(
        jnp.einsum("jgw,jdw->gd", grad_triple, txt_qkv, preferred_element_type=jnp.float32).astype(
            jnp.bfloat16
        ),
        "mp",
        scatter_dimension=0,
        tiled=True,
    ).astype(jnp.float32)
    grad_inputs = grad_middle + norm_back(grad_normed1, unit1, inverse1, txt_gains[0])
    summed16 = lax.psum(
        tuple(g.astype(jnp.bfloat16) for g in (grad_qkv, grad_out, grad_fc1, grad_fc2)), "dp"
    )
    summed_bias = lax.psum((grad_qv_bias, grad_fc1_bias), "dp")
    summed_grads = (
        summed16[0].astype(jnp.float32),
        summed_bias[0],
        summed16[1].astype(jnp.float32),
        summed16[2].astype(jnp.float32),
        summed_bias[1],
        summed16[3].astype(jnp.float32),
    )
    small_parts = jnp.stack(
        [
            jnp.sum(grad_normed1 * unit1, 0),
            jnp.sum(grad_normed2 * unit2, 0),
            jnp.sum(grad_normed1, 0),
            jnp.sum(grad_normed2, 0),
            jnp.sum(grad_middle, 0),
            jnp.sum(grad_result, 0),
        ]
    )
    shared = lax.psum(small_parts, ("dp", "mp"))
    return (
        loss,
        grad_inputs,
        summed_grads[0],
        summed_grads[1],
        summed_grads[2],
        summed_grads[3],
        summed_grads[4],
        summed_grads[5],
        shared[0:2],
        shared[2:4],
        shared[4:6],
    )


def solution(mesh):
    placed = (
        P(("dp", "mp"), None),
        P("dp", None),
        P(),
        P(("dp", "mp"), None),
        P(("dp", "mp"), None),
        P(),
        P(None, None, "mp"),
        P("mp", None),
        P(None, "mp"),
        P("mp", None),
        P(None, None, "mp"),
        P(None, "mp"),
        P("mp", None),
        P(None, "mp"),
        P("mp"),
        P("mp", None),
        P(),
        P(),
        P(),
    )
    return jax.shard_map(
        local,
        mesh=mesh,
        in_specs=placed,
        out_specs=(
            P(),
            P(("dp", "mp"), None),
            P(None, None, "mp"),
            P(None, "mp"),
            P("mp", None),
            P(None, "mp"),
            P("mp"),
            P("mp", None),
            P(),
            P(),
            P(),
        ),
        check_vma=False,
    )
```

```python
import jax
import jax.numpy as jnp
from jax import lax
from jax.sharding import PartitionSpec as P

D = 768
HEAD = 64
L = 16
P_LOW = 50
P_HIGH = 145


EPS = 1e-06
SCALE = 40.0
LOSS_SCALE = 16.0
MASKED = -1e30


def layer_stats(values):
    center = values - jnp.mean(values, -1, keepdims=True)
    inverse = lax.rsqrt(jnp.mean(center * center, -1, keepdims=True) + EPS)
    return (center * inverse, inverse)


def norm_back(grad_out, unit, inverse, gain):
    scaled = grad_out * gain
    return inverse * (
        scaled
        - jnp.mean(scaled, -1, keepdims=True)
        - unit * jnp.mean(scaled * unit, -1, keepdims=True)
    )


def gelu_exact(values):
    return jax.nn.gelu(values, approximate=False)


def score_rows(queries, keys_all, keep):
    scores = (
        jnp.einsum("nqhe,nkhe->nhqk", queries, keys_all, preferred_element_type=jnp.float32) * 0.125
    )
    if keep is not None:
        scores = jnp.where(keep, scores, MASKED)
    return scores


def attention_shares(queries, keys_all, keep):
    scores = score_rows(queries, keys_all, keep)
    highest = jnp.max(scores, -1, keepdims=True)
    raised = jnp.exp(scores - highest)
    totals = jnp.sum(raised, -1, keepdims=True)
    return (raised / totals, highest + jnp.log(totals))


def image_tower(tokens, count, length, gains, weights):
    w_qkv, w_out, w_fc1, w_fc2 = weights
    head_count = D // HEAD
    inputs = tokens.astype(jnp.float32)
    unit, spare = layer_stats(inputs)
    normed = (unit * gains[0]).astype(jnp.bfloat16)
    projected = jnp.einsum("rd,jdw->jrw", normed, w_qkv, preferred_element_type=jnp.float32).astype(
        jnp.bfloat16
    )
    shaped = projected.reshape(3, count, length, head_count, HEAD)
    shares, spare_lse = attention_shares(shaped[0], shaped[1], None)
    context = jnp.einsum(
        "nhqk,nkhe->nqhe",
        shares.astype(jnp.bfloat16),
        shaped[2],
        preferred_element_type=jnp.float32,
    )
    context = context.astype(jnp.bfloat16).reshape(count * length, D)
    middle = inputs + jnp.dot(context, w_out, preferred_element_type=jnp.float32)
    unit2, spare2 = layer_stats(middle)
    normed2 = (unit2 * gains[1]).astype(jnp.bfloat16)
    active = gelu_exact(jnp.dot(normed2, w_fc1, preferred_element_type=jnp.float32)).astype(
        jnp.bfloat16
    )
    result = middle + jnp.dot(active, w_fc2, preferred_element_type=jnp.float32)
    pooled = jnp.mean(result.reshape(count, length, D), 1)
    return (pooled * lax.rsqrt(jnp.sum(pooled * pooled, -1, keepdims=True) + EPS)).astype(
        jnp.bfloat16
    )


def local(
    text_in,
    caption_ids,
    pairing,
    image_low,
    image_high,
    img_gains,
    img_qkv,
    img_out,
    img_fc1,
    img_fc2,
    txt_qkv,
    txt_qv_bias,
    txt_out,
    txt_fc1,
    txt_fc1_bias,
    txt_fc2,
    txt_gains,
    txt_shifts,
    txt_biases,
):
    weights = (
        lax.all_gather(img_qkv, "mp", axis=2, tiled=True),
        lax.all_gather(img_out, "mp", axis=0, tiled=True),
        lax.all_gather(img_fc1, "mp", axis=1, tiled=True),
        lax.all_gather(img_fc2, "mp", axis=0, tiled=True),
    )
    low_count = image_low.shape[0] // P_LOW
    high_count = image_high.shape[0] // P_HIGH
    images16 = jnp.concatenate(
        [
            image_tower(image_low, low_count, P_LOW, img_gains, weights),
            image_tower(image_high, high_count, P_HIGH, img_gains, weights),
        ],
        0,
    )
    width = txt_qkv.shape[2]
    head_count = width // HEAD
    own_rows = text_in.shape[0]
    own_caps = own_rows // L
    group_caps = caption_ids.shape[0]
    group_rows = group_caps * L
    mp_index = lax.axis_index("mp")
    present = (caption_ids > 0).astype(jnp.float32)
    keep = (caption_ids > 0)[:, None, None, :]
    counts = jnp.sum(present, 1, keepdims=True)
    inputs = lax.all_gather(text_in, "mp", axis=0, tiled=True).astype(jnp.float32)
    unit1, inverse1 = layer_stats(inputs)
    normed1_all = (unit1 * txt_gains[0] + txt_shifts[0]).astype(jnp.bfloat16)
    bias_rows = jnp.stack([txt_qv_bias[0], jnp.zeros_like(txt_qv_bias[0]), txt_qv_bias[1]])
    made = (
        jnp.einsum("rd,jdw->rjw", normed1_all, txt_qkv, preferred_element_type=jnp.float32)
        + bias_rows
    )
    triple = made.astype(jnp.bfloat16).reshape(group_caps, L, 3, head_count, HEAD)
    queries = triple[:, :, 0]
    keys_all = triple[:, :, 1]
    values_all = triple[:, :, 2]
    shares, log_totals = attention_shares(queries, keys_all, keep)
    context = jnp.einsum(
        "nhqk,nkhe->nqhe",
        shares.astype(jnp.bfloat16),
        values_all,
        preferred_element_type=jnp.float32,
    )
    context = context.astype(jnp.bfloat16).reshape(group_rows, width)
    middle = inputs + (
        lax.psum(
            jnp.dot(context, txt_out, preferred_element_type=jnp.float32).astype(jnp.bfloat16),
            "mp",
        ).astype(jnp.float32)
        + txt_biases[0]
    )
    unit2, inverse2 = layer_stats(middle)
    normed2_all = (unit2 * txt_gains[1] + txt_shifts[1]).astype(jnp.bfloat16)
    hidden = jnp.dot(normed2_all, txt_fc1, preferred_element_type=jnp.float32) + txt_fc1_bias
    active, gelu_pull = jax.vjp(gelu_exact, hidden)
    active16 = active.astype(jnp.bfloat16)
    ffn_part = jnp.dot(active16, txt_fc2, preferred_element_type=jnp.float32)
    ffn_pooled = jnp.sum(ffn_part.reshape(group_caps, L, D) * present[:, :, None], 1)
    image_slots = lax.dynamic_update_slice_in_dim(
        jnp.zeros((group_caps, D), jnp.float32),
        images16.astype(jnp.float32),
        mp_index * own_caps,
        0,
    )
    both = lax.psum(jnp.concatenate([ffn_pooled, image_slots], 0), "mp")
    mid_pooled = jnp.sum(middle.reshape(group_caps, L, D) * present[:, :, None], 1)
    pooled = (mid_pooled + both[:group_caps]) / counts + txt_biases[1]
    inverse_len = lax.rsqrt(jnp.sum(pooled * pooled, -1, keepdims=True) + EPS)
    captions_unit = pooled * inverse_len
    captions16 = captions_unit.astype(jnp.bfloat16)
    gathered = lax.all_gather(
        jnp.concatenate([captions16, both[group_caps:].astype(jnp.bfloat16)], 0), "dp", axis=0
    )
    arrived = gathered[:, :group_caps].reshape(-1, D)
    images_all = gathered[:, group_caps:].reshape(-1, D)
    total_pairs = pairing.shape[0]
    first_pair = lax.axis_index("dp") * group_caps
    logits = SCALE * jnp.einsum("id,jd->ij", images_all, arrived, preferred_element_type=jnp.float32)
    matched = (pairing[:, None] == jnp.arange(total_pairs)[None, :]).astype(jnp.float32)
    raised = jnp.exp(logits - SCALE)
    row_lse = SCALE + jnp.log(jnp.sum(raised, 1))
    col_lse = SCALE + jnp.log(jnp.sum(raised, 0))
    total = 0.5 * jnp.sum(row_lse) + 0.5 * jnp.sum(col_lse) - jnp.sum(matched * logits)
    loss = total / total_pairs
    own_logits = lax.dynamic_slice_in_dim(logits, first_pair, group_caps, 1)
    own_col_lse = lax.dynamic_slice_in_dim(col_lse, first_pair, group_caps, 0)
    own_matched = lax.dynamic_slice_in_dim(matched, first_pair, group_caps, 1)
    grads16 = (
        LOSS_SCALE
        * (
            0.5 * jnp.exp(own_logits - row_lse[:, None])
            + 0.5 * jnp.exp(own_logits - own_col_lse[None, :])
            - own_matched
        )
    ).astype(jnp.bfloat16)
    grad_caps = SCALE * jnp.einsum(
        "ic,id->cd", grads16, images_all, preferred_element_type=jnp.float32
    )
    grad_pooled = inverse_len * (
        grad_caps - captions_unit * jnp.sum(captions_unit * grad_caps, -1, keepdims=True)
    )
    grad_result = (grad_pooled[:, None, :] * (present / counts)[:, :, None]).reshape(group_rows, D)
    grad_all = grad_result.astype(jnp.bfloat16)
    grad_fc2 = jnp.einsum("gf,gd->fd", active16, grad_all, preferred_element_type=jnp.float32)
    grad_active = jnp.einsum("gd,fd->gf", grad_all, txt_fc2, preferred_element_type=jnp.float32)
    grad_hidden16 = gelu_pull(grad_active)[0].astype(jnp.bfloat16)
    grad_fc1 = jnp.einsum(
        "gd,gf->df", normed2_all, grad_hidden16, preferred_element_type=jnp.float32
    )
    grad_fc1_bias = jnp.sum(grad_hidden16.astype(jnp.float32), 0)
    grad_normed2 = lax.psum(
        jnp.einsum("gf,df->gd", grad_hidden16, txt_fc1, preferred_element_type=jnp.float32).astype(
            jnp.bfloat16
        ),
        "mp",
    ).astype(jnp.float32)
    grad_middle = grad_result + norm_back(grad_normed2, unit2, inverse2, txt_gains[1])
    grad_mid_all = grad_middle.astype(jnp.bfloat16)
    grad_out = jnp.einsum("gw,gd->wd", context, grad_mid_all, preferred_element_type=jnp.float32)
    grad_context = jnp.einsum(
        "gd,wd->gw", grad_mid_all, txt_out, preferred_element_type=jnp.float32
    )
    grad_context = grad_context.astype(jnp.bfloat16).reshape(group_caps, L, head_count, HEAD)
    shares_again = jnp.exp(score_rows(queries, keys_all, keep) - log_totals)
    grad_shares = jnp.einsum(
        "nqhe,nkhe->nhqk", grad_context, values_all, preferred_element_type=jnp.float32
    )
    grad_values = jnp.einsum(
        "nhqk,nqhe->nkhe",
        shares_again.astype(jnp.bfloat16),
        grad_context,
        preferred_element_type=jnp.float32,
    ).astype(jnp.bfloat16)
    grad_scores = (
        shares_again * (grad_shares - jnp.sum(grad_shares * shares_again, -1, keepdims=True))
    ).astype(jnp.bfloat16)
    grad_queries = (
        jnp.einsum("nhqk,nkhe->nqhe", grad_scores, keys_all, preferred_element_type=jnp.float32)
        * 0.125
    ).astype(jnp.bfloat16)
    grad_keys = (
        jnp.einsum("nhqk,nqhe->nkhe", grad_scores, queries, preferred_element_type=jnp.float32)
        * 0.125
    ).astype(jnp.bfloat16)
    grad_triple = jnp.stack([grad_queries, grad_keys, grad_values], 0).reshape(3, group_rows, width)
    grad_qkv = jnp.einsum(
        "gd,jgw->jdw", normed1_all, grad_triple, preferred_element_type=jnp.float32
    )
    grad_qv_bias = jnp.stack(
        [
            jnp.sum(grad_triple[0].astype(jnp.float32), 0),
            jnp.sum(grad_triple[2].astype(jnp.float32), 0),
        ]
    )
    grad_normed1 = lax.psum_scatter(
        jnp.einsum("jgw,jdw->gd", grad_triple, txt_qkv, preferred_element_type=jnp.float32).astype(
            jnp.bfloat16
        ),
        "mp",
        scatter_dimension=0,
        tiled=True,
    ).astype(jnp.float32)

    def own(values):
        return lax.dynamic_slice_in_dim(values, mp_index * own_rows, own_rows, 0)

    unit1_own = own(unit1)
    grad_normed2_own = own(grad_normed2)
    unit2_own = own(unit2)
    grad_middle_own = own(grad_middle)
    grad_inputs = grad_middle_own + norm_back(grad_normed1, unit1_own, own(inverse1), txt_gains[0])
    summed16 = lax.psum(
        tuple(g.astype(jnp.bfloat16) for g in (grad_qkv, grad_out, grad_fc1, grad_fc2)), "dp"
    )
    summed_bias = lax.psum((grad_qv_bias, grad_fc1_bias), "dp")
    small_parts = jnp.stack(
        [
            jnp.sum(grad_normed1 * unit1_own, 0),
            jnp.sum(grad_normed2_own * unit2_own, 0),
            jnp.sum(grad_normed1, 0),
            jnp.sum(grad_normed2_own, 0),
            jnp.sum(grad_middle_own, 0),
            jnp.sum(own(grad_result), 0),
        ]
    )
    shared = lax.psum(small_parts, ("dp", "mp"))
    return (
        loss,
        grad_inputs,
        summed16[0].astype(jnp.float32),
        summed_bias[0],
        summed16[1].astype(jnp.float32),
        summed16[2].astype(jnp.float32),
        summed_bias[1],
        summed16[3].astype(jnp.float32),
        shared[0:2],
        shared[2:4],
        shared[4:6],
    )


def solution(mesh):
    placed = (
        P(("dp", "mp"), None),
        P("dp", None),
        P(),
        P(("dp", "mp"), None),
        P(("dp", "mp"), None),
        P(),
        P(None, None, "mp"),
        P("mp", None),
        P(None, "mp"),
        P("mp", None),
        P(None, None, "mp"),
        P(None, "mp"),
        P("mp", None),
        P(None, "mp"),
        P("mp"),
        P("mp", None),
        P(),
        P(),
        P(),
    )
    return jax.shard_map(
        local,
        mesh=mesh,
        in_specs=placed,
        out_specs=(
            P(),
            P(("dp", "mp"), None),
            P(None, None, "mp"),
            P(None, "mp"),
            P("mp", None),
            P(None, "mp"),
            P("mp"),
            P("mp", None),
            P(),
            P(),
            P(),
        ),
        check_vma=False,
    )
```

```python
import jax
import jax.numpy as jnp
from jax import lax
from jax.sharding import PartitionSpec as P

D = 768
HEAD = 64
L = 16
P_LOW = 50
P_HIGH = 145


EPS = 1e-06
SCALE = 40.0
LOSS_SCALE = 16.0
MASKED = -1e30


def layer_stats(values):
    center = values - jnp.mean(values, -1, keepdims=True)
    inverse = lax.rsqrt(jnp.mean(center * center, -1, keepdims=True) + EPS)
    return (center * inverse, inverse)


def norm_back(grad_out, unit, inverse, gain):
    scaled = grad_out * gain
    return inverse * (
        scaled
        - jnp.mean(scaled, -1, keepdims=True)
        - unit * jnp.mean(scaled * unit, -1, keepdims=True)
    )


def gelu_exact(values):
    return jax.nn.gelu(values, approximate=False)


def score_rows(queries, keys_all, keep):
    scores = (
        jnp.einsum("nqhe,nkhe->nhqk", queries, keys_all, preferred_element_type=jnp.float32) * 0.125
    )
    if keep is not None:
        scores = jnp.where(keep, scores, MASKED)
    return scores


def attention_shares(queries, keys_all, keep):
    scores = score_rows(queries, keys_all, keep)
    highest = jnp.max(scores, -1, keepdims=True)
    raised = jnp.exp(scores - highest)
    totals = jnp.sum(raised, -1, keepdims=True)
    return (raised / totals, highest + jnp.log(totals))


def axis_bits(axis):
    count = lax.axis_size(axis)
    bits = count.bit_length() - 1
    assert 1 << bits == count
    return count, list(reversed(range(bits)))


def exchange(values, axis, count, bit):
    return lax.ppermute(values, axis, [(i, i ^ (1 << bit)) for i in range(count)])


def gather_stacked(values, axis):
    count, bits = axis_bits(axis)
    data = values[None]
    for bit in bits:
        data = jnp.concatenate([data, exchange(data, axis, count, bit)], 0)
    return data


def gather_ordered(values, axis):
    count, bits = axis_bits(axis)
    index = lax.axis_index(axis)
    data = values
    done = []
    for bit in bits:
        other = exchange(data, axis, count, bit)
        upper = ((index >> bit) & 1) == 1
        data = jnp.stack([jnp.where(upper, other, data), jnp.where(upper, data, other)], 0)
        done.insert(0, bit)
    order = sorted(range(len(done)), key=lambda a: -done[a])
    data = data.transpose(order + list(range(len(done), data.ndim)))
    return data.reshape((count,) + values.shape)


def sum_exchanged(values, axis):
    count, bits = axis_bits(axis)
    for bit in reversed(bits):
        values = values + exchange(values, axis, count, bit)
    return values


def image_tower(tokens, count, length, gains, weights):
    w_qkv, w_out, w_fc1, w_fc2 = weights
    head_count = D // HEAD
    inputs = tokens.astype(jnp.float32)
    unit, spare = layer_stats(inputs)
    normed = (unit * gains[0]).astype(jnp.bfloat16)
    projected = jnp.einsum("rd,jdw->jrw", normed, w_qkv, preferred_element_type=jnp.float32).astype(
        jnp.bfloat16
    )
    shaped = projected.reshape(3, count, length, head_count, HEAD)
    shares, spare_lse = attention_shares(shaped[0], shaped[1], None)
    context = jnp.einsum(
        "nhqk,nkhe->nqhe",
        shares.astype(jnp.bfloat16),
        shaped[2],
        preferred_element_type=jnp.float32,
    )
    context = context.astype(jnp.bfloat16).reshape(count * length, D)
    middle = inputs + jnp.dot(context, w_out, preferred_element_type=jnp.float32)
    unit2, spare2 = layer_stats(middle)
    normed2 = (unit2 * gains[1]).astype(jnp.bfloat16)
    active = gelu_exact(jnp.dot(normed2, w_fc1, preferred_element_type=jnp.float32)).astype(
        jnp.bfloat16
    )
    result = middle + jnp.dot(active, w_fc2, preferred_element_type=jnp.float32)
    pooled = jnp.mean(result.reshape(count, length, D), 1)
    return (pooled * lax.rsqrt(jnp.sum(pooled * pooled, -1, keepdims=True) + EPS)).astype(
        jnp.bfloat16
    )


def local(
    text_in,
    caption_ids,
    pairing,
    image_low,
    image_high,
    img_gains,
    img_qkv,
    img_out,
    img_fc1,
    img_fc2,
    txt_qkv,
    txt_qv_bias,
    txt_out,
    txt_fc1,
    txt_fc1_bias,
    txt_fc2,
    txt_gains,
    txt_shifts,
    txt_biases,
):
    qkv_parts = gather_stacked(img_qkv, "mp")
    fc1_parts = gather_stacked(img_fc1, "mp")
    weights = (
        qkv_parts.transpose(1, 2, 0, 3).reshape(3, D, -1),
        gather_stacked(img_out, "mp").reshape(-1, D),
        fc1_parts.transpose(1, 0, 2).reshape(D, -1),
        gather_stacked(img_fc2, "mp").reshape(-1, D),
    )
    low_count = image_low.shape[0] // P_LOW
    high_count = image_high.shape[0] // P_HIGH
    images16 = jnp.concatenate(
        [
            image_tower(image_low, low_count, P_LOW, img_gains, weights),
            image_tower(image_high, high_count, P_HIGH, img_gains, weights),
        ],
        0,
    )
    width = txt_qkv.shape[2]
    head_count = width // HEAD
    own_rows = text_in.shape[0]
    own_caps = own_rows // L
    group_caps = caption_ids.shape[0]
    group_rows = group_caps * L
    mp_index = lax.axis_index("mp")
    present = (caption_ids > 0).astype(jnp.float32)
    keep = (caption_ids > 0)[:, None, None, :]
    counts = jnp.sum(present, 1, keepdims=True)
    inputs = lax.all_gather(text_in, "mp", axis=0, tiled=True).astype(jnp.float32)
    unit1, inverse1 = layer_stats(inputs)
    normed1_all = (unit1 * txt_gains[0] + txt_shifts[0]).astype(jnp.bfloat16)
    bias_rows = jnp.stack([txt_qv_bias[0], jnp.zeros_like(txt_qv_bias[0]), txt_qv_bias[1]])
    made = (
        jnp.einsum("rd,jdw->rjw", normed1_all, txt_qkv, preferred_element_type=jnp.float32)
        + bias_rows
    )
    triple = made.astype(jnp.bfloat16).reshape(group_caps, L, 3, head_count, HEAD)
    queries = triple[:, :, 0]
    keys_all = triple[:, :, 1]
    values_all = triple[:, :, 2]
    shares, log_totals = attention_shares(queries, keys_all, keep)
    context = jnp.einsum(
        "nhqk,nkhe->nqhe",
        shares.astype(jnp.bfloat16),
        values_all,
        preferred_element_type=jnp.float32,
    )
    context = context.astype(jnp.bfloat16).reshape(group_rows, width)
    middle = inputs + (
        lax.psum(
            jnp.dot(context, txt_out, preferred_element_type=jnp.float32).astype(jnp.bfloat16),
            "mp",
        ).astype(jnp.float32)
        + txt_biases[0]
    )
    unit2, inverse2 = layer_stats(middle)
    normed2_all = (unit2 * txt_gains[1] + txt_shifts[1]).astype(jnp.bfloat16)
    hidden = jnp.dot(normed2_all, txt_fc1, preferred_element_type=jnp.float32) + txt_fc1_bias
    active, gelu_pull = jax.vjp(gelu_exact, hidden)
    active16 = active.astype(jnp.bfloat16)
    ffn_part = jnp.dot(active16, txt_fc2, preferred_element_type=jnp.float32)
    ffn_pooled = jnp.sum(ffn_part.reshape(group_caps, L, D) * present[:, :, None], 1)
    image_slots = lax.dynamic_update_slice_in_dim(
        jnp.zeros((group_caps, D), jnp.float32),
        images16.astype(jnp.float32),
        mp_index * own_caps,
        0,
    )
    both = sum_exchanged(jnp.concatenate([ffn_pooled, image_slots], 0), "mp")
    mid_pooled = jnp.sum(middle.reshape(group_caps, L, D) * present[:, :, None], 1)
    pooled = (mid_pooled + both[:group_caps]) / counts + txt_biases[1]
    inverse_len = lax.rsqrt(jnp.sum(pooled * pooled, -1, keepdims=True) + EPS)
    captions_unit = pooled * inverse_len
    captions16 = captions_unit.astype(jnp.bfloat16)
    gathered = gather_ordered(
        jnp.concatenate([captions16, both[group_caps:].astype(jnp.bfloat16)], 0), "dp"
    )
    arrived = gathered[:, :group_caps].reshape(-1, D)
    images_all = gathered[:, group_caps:].reshape(-1, D)
    total_pairs = pairing.shape[0]
    first_pair = lax.axis_index("dp") * group_caps
    logits = SCALE * jnp.einsum("id,jd->ij", images_all, arrived, preferred_element_type=jnp.float32)
    matched = (pairing[:, None] == jnp.arange(total_pairs)[None, :]).astype(jnp.float32)
    raised = jnp.exp(logits - SCALE)
    row_lse = SCALE + jnp.log(jnp.sum(raised, 1))
    col_lse = SCALE + jnp.log(jnp.sum(raised, 0))
    total = 0.5 * jnp.sum(row_lse) + 0.5 * jnp.sum(col_lse) - jnp.sum(matched * logits)
    loss = total / total_pairs
    own_logits = lax.dynamic_slice_in_dim(logits, first_pair, group_caps, 1)
    own_col_lse = lax.dynamic_slice_in_dim(col_lse, first_pair, group_caps, 0)
    own_matched = lax.dynamic_slice_in_dim(matched, first_pair, group_caps, 1)
    grads16 = (
        LOSS_SCALE
        * (
            0.5 * jnp.exp(own_logits - row_lse[:, None])
            + 0.5 * jnp.exp(own_logits - own_col_lse[None, :])
            - own_matched
        )
    ).astype(jnp.bfloat16)
    grad_caps = SCALE * jnp.einsum(
        "ic,id->cd", grads16, images_all, preferred_element_type=jnp.float32
    )
    grad_pooled = inverse_len * (
        grad_caps - captions_unit * jnp.sum(captions_unit * grad_caps, -1, keepdims=True)
    )
    grad_result = (grad_pooled[:, None, :] * (present / counts)[:, :, None]).reshape(group_rows, D)
    grad_all = grad_result.astype(jnp.bfloat16)
    grad_fc2 = jnp.einsum("gf,gd->fd", active16, grad_all, preferred_element_type=jnp.float32)
    grad_active = jnp.einsum("gd,fd->gf", grad_all, txt_fc2, preferred_element_type=jnp.float32)
    grad_hidden16 = gelu_pull(grad_active)[0].astype(jnp.bfloat16)
    grad_fc1 = jnp.einsum(
        "gd,gf->df", normed2_all, grad_hidden16, preferred_element_type=jnp.float32
    )
    grad_fc1_bias = jnp.sum(grad_hidden16.astype(jnp.float32), 0)
    grad_normed2 = lax.psum(
        jnp.einsum("gf,df->gd", grad_hidden16, txt_fc1, preferred_element_type=jnp.float32).astype(
            jnp.bfloat16
        ),
        "mp",
    ).astype(jnp.float32)
    grad_middle = grad_result + norm_back(grad_normed2, unit2, inverse2, txt_gains[1])
    grad_mid_all = grad_middle.astype(jnp.bfloat16)
    grad_out = jnp.einsum("gw,gd->wd", context, grad_mid_all, preferred_element_type=jnp.float32)
    grad_context = jnp.einsum(
        "gd,wd->gw", grad_mid_all, txt_out, preferred_element_type=jnp.float32
    )
    grad_context = grad_context.astype(jnp.bfloat16).reshape(group_caps, L, head_count, HEAD)
    shares_again = jnp.exp(score_rows(queries, keys_all, keep) - log_totals)
    grad_shares = jnp.einsum(
        "nqhe,nkhe->nhqk", grad_context, values_all, preferred_element_type=jnp.float32
    )
    grad_values = jnp.einsum(
        "nhqk,nqhe->nkhe",
        shares_again.astype(jnp.bfloat16),
        grad_context,
        preferred_element_type=jnp.float32,
    ).astype(jnp.bfloat16)
    grad_scores = (
        shares_again * (grad_shares - jnp.sum(grad_shares * shares_again, -1, keepdims=True))
    ).astype(jnp.bfloat16)
    grad_queries = (
        jnp.einsum("nhqk,nkhe->nqhe", grad_scores, keys_all, preferred_element_type=jnp.float32)
        * 0.125
    ).astype(jnp.bfloat16)
    grad_keys = (
        jnp.einsum("nhqk,nqhe->nkhe", grad_scores, queries, preferred_element_type=jnp.float32)
        * 0.125
    ).astype(jnp.bfloat16)
    grad_triple = jnp.stack([grad_queries, grad_keys, grad_values], 0).reshape(3, group_rows, width)
    grad_qkv = jnp.einsum(
        "gd,jgw->jdw", normed1_all, grad_triple, preferred_element_type=jnp.float32
    )
    grad_qv_bias = jnp.stack(
        [
            jnp.sum(grad_triple[0].astype(jnp.float32), 0),
            jnp.sum(grad_triple[2].astype(jnp.float32), 0),
        ]
    )
    grad_normed1 = lax.psum_scatter(
        jnp.einsum("jgw,jdw->gd", grad_triple, txt_qkv, preferred_element_type=jnp.float32).astype(
            jnp.bfloat16
        ),
        "mp",
        scatter_dimension=0,
        tiled=True,
    ).astype(jnp.float32)

    def own(values):
        return lax.dynamic_slice_in_dim(values, mp_index * own_rows, own_rows, 0)

    unit1_own = own(unit1)
    grad_normed2_own = own(grad_normed2)
    unit2_own = own(unit2)
    grad_middle_own = own(grad_middle)
    grad_inputs = grad_middle_own + norm_back(grad_normed1, unit1_own, own(inverse1), txt_gains[0])
    summed16 = lax.psum(
        tuple(g.astype(jnp.bfloat16) for g in (grad_qkv, grad_out, grad_fc1, grad_fc2)), "dp"
    )
    summed_bias = lax.psum((grad_qv_bias, grad_fc1_bias), "dp")
    small_parts = jnp.stack(
        [
            jnp.sum(grad_normed1 * unit1_own, 0),
            jnp.sum(grad_normed2_own * unit2_own, 0),
            jnp.sum(grad_normed1, 0),
            jnp.sum(grad_normed2_own, 0),
            jnp.sum(grad_middle_own, 0),
            jnp.sum(own(grad_result), 0),
        ]
    )
    shared = lax.psum(small_parts, ("dp", "mp"))
    return (
        loss,
        grad_inputs,
        summed16[0].astype(jnp.float32),
        summed_bias[0],
        summed16[1].astype(jnp.float32),
        summed16[2].astype(jnp.float32),
        summed_bias[1],
        summed16[3].astype(jnp.float32),
        shared[0:2],
        shared[2:4],
        shared[4:6],
    )


def solution(mesh):
    placed = (
        P(("dp", "mp"), None),
        P("dp", None),
        P(),
        P(("dp", "mp"), None),
        P(("dp", "mp"), None),
        P(),
        P(None, None, "mp"),
        P("mp", None),
        P(None, "mp"),
        P("mp", None),
        P(None, None, "mp"),
        P(None, "mp"),
        P("mp", None),
        P(None, "mp"),
        P("mp"),
        P("mp", None),
        P(),
        P(),
        P(),
    )
    return jax.shard_map(
        local,
        mesh=mesh,
        in_specs=placed,
        out_specs=(
            P(),
            P(("dp", "mp"), None),
            P(None, None, "mp"),
            P(None, "mp"),
            P("mp", None),
            P(None, "mp"),
            P("mp"),
            P("mp", None),
            P(),
            P(),
            P(),
        ),
        check_vma=False,
    )
```

```python
import jax
import jax.numpy as jnp
from jax import lax
from jax.sharding import PartitionSpec as P

D = 768
HEAD = 64
L = 16
P_LOW = 50
P_HIGH = 145


EPS = 1e-06
SCALE = 40.0
LOSS_SCALE = 16.0
MASKED = -1e30


def layer_stats(values):
    center = values - jnp.mean(values, -1, keepdims=True)
    inverse = lax.rsqrt(jnp.mean(center * center, -1, keepdims=True) + EPS)
    return (center * inverse, inverse)


def norm_back(grad_out, unit, inverse, gain):
    scaled = grad_out * gain
    return inverse * (
        scaled
        - jnp.mean(scaled, -1, keepdims=True)
        - unit * jnp.mean(scaled * unit, -1, keepdims=True)
    )


def gelu_exact(values):
    return jax.nn.gelu(values, approximate=False)


def score_rows(queries, keys_all, keep):
    scores = (
        jnp.einsum("nqhe,nkhe->nhqk", queries, keys_all, preferred_element_type=jnp.float32) * 0.125
    )
    if keep is not None:
        scores = jnp.where(keep, scores, MASKED)
    return scores


def attention_shares(queries, keys_all, keep):
    scores = score_rows(queries, keys_all, keep)
    highest = jnp.max(scores, -1, keepdims=True)
    raised = jnp.exp(scores - highest)
    totals = jnp.sum(raised, -1, keepdims=True)
    return (raised / totals, highest + jnp.log(totals))


def axis_bits(axis):
    count = lax.axis_size(axis)
    bits = count.bit_length() - 1
    assert 1 << bits == count
    return count, list(reversed(range(bits)))


def exchange(values, axis, count, bit):
    return lax.ppermute(values, axis, [(i, i ^ (1 << bit)) for i in range(count)])


def gather_stacked(values, axis):
    count, bits = axis_bits(axis)
    data = values[None]
    for bit in bits:
        data = jnp.concatenate([data, exchange(data, axis, count, bit)], 0)
    return data


def gather_ordered(values, axis):
    count, bits = axis_bits(axis)
    index = lax.axis_index(axis)
    data = values
    done = []
    for bit in bits:
        other = exchange(data, axis, count, bit)
        upper = ((index >> bit) & 1) == 1
        data = jnp.stack([jnp.where(upper, other, data), jnp.where(upper, data, other)], 0)
        done.insert(0, bit)
    order = sorted(range(len(done)), key=lambda a: -done[a])
    data = data.transpose(order + list(range(len(done), data.ndim)))
    return data.reshape((count,) + values.shape)


def sum_exchanged(values, axis):
    count, bits = axis_bits(axis)
    for bit in reversed(bits):
        values = values + exchange(values, axis, count, bit)
    return values


def scatter_exchanged(values, axis):
    count, bits = axis_bits(axis)
    index = lax.axis_index(axis)
    data = values.reshape((2,) * len(bits) + (values.shape[0] // count,) + values.shape[1:])
    for bit in reversed(bits):
        place = len(bits) - 1 - bit
        mine = (index >> bit) & 1
        kept = lax.dynamic_index_in_dim(data, mine, place, keepdims=False)
        sent = lax.dynamic_index_in_dim(data, 1 - mine, place, keepdims=False)
        data = kept + exchange(sent.astype(jnp.bfloat16), axis, count, bit).astype(jnp.float32)
    return data


def reduce_exchanged(values, axis):
    part = scatter_exchanged(values, axis).astype(jnp.bfloat16)
    return gather_ordered(part, axis).reshape(values.shape)


def image_tower(tokens, count, length, gains, weights):
    w_qkv, w_out, w_fc1, w_fc2 = weights
    head_count = D // HEAD
    inputs = tokens.astype(jnp.float32)
    unit, spare = layer_stats(inputs)
    normed = (unit * gains[0]).astype(jnp.bfloat16)
    projected = jnp.einsum("rd,jdw->jrw", normed, w_qkv, preferred_element_type=jnp.float32).astype(
        jnp.bfloat16
    )
    shaped = projected.reshape(3, count, length, head_count, HEAD)
    shares, spare_lse = attention_shares(shaped[0], shaped[1], None)
    context = jnp.einsum(
        "nhqk,nkhe->nqhe",
        shares.astype(jnp.bfloat16),
        shaped[2],
        preferred_element_type=jnp.float32,
    )
    context = context.astype(jnp.bfloat16).reshape(count * length, D)
    middle = inputs + jnp.dot(context, w_out, preferred_element_type=jnp.float32)
    unit2, spare2 = layer_stats(middle)
    normed2 = (unit2 * gains[1]).astype(jnp.bfloat16)
    active = gelu_exact(jnp.dot(normed2, w_fc1, preferred_element_type=jnp.float32)).astype(
        jnp.bfloat16
    )
    result = middle + jnp.dot(active, w_fc2, preferred_element_type=jnp.float32)
    pooled = jnp.mean(result.reshape(count, length, D), 1)
    return (pooled * lax.rsqrt(jnp.sum(pooled * pooled, -1, keepdims=True) + EPS)).astype(
        jnp.bfloat16
    )


def local(
    text_in,
    caption_ids,
    pairing,
    image_low,
    image_high,
    img_gains,
    img_qkv,
    img_out,
    img_fc1,
    img_fc2,
    txt_qkv,
    txt_qv_bias,
    txt_out,
    txt_fc1,
    txt_fc1_bias,
    txt_fc2,
    txt_gains,
    txt_shifts,
    txt_biases,
):
    qkv_parts = gather_stacked(img_qkv, "mp")
    fc1_parts = gather_stacked(img_fc1, "mp")
    weights = (
        qkv_parts.transpose(1, 2, 0, 3).reshape(3, D, -1),
        gather_stacked(img_out, "mp").reshape(-1, D),
        fc1_parts.transpose(1, 0, 2).reshape(D, -1),
        gather_stacked(img_fc2, "mp").reshape(-1, D),
    )
    low_count = image_low.shape[0] // P_LOW
    high_count = image_high.shape[0] // P_HIGH
    images16 = jnp.concatenate(
        [
            image_tower(image_low, low_count, P_LOW, img_gains, weights),
            image_tower(image_high, high_count, P_HIGH, img_gains, weights),
        ],
        0,
    )
    width = txt_qkv.shape[2]
    head_count = width // HEAD
    own_rows = text_in.shape[0]
    own_caps = own_rows // L
    group_caps = caption_ids.shape[0]
    group_rows = group_caps * L
    mp_index = lax.axis_index("mp")
    present = (caption_ids > 0).astype(jnp.float32)
    keep = (caption_ids > 0)[:, None, None, :]
    counts = jnp.sum(present, 1, keepdims=True)
    inputs = lax.all_gather(text_in, "mp", axis=0, tiled=True).astype(jnp.float32)
    unit1, inverse1 = layer_stats(inputs)
    normed1_all = (unit1 * txt_gains[0] + txt_shifts[0]).astype(jnp.bfloat16)
    bias_rows = jnp.stack([txt_qv_bias[0], jnp.zeros_like(txt_qv_bias[0]), txt_qv_bias[1]])
    made = (
        jnp.einsum("rd,jdw->rjw", normed1_all, txt_qkv, preferred_element_type=jnp.float32)
        + bias_rows
    )
    triple = made.astype(jnp.bfloat16).reshape(group_caps, L, 3, head_count, HEAD)
    queries = triple[:, :, 0]
    keys_all = triple[:, :, 1]
    values_all = triple[:, :, 2]
    shares, log_totals = attention_shares(queries, keys_all, keep)
    context = jnp.einsum(
        "nhqk,nkhe->nqhe",
        shares.astype(jnp.bfloat16),
        values_all,
        preferred_element_type=jnp.float32,
    )
    context = context.astype(jnp.bfloat16).reshape(group_rows, width)
    middle = inputs + (
        lax.psum(
            jnp.dot(context, txt_out, preferred_element_type=jnp.float32).astype(jnp.bfloat16),
            "mp",
        ).astype(jnp.float32)
        + txt_biases[0]
    )
    unit2, inverse2 = layer_stats(middle)
    normed2_all = (unit2 * txt_gains[1] + txt_shifts[1]).astype(jnp.bfloat16)
    hidden = jnp.dot(normed2_all, txt_fc1, preferred_element_type=jnp.float32) + txt_fc1_bias
    active, gelu_pull = jax.vjp(gelu_exact, hidden)
    active16 = active.astype(jnp.bfloat16)
    ffn_part = jnp.dot(active16, txt_fc2, preferred_element_type=jnp.float32)
    ffn_pooled = jnp.sum(ffn_part.reshape(group_caps, L, D) * present[:, :, None], 1)
    image_slots = lax.dynamic_update_slice_in_dim(
        jnp.zeros((group_caps, D), jnp.float32),
        images16.astype(jnp.float32),
        mp_index * own_caps,
        0,
    )
    both = sum_exchanged(jnp.concatenate([ffn_pooled, image_slots], 0), "mp")
    mid_pooled = jnp.sum(middle.reshape(group_caps, L, D) * present[:, :, None], 1)
    pooled = (mid_pooled + both[:group_caps]) / counts + txt_biases[1]
    inverse_len = lax.rsqrt(jnp.sum(pooled * pooled, -1, keepdims=True) + EPS)
    captions_unit = pooled * inverse_len
    captions16 = captions_unit.astype(jnp.bfloat16)
    gathered = gather_ordered(
        jnp.concatenate([captions16, both[group_caps:].astype(jnp.bfloat16)], 0), "dp"
    )
    arrived = gathered[:, :group_caps].reshape(-1, D)
    images_all = gathered[:, group_caps:].reshape(-1, D)
    total_pairs = pairing.shape[0]
    first_pair = lax.axis_index("dp") * group_caps
    logits = SCALE * jnp.einsum("id,jd->ij", images_all, arrived, preferred_element_type=jnp.float32)
    matched = (pairing[:, None] == jnp.arange(total_pairs)[None, :]).astype(jnp.float32)
    raised = jnp.exp(logits - SCALE)
    row_lse = SCALE + jnp.log(jnp.sum(raised, 1))
    col_lse = SCALE + jnp.log(jnp.sum(raised, 0))
    total = 0.5 * jnp.sum(row_lse) + 0.5 * jnp.sum(col_lse) - jnp.sum(matched * logits)
    loss = total / total_pairs
    own_logits = lax.dynamic_slice_in_dim(logits, first_pair, group_caps, 1)
    own_col_lse = lax.dynamic_slice_in_dim(col_lse, first_pair, group_caps, 0)
    own_matched = lax.dynamic_slice_in_dim(matched, first_pair, group_caps, 1)
    grads16 = (
        LOSS_SCALE
        * (
            0.5 * jnp.exp(own_logits - row_lse[:, None])
            + 0.5 * jnp.exp(own_logits - own_col_lse[None, :])
            - own_matched
        )
    ).astype(jnp.bfloat16)
    grad_caps = SCALE * jnp.einsum(
        "ic,id->cd", grads16, images_all, preferred_element_type=jnp.float32
    )
    grad_pooled = inverse_len * (
        grad_caps - captions_unit * jnp.sum(captions_unit * grad_caps, -1, keepdims=True)
    )
    grad_result = (grad_pooled[:, None, :] * (present / counts)[:, :, None]).reshape(group_rows, D)
    grad_all = grad_result.astype(jnp.bfloat16)
    grad_fc2 = jnp.einsum("gf,gd->fd", active16, grad_all, preferred_element_type=jnp.float32)
    grad_active = jnp.einsum("gd,fd->gf", grad_all, txt_fc2, preferred_element_type=jnp.float32)
    grad_hidden16 = gelu_pull(grad_active)[0].astype(jnp.bfloat16)
    grad_fc1 = jnp.einsum(
        "gd,gf->df", normed2_all, grad_hidden16, preferred_element_type=jnp.float32
    )
    grad_fc1_bias = jnp.sum(grad_hidden16.astype(jnp.float32), 0)
    fc_sums = lax.psum((grad_fc1.astype(jnp.bfloat16), grad_fc2.astype(jnp.bfloat16)), "dp")
    grad_normed2 = reduce_exchanged(
        jnp.einsum("gf,df->gd", grad_hidden16, txt_fc1, preferred_element_type=jnp.float32), "mp"
    ).astype(jnp.float32)
    grad_middle = grad_result + norm_back(grad_normed2, unit2, inverse2, txt_gains[1])
    grad_mid_all = grad_middle.astype(jnp.bfloat16)
    grad_out = jnp.einsum("gw,gd->wd", context, grad_mid_all, preferred_element_type=jnp.float32)
    grad_context = jnp.einsum(
        "gd,wd->gw", grad_mid_all, txt_out, preferred_element_type=jnp.float32
    )
    grad_context = grad_context.astype(jnp.bfloat16).reshape(group_caps, L, head_count, HEAD)
    shares_again = jnp.exp(score_rows(queries, keys_all, keep) - log_totals)
    grad_shares = jnp.einsum(
        "nqhe,nkhe->nhqk", grad_context, values_all, preferred_element_type=jnp.float32
    )
    grad_values = jnp.einsum(
        "nhqk,nqhe->nkhe",
        shares_again.astype(jnp.bfloat16),
        grad_context,
        preferred_element_type=jnp.float32,
    ).astype(jnp.bfloat16)
    grad_scores = (
        shares_again * (grad_shares - jnp.sum(grad_shares * shares_again, -1, keepdims=True))
    ).astype(jnp.bfloat16)
    grad_queries = (
        jnp.einsum("nhqk,nkhe->nqhe", grad_scores, keys_all, preferred_element_type=jnp.float32)
        * 0.125
    ).astype(jnp.bfloat16)
    grad_keys = (
        jnp.einsum("nhqk,nqhe->nkhe", grad_scores, queries, preferred_element_type=jnp.float32)
        * 0.125
    ).astype(jnp.bfloat16)
    grad_triple = jnp.stack([grad_queries, grad_keys, grad_values], 0).reshape(3, group_rows, width)
    grad_qkv = jnp.einsum(
        "gd,jgw->jdw", normed1_all, grad_triple, preferred_element_type=jnp.float32
    )
    grad_qv_bias = jnp.stack(
        [
            jnp.sum(grad_triple[0].astype(jnp.float32), 0),
            jnp.sum(grad_triple[2].astype(jnp.float32), 0),
        ]
    )
    fc_sums, attn_parts = lax.optimization_barrier(
        (fc_sums, (grad_qkv.astype(jnp.bfloat16), grad_out.astype(jnp.bfloat16)))
    )
    attn_sums = lax.psum(attn_parts, "dp")
    grad_normed1 = scatter_exchanged(
        jnp.einsum("jgw,jdw->gd", grad_triple, txt_qkv, preferred_element_type=jnp.float32), "mp"
    )

    def own(values):
        return lax.dynamic_slice_in_dim(values, mp_index * own_rows, own_rows, 0)

    unit1_own = own(unit1)
    grad_normed2_own = own(grad_normed2)
    unit2_own = own(unit2)
    grad_middle_own = own(grad_middle)
    grad_inputs = grad_middle_own + norm_back(grad_normed1, unit1_own, own(inverse1), txt_gains[0])
    small_parts = jnp.stack(
        [
            jnp.sum(grad_normed1 * unit1_own, 0),
            jnp.sum(grad_normed2_own * unit2_own, 0),
            jnp.sum(grad_normed1, 0),
            jnp.sum(grad_normed2_own, 0),
            jnp.sum(grad_middle_own, 0),
            jnp.sum(own(grad_result), 0),
        ]
    )
    shared, summed_bias = lax.psum(
        (sum_exchanged(small_parts, "mp"), (grad_qv_bias, grad_fc1_bias)), "dp"
    )
    return (
        loss,
        grad_inputs,
        attn_sums[0].astype(jnp.float32),
        summed_bias[0],
        attn_sums[1].astype(jnp.float32),
        fc_sums[0].astype(jnp.float32),
        summed_bias[1],
        fc_sums[1].astype(jnp.float32),
        shared[0:2],
        shared[2:4],
        shared[4:6],
    )


def solution(mesh):
    placed = (
        P(("dp", "mp"), None),
        P("dp", None),
        P(),
        P(("dp", "mp"), None),
        P(("dp", "mp"), None),
        P(),
        P(None, None, "mp"),
        P("mp", None),
        P(None, "mp"),
        P("mp", None),
        P(None, None, "mp"),
        P(None, "mp"),
        P("mp", None),
        P(None, "mp"),
        P("mp"),
        P("mp", None),
        P(),
        P(),
        P(),
    )
    return jax.shard_map(
        local,
        mesh=mesh,
        in_specs=placed,
        out_specs=(
            P(),
            P(("dp", "mp"), None),
            P(None, None, "mp"),
            P(None, "mp"),
            P("mp", None),
            P(None, "mp"),
            P("mp"),
            P("mp", None),
            P(),
            P(),
            P(),
        ),
        check_vma=False,
    )
```

```python
import jax
import jax.numpy as jnp
from jax import lax
from jax.sharding import PartitionSpec as P

D = 768
HEAD = 64
L = 16
P_LOW = 50
P_HIGH = 145


EPS = 1e-06
SCALE = 40.0
LOSS_SCALE = 16.0
MASKED = -1e30


def layer_stats(values):
    center = values - jnp.mean(values, -1, keepdims=True)
    inverse = lax.rsqrt(jnp.mean(center * center, -1, keepdims=True) + EPS)
    return (center * inverse, inverse)


def norm_back(grad_out, unit, inverse, gain):
    scaled = grad_out * gain
    return inverse * (
        scaled
        - jnp.mean(scaled, -1, keepdims=True)
        - unit * jnp.mean(scaled * unit, -1, keepdims=True)
    )


def gelu_exact(values):
    return jax.nn.gelu(values, approximate=False)


def score_rows(queries, keys_all, keep):
    scores = (
        jnp.einsum("nqhe,nkhe->nhqk", queries, keys_all, preferred_element_type=jnp.float32) * 0.125
    )
    if keep is not None:
        scores = jnp.where(keep, scores, MASKED)
    return scores


def attention_shares(queries, keys_all, keep):
    scores = score_rows(queries, keys_all, keep)
    highest = jnp.max(scores, -1, keepdims=True)
    raised = jnp.exp(scores - highest)
    totals = jnp.sum(raised, -1, keepdims=True)
    return (raised / totals, highest + jnp.log(totals))


def axis_bits(axis):
    count = lax.axis_size(axis)
    bits = count.bit_length() - 1
    assert 1 << bits == count
    return count, list(reversed(range(bits)))


def exchange(values, axis, count, bit):
    return lax.ppermute(values, axis, [(i, i ^ (1 << bit)) for i in range(count)])


def gather_stacked(values, axis):
    count, bits = axis_bits(axis)
    data = values[None]
    for bit in bits:
        data = jnp.concatenate([data, exchange(data, axis, count, bit)], 0)
    return data


def gather_ordered(values, axis):
    count, bits = axis_bits(axis)
    index = lax.axis_index(axis)
    data = values
    done = []
    for bit in bits:
        other = exchange(data, axis, count, bit)
        upper = ((index >> bit) & 1) == 1
        data = jnp.stack([jnp.where(upper, other, data), jnp.where(upper, data, other)], 0)
        done.insert(0, bit)
    order = sorted(range(len(done)), key=lambda a: -done[a])
    data = data.transpose(order + list(range(len(done), data.ndim)))
    return data.reshape((count,) + values.shape)


def sum_exchanged(values, axis):
    count, bits = axis_bits(axis)
    for bit in reversed(bits):
        values = values + exchange(values, axis, count, bit)
    return values


def scatter_exchanged(values, axis):
    count, bits = axis_bits(axis)
    index = lax.axis_index(axis)
    data = values.reshape((2,) * len(bits) + (values.shape[0] // count,) + values.shape[1:])
    for bit in reversed(bits):
        place = len(bits) - 1 - bit
        mine = (index >> bit) & 1
        kept = lax.dynamic_index_in_dim(data, mine, place, keepdims=False)
        sent = lax.dynamic_index_in_dim(data, 1 - mine, place, keepdims=False)
        data = kept + exchange(sent.astype(jnp.bfloat16), axis, count, bit).astype(jnp.float32)
    return data


def reduce_exchanged(values, axis):
    part = scatter_exchanged(values, axis).astype(jnp.bfloat16)
    return gather_ordered(part, axis).reshape(values.shape)


def image_tower(tokens, count, length, gains, weights):
    w_qkv, w_out, w_fc1, w_fc2 = weights
    head_count = D // HEAD
    inputs = tokens.astype(jnp.float32)
    unit, spare = layer_stats(inputs)
    normed = (unit * gains[0]).astype(jnp.bfloat16)
    projected = jnp.einsum("rd,jdw->jrw", normed, w_qkv, preferred_element_type=jnp.float32).astype(
        jnp.bfloat16
    )
    shaped = projected.reshape(3, count, length, head_count, HEAD)
    shares, spare_lse = attention_shares(shaped[0], shaped[1], None)
    context = jnp.einsum(
        "nhqk,nkhe->nqhe",
        shares.astype(jnp.bfloat16),
        shaped[2],
        preferred_element_type=jnp.float32,
    )
    context = context.astype(jnp.bfloat16).reshape(count * length, D)
    middle = inputs + jnp.dot(context, w_out, preferred_element_type=jnp.float32)
    unit2, spare2 = layer_stats(middle)
    normed2 = (unit2 * gains[1]).astype(jnp.bfloat16)
    active = gelu_exact(jnp.dot(normed2, w_fc1, preferred_element_type=jnp.float32)).astype(
        jnp.bfloat16
    )
    result = middle + jnp.dot(active, w_fc2, preferred_element_type=jnp.float32)
    pooled = jnp.mean(result.reshape(count, length, D), 1)
    return (pooled * lax.rsqrt(jnp.sum(pooled * pooled, -1, keepdims=True) + EPS)).astype(
        jnp.bfloat16
    )


def local(
    text_in,
    caption_ids,
    pairing,
    image_low,
    image_high,
    img_gains,
    img_qkv,
    img_out,
    img_fc1,
    img_fc2,
    txt_qkv,
    txt_qv_bias,
    txt_out,
    txt_fc1,
    txt_fc1_bias,
    txt_fc2,
    txt_gains,
    txt_shifts,
    txt_biases,
):
    qkv_parts = gather_stacked(img_qkv, "mp")
    fc1_parts = gather_stacked(img_fc1, "mp")
    weights = (
        qkv_parts.transpose(1, 2, 0, 3).reshape(3, D, -1),
        gather_stacked(img_out, "mp").reshape(-1, D),
        fc1_parts.transpose(1, 0, 2).reshape(D, -1),
        gather_stacked(img_fc2, "mp").reshape(-1, D),
    )
    low_count = image_low.shape[0] // P_LOW
    high_count = image_high.shape[0] // P_HIGH
    images16 = jnp.concatenate(
        [
            image_tower(image_low, low_count, P_LOW, img_gains, weights),
            image_tower(image_high, high_count, P_HIGH, img_gains, weights),
        ],
        0,
    )
    width = txt_qkv.shape[2]
    head_count = width // HEAD
    own_rows = text_in.shape[0]
    own_caps = own_rows // L
    group_caps = caption_ids.shape[0]
    group_rows = group_caps * L
    mp_index = lax.axis_index("mp")
    present = (caption_ids > 0).astype(jnp.float32)
    keep = (caption_ids > 0)[:, None, None, :]
    counts = jnp.sum(present, 1, keepdims=True)
    inputs = lax.all_gather(text_in, "mp", axis=0, tiled=True).astype(jnp.float32)
    unit1, inverse1 = layer_stats(inputs)
    normed1_all = (unit1 * txt_gains[0] + txt_shifts[0]).astype(jnp.bfloat16)
    bias_rows = jnp.stack([txt_qv_bias[0], jnp.zeros_like(txt_qv_bias[0]), txt_qv_bias[1]])
    made = (
        jnp.einsum("rd,jdw->rjw", normed1_all, txt_qkv, preferred_element_type=jnp.float32)
        + bias_rows
    )
    triple = made.astype(jnp.bfloat16).reshape(group_caps, L, 3, head_count, HEAD)
    queries = triple[:, :, 0]
    keys_all = triple[:, :, 1]
    values_all = triple[:, :, 2]
    shares, log_totals = attention_shares(queries, keys_all, keep)
    context = jnp.einsum(
        "nhqk,nkhe->nqhe",
        shares.astype(jnp.bfloat16),
        values_all,
        preferred_element_type=jnp.float32,
    )
    context = context.astype(jnp.bfloat16).reshape(group_rows, width)
    middle = inputs + (
        lax.psum(
            jnp.dot(context, txt_out, preferred_element_type=jnp.float32).astype(jnp.bfloat16),
            "mp",
        ).astype(jnp.float32)
        + txt_biases[0]
    )
    unit2, inverse2 = layer_stats(middle)
    normed2_all = (unit2 * txt_gains[1] + txt_shifts[1]).astype(jnp.bfloat16)
    hidden = jnp.dot(normed2_all, txt_fc1, preferred_element_type=jnp.float32) + txt_fc1_bias
    active, gelu_pull = jax.vjp(gelu_exact, hidden)
    active16 = active.astype(jnp.bfloat16)
    ffn_part = jnp.dot(active16, txt_fc2, preferred_element_type=jnp.float32)
    ffn_pooled = jnp.sum(ffn_part.reshape(group_caps, L, D) * present[:, :, None], 1)
    image_slots = lax.dynamic_update_slice_in_dim(
        jnp.zeros((group_caps, D), jnp.float32),
        images16.astype(jnp.float32),
        mp_index * own_caps,
        0,
    )
    both = sum_exchanged(jnp.concatenate([ffn_pooled, image_slots], 0), "mp")
    mid_pooled = jnp.sum(middle.reshape(group_caps, L, D) * present[:, :, None], 1)
    pooled = (mid_pooled + both[:group_caps]) / counts + txt_biases[1]
    inverse_len = lax.rsqrt(jnp.sum(pooled * pooled, -1, keepdims=True) + EPS)
    captions_unit = pooled * inverse_len
    captions16 = captions_unit.astype(jnp.bfloat16)
    gathered = gather_ordered(
        jnp.concatenate([captions16, both[group_caps:].astype(jnp.bfloat16)], 0), "dp"
    )
    arrived = gathered[:, :group_caps].reshape(-1, D)
    images_all = gathered[:, group_caps:].reshape(-1, D)
    total_pairs = pairing.shape[0]
    first_pair = lax.axis_index("dp") * group_caps
    logits = SCALE * jnp.einsum("id,jd->ij", images_all, arrived, preferred_element_type=jnp.float32)
    matched = (pairing[:, None] == jnp.arange(total_pairs)[None, :]).astype(jnp.float32)
    raised = jnp.exp(logits - SCALE)
    row_lse = SCALE + jnp.log(jnp.sum(raised, 1))
    col_lse = SCALE + jnp.log(jnp.sum(raised, 0))
    total = 0.5 * jnp.sum(row_lse) + 0.5 * jnp.sum(col_lse) - jnp.sum(matched * logits)
    loss = total / total_pairs
    own_logits = lax.dynamic_slice_in_dim(logits, first_pair, group_caps, 1)
    own_col_lse = lax.dynamic_slice_in_dim(col_lse, first_pair, group_caps, 0)
    own_matched = lax.dynamic_slice_in_dim(matched, first_pair, group_caps, 1)
    grads16 = (
        LOSS_SCALE
        * (
            0.5 * jnp.exp(own_logits - row_lse[:, None])
            + 0.5 * jnp.exp(own_logits - own_col_lse[None, :])
            - own_matched
        )
    ).astype(jnp.bfloat16)
    grad_caps = SCALE * jnp.einsum(
        "ic,id->cd", grads16, images_all, preferred_element_type=jnp.float32
    )
    grad_pooled = inverse_len * (
        grad_caps - captions_unit * jnp.sum(captions_unit * grad_caps, -1, keepdims=True)
    )
    grad_result = (grad_pooled[:, None, :] * (present / counts)[:, :, None]).reshape(group_rows, D)
    grad_all = grad_result.astype(jnp.bfloat16)
    grad_fc2 = jnp.einsum("gf,gd->fd", active16, grad_all, preferred_element_type=jnp.float32)
    grad_active = jnp.einsum("gd,fd->gf", grad_all, txt_fc2, preferred_element_type=jnp.float32)
    grad_hidden16 = gelu_pull(grad_active)[0].astype(jnp.bfloat16)
    grad_fc1 = jnp.einsum(
        "gd,gf->df", normed2_all, grad_hidden16, preferred_element_type=jnp.float32
    )
    grad_fc1_bias = jnp.sum(grad_hidden16.astype(jnp.float32), 0)
    fc_sums = reduce_exchanged(jnp.concatenate([grad_fc1, grad_fc2], 0), "dp")
    grad_normed2 = reduce_exchanged(
        jnp.einsum("gf,df->gd", grad_hidden16, txt_fc1, preferred_element_type=jnp.float32), "mp"
    ).astype(jnp.float32)
    grad_middle = grad_result + norm_back(grad_normed2, unit2, inverse2, txt_gains[1])
    grad_mid_all = grad_middle.astype(jnp.bfloat16)
    grad_out = jnp.einsum("gw,gd->wd", context, grad_mid_all, preferred_element_type=jnp.float32)
    grad_context = jnp.einsum(
        "gd,wd->gw", grad_mid_all, txt_out, preferred_element_type=jnp.float32
    )
    grad_context = grad_context.astype(jnp.bfloat16).reshape(group_caps, L, head_count, HEAD)
    shares_again = jnp.exp(score_rows(queries, keys_all, keep) - log_totals)
    grad_shares = jnp.einsum(
        "nqhe,nkhe->nhqk", grad_context, values_all, preferred_element_type=jnp.float32
    )
    grad_values = jnp.einsum(
        "nhqk,nqhe->nkhe",
        shares_again.astype(jnp.bfloat16),
        grad_context,
        preferred_element_type=jnp.float32,
    ).astype(jnp.bfloat16)
    grad_scores = (
        shares_again * (grad_shares - jnp.sum(grad_shares * shares_again, -1, keepdims=True))
    ).astype(jnp.bfloat16)
    grad_queries = (
        jnp.einsum("nhqk,nkhe->nqhe", grad_scores, keys_all, preferred_element_type=jnp.float32)
        * 0.125
    ).astype(jnp.bfloat16)
    grad_keys = (
        jnp.einsum("nhqk,nqhe->nkhe", grad_scores, queries, preferred_element_type=jnp.float32)
        * 0.125
    ).astype(jnp.bfloat16)
    grad_triple = jnp.stack([grad_queries, grad_keys, grad_values], 0).reshape(3, group_rows, width)
    grad_qkv = jnp.einsum(
        "gd,jgw->jdw", normed1_all, grad_triple, preferred_element_type=jnp.float32
    )
    grad_qv_bias = jnp.stack(
        [
            jnp.sum(grad_triple[0].astype(jnp.float32), 0),
            jnp.sum(grad_triple[2].astype(jnp.float32), 0),
        ]
    )
    attn_sums = reduce_exchanged(jnp.concatenate([grad_qkv.reshape(-1, D), grad_out], 0), "dp")
    grad_normed1 = scatter_exchanged(
        jnp.einsum("jgw,jdw->gd", grad_triple, txt_qkv, preferred_element_type=jnp.float32), "mp"
    )

    def own(values):
        return lax.dynamic_slice_in_dim(values, mp_index * own_rows, own_rows, 0)

    unit1_own = own(unit1)
    grad_normed2_own = own(grad_normed2)
    unit2_own = own(unit2)
    grad_middle_own = own(grad_middle)
    grad_inputs = grad_middle_own + norm_back(grad_normed1, unit1_own, own(inverse1), txt_gains[0])
    small_parts = jnp.stack(
        [
            jnp.sum(grad_normed1 * unit1_own, 0),
            jnp.sum(grad_normed2_own * unit2_own, 0),
            jnp.sum(grad_normed1, 0),
            jnp.sum(grad_normed2_own, 0),
            jnp.sum(grad_middle_own, 0),
            jnp.sum(own(grad_result), 0),
        ]
    )
    bias_rows = jnp.stack(
        [jnp.concatenate([grad_qv_bias.reshape(-1), jnp.zeros_like(grad_qv_bias.reshape(-1))]), grad_fc1_bias]
    )
    shared = sum_exchanged(jnp.concatenate([sum_exchanged(small_parts, "mp"), bias_rows], 0), "dp")
    qv_count = grad_qv_bias.size
    fc1_rows = grad_fc1.shape[0]
    return (
        loss,
        grad_inputs,
        attn_sums[: grad_qkv.size // D].astype(jnp.float32).reshape(grad_qkv.shape),
        shared[6, :qv_count].reshape(grad_qv_bias.shape),
        attn_sums[grad_qkv.size // D :].astype(jnp.float32),
        fc_sums[:fc1_rows].astype(jnp.float32),
        shared[7],
        fc_sums[fc1_rows:].astype(jnp.float32),
        shared[0:2],
        shared[2:4],
        shared[4:6],
    )


def solution(mesh):
    placed = (
        P(("dp", "mp"), None),
        P("dp", None),
        P(),
        P(("dp", "mp"), None),
        P(("dp", "mp"), None),
        P(),
        P(None, None, "mp"),
        P("mp", None),
        P(None, "mp"),
        P("mp", None),
        P(None, None, "mp"),
        P(None, "mp"),
        P("mp", None),
        P(None, "mp"),
        P("mp"),
        P("mp", None),
        P(),
        P(),
        P(),
    )
    return jax.shard_map(
        local,
        mesh=mesh,
        in_specs=placed,
        out_specs=(
            P(),
            P(("dp", "mp"), None),
            P(None, None, "mp"),
            P(None, "mp"),
            P("mp", None),
            P(None, "mp"),
            P("mp"),
            P("mp", None),
            P(),
            P(),
            P(),
        ),
        check_vma=False,
    )
```

```python
import jax
import jax.numpy as jnp
from jax import lax
from jax.sharding import PartitionSpec as P

D = 768
HEAD = 64
L = 16
P_LOW = 50
P_HIGH = 145


EPS = 1e-06
SCALE = 40.0
LOSS_SCALE = 16.0
MASKED = -1e30


def layer_stats(values):
    center = values - jnp.mean(values, -1, keepdims=True)
    inverse = lax.rsqrt(jnp.mean(center * center, -1, keepdims=True) + EPS)
    return (center * inverse, inverse)


def norm_back(grad_out, unit, inverse, gain):
    scaled = grad_out * gain
    return inverse * (
        scaled
        - jnp.mean(scaled, -1, keepdims=True)
        - unit * jnp.mean(scaled * unit, -1, keepdims=True)
    )


def gelu_exact(values):
    return jax.nn.gelu(values, approximate=False)


def score_rows(queries, keys_all, keep):
    scores = (
        jnp.einsum("nqhe,nkhe->nhqk", queries, keys_all, preferred_element_type=jnp.float32) * 0.125
    )
    if keep is not None:
        scores = jnp.where(keep, scores, MASKED)
    return scores


def attention_shares(queries, keys_all, keep):
    scores = score_rows(queries, keys_all, keep)
    highest = jnp.max(scores, -1, keepdims=True)
    raised = jnp.exp(scores - highest)
    totals = jnp.sum(raised, -1, keepdims=True)
    return (raised / totals, highest + jnp.log(totals))


def axis_bits(axis):
    count = lax.axis_size(axis)
    bits = count.bit_length() - 1
    assert 1 << bits == count
    return count, list(reversed(range(bits)))


def exchange(values, axis, count, bit):
    return lax.ppermute(values, axis, [(i, i ^ (1 << bit)) for i in range(count)])


def gather_stacked(values, axis):
    count, bits = axis_bits(axis)
    data = values[None]
    for bit in bits:
        data = jnp.concatenate([data, exchange(data, axis, count, bit)], 0)
    return data


def gather_ordered(values, axis):
    count, bits = axis_bits(axis)
    index = lax.axis_index(axis)
    data = values
    done = []
    for bit in bits:
        other = exchange(data, axis, count, bit)
        upper = ((index >> bit) & 1) == 1
        data = jnp.stack([jnp.where(upper, other, data), jnp.where(upper, data, other)], 0)
        done.insert(0, bit)
    order = sorted(range(len(done)), key=lambda a: -done[a])
    data = data.transpose(order + list(range(len(done), data.ndim)))
    return data.reshape((count,) + values.shape)


def sum_exchanged(values, axis):
    count, bits = axis_bits(axis)
    for bit in reversed(bits):
        values = values + exchange(values, axis, count, bit)
    return values


def scatter_exchanged(values, axis):
    count, bits = axis_bits(axis)
    index = lax.axis_index(axis)
    data = values.reshape((2,) * len(bits) + (values.shape[0] // count,) + values.shape[1:])
    for bit in reversed(bits):
        place = len(bits) - 1 - bit
        mine = (index >> bit) & 1
        kept = lax.dynamic_index_in_dim(data, mine, place, keepdims=False)
        sent = lax.dynamic_index_in_dim(data, 1 - mine, place, keepdims=False)
        data = kept + exchange(sent.astype(jnp.bfloat16), axis, count, bit).astype(jnp.float32)
    return data


def reduce_exchanged(values, axis):
    part = scatter_exchanged(values, axis).astype(jnp.bfloat16)
    return gather_ordered(part, axis).reshape(values.shape)


def image_tower(tokens, count, length, gains, weights):
    w_qkv, w_out, w_fc1, w_fc2 = weights
    _, middle = image_attention(tokens, count, length, gains, w_qkv, w_out)
    return image_ffn(middle, count, length, gains, w_fc1, w_fc2)


def image_attention(tokens, count, length, gains, w_qkv, w_out):
    head_count = D // HEAD
    inputs = tokens.astype(jnp.float32)
    unit, _ = layer_stats(inputs)
    normed = (unit * gains[0]).astype(jnp.bfloat16)
    projected = jnp.einsum("rd,jdw->jrw", normed, w_qkv, preferred_element_type=jnp.float32).astype(
        jnp.bfloat16
    )
    shaped = projected.reshape(3, count, length, head_count, HEAD)
    shares, _ = attention_shares(shaped[0], shaped[1], None)
    context = jnp.einsum(
        "nhqk,nkhe->nqhe",
        shares.astype(jnp.bfloat16),
        shaped[2],
        preferred_element_type=jnp.float32,
    )
    context = context.astype(jnp.bfloat16).reshape(count * length, D)
    middle = inputs + jnp.dot(context, w_out, preferred_element_type=jnp.float32)
    return inputs, middle


def image_ffn(middle, count, length, gains, w_fc1, w_fc2):
    unit2, _ = layer_stats(middle)
    normed2 = (unit2 * gains[1]).astype(jnp.bfloat16)
    active = gelu_exact(jnp.dot(normed2, w_fc1, preferred_element_type=jnp.float32)).astype(
        jnp.bfloat16
    )
    mean_active = jnp.mean(active.astype(jnp.float32).reshape(count, length, -1), 1)
    pooled = jnp.mean(middle.reshape(count, length, D), 1) + jnp.dot(
        mean_active, w_fc2.astype(jnp.float32), precision=lax.Precision.HIGHEST
    )
    return (pooled * lax.rsqrt(jnp.sum(pooled * pooled, -1, keepdims=True) + EPS)).astype(
        jnp.bfloat16
    )


def local_body(
    text_in,
    caption_ids,
    pairing,
    image_low,
    image_high,
    img_gains,
    img_qkv,
    img_out,
    img_fc1,
    img_fc2,
    txt_qkv,
    txt_qv_bias,
    txt_out,
    txt_fc1,
    txt_fc1_bias,
    txt_fc2,
    txt_gains,
    txt_shifts,
    txt_biases,
):
    qkv_parts = gather_stacked(img_qkv, "mp")
    fc1_parts = gather_stacked(img_fc1, "mp")
    weights = (
        qkv_parts.transpose(1, 2, 0, 3).reshape(3, D, -1),
        gather_stacked(img_out, "mp").reshape(-1, D),
        fc1_parts.transpose(1, 0, 2).reshape(D, -1),
        gather_stacked(img_fc2, "mp").reshape(-1, D),
    )
    low_count = image_low.shape[0] // P_LOW
    high_count = image_high.shape[0] // P_HIGH
    images16 = jnp.concatenate(
        [
            image_tower(image_low, low_count, P_LOW, img_gains, weights),
            image_tower(image_high, high_count, P_HIGH, img_gains, weights),
        ],
        0,
    )
    width = txt_qkv.shape[2]
    head_count = width // HEAD
    own_rows = text_in.shape[0]
    own_caps = own_rows // L
    group_caps = caption_ids.shape[0]
    group_rows = group_caps * L
    mp_index = lax.axis_index("mp")
    present = (caption_ids > 0).astype(jnp.float32)
    keep = (caption_ids > 0)[:, None, None, :]
    counts = jnp.sum(present, 1, keepdims=True)
    inputs = lax.all_gather(text_in, "mp", axis=0, tiled=True).astype(jnp.float32)
    unit1, inverse1 = layer_stats(inputs)
    normed1_all = (unit1 * txt_gains[0] + txt_shifts[0]).astype(jnp.bfloat16)
    bias_rows = jnp.stack([txt_qv_bias[0], jnp.zeros_like(txt_qv_bias[0]), txt_qv_bias[1]])
    made = (
        jnp.einsum("rd,jdw->rjw", normed1_all, txt_qkv, preferred_element_type=jnp.float32)
        + bias_rows
    )
    triple = made.astype(jnp.bfloat16).reshape(group_caps, L, 3, head_count, HEAD)
    queries = triple[:, :, 0]
    keys_all = triple[:, :, 1]
    values_all = triple[:, :, 2]
    shares, log_totals = attention_shares(queries, keys_all, keep)
    context = jnp.einsum(
        "nhqk,nkhe->nqhe",
        shares.astype(jnp.bfloat16),
        values_all,
        preferred_element_type=jnp.float32,
    )
    context = context.astype(jnp.bfloat16).reshape(group_rows, width)
    middle = inputs + (
        lax.psum(
            jnp.dot(context, txt_out, preferred_element_type=jnp.float32).astype(jnp.bfloat16),
            "mp",
        ).astype(jnp.float32)
        + txt_biases[0]
    )
    unit2, inverse2 = layer_stats(middle)
    normed2_all = (unit2 * txt_gains[1] + txt_shifts[1]).astype(jnp.bfloat16)
    hidden = jnp.dot(normed2_all, txt_fc1, preferred_element_type=jnp.float32) + txt_fc1_bias
    active, gelu_pull = jax.vjp(gelu_exact, hidden)
    active16 = active.astype(jnp.bfloat16)
    ffn_part = jnp.dot(active16, txt_fc2, preferred_element_type=jnp.float32)
    ffn_pooled = jnp.sum(ffn_part.reshape(group_caps, L, D) * present[:, :, None], 1)
    image_slots = lax.dynamic_update_slice_in_dim(
        jnp.zeros((group_caps, D), jnp.float32),
        images16.astype(jnp.float32),
        mp_index * own_caps,
        0,
    )
    both = sum_exchanged(jnp.concatenate([ffn_pooled, image_slots], 0), "mp")
    mid_pooled = jnp.sum(middle.reshape(group_caps, L, D) * present[:, :, None], 1)
    pooled = (mid_pooled + both[:group_caps]) / counts + txt_biases[1]
    inverse_len = lax.rsqrt(jnp.sum(pooled * pooled, -1, keepdims=True) + EPS)
    captions_unit = pooled * inverse_len
    captions16 = captions_unit.astype(jnp.bfloat16)
    gathered = gather_ordered(
        jnp.concatenate([captions16, both[group_caps:].astype(jnp.bfloat16)], 0), "dp"
    )
    arrived = gathered[:, :group_caps].reshape(-1, D)
    images_all = gathered[:, group_caps:].reshape(-1, D)
    total_pairs = pairing.shape[0]
    first_pair = lax.axis_index("dp") * group_caps
    logits = SCALE * jnp.einsum("id,jd->ij", images_all, arrived, preferred_element_type=jnp.float32)
    matched = (pairing[:, None] == jnp.arange(total_pairs)[None, :]).astype(jnp.float32)
    raised = jnp.exp(logits - SCALE)
    row_lse = SCALE + jnp.log(jnp.sum(raised, 1))
    col_lse = SCALE + jnp.log(jnp.sum(raised, 0))
    total = 0.5 * jnp.sum(row_lse) + 0.5 * jnp.sum(col_lse) - jnp.sum(matched * logits)
    loss = total / total_pairs
    own_logits = lax.dynamic_slice_in_dim(logits, first_pair, group_caps, 1)
    own_col_lse = lax.dynamic_slice_in_dim(col_lse, first_pair, group_caps, 0)
    own_matched = lax.dynamic_slice_in_dim(matched, first_pair, group_caps, 1)
    grads16 = (
        LOSS_SCALE
        * (
            0.5 * jnp.exp(own_logits - row_lse[:, None])
            + 0.5 * jnp.exp(own_logits - own_col_lse[None, :])
            - own_matched
        )
    ).astype(jnp.bfloat16)
    grad_caps = SCALE * jnp.einsum(
        "ic,id->cd", grads16, images_all, preferred_element_type=jnp.float32
    )
    grad_pooled = inverse_len * (
        grad_caps - captions_unit * jnp.sum(captions_unit * grad_caps, -1, keepdims=True)
    )
    grad_result = (grad_pooled[:, None, :] * (present / counts)[:, :, None]).reshape(group_rows, D)
    grad_all = grad_result.astype(jnp.bfloat16)
    grad_fc2 = jnp.einsum("gf,gd->fd", active16, grad_all, preferred_element_type=jnp.float32)
    grad_active = jnp.einsum("gd,fd->gf", grad_all, txt_fc2, preferred_element_type=jnp.float32)
    grad_hidden16 = gelu_pull(grad_active)[0].astype(jnp.bfloat16)
    grad_fc1 = jnp.einsum(
        "gd,gf->df", normed2_all, grad_hidden16, preferred_element_type=jnp.float32
    )
    grad_fc1_bias = jnp.sum(grad_hidden16.astype(jnp.float32), 0)
    fc_sums = reduce_exchanged(jnp.concatenate([grad_fc1, grad_fc2], 0), "dp")
    grad_normed2 = reduce_exchanged(
        jnp.einsum("gf,df->gd", grad_hidden16, txt_fc1, preferred_element_type=jnp.float32), "mp"
    ).astype(jnp.float32)
    grad_middle = grad_result + norm_back(grad_normed2, unit2, inverse2, txt_gains[1])
    grad_mid_all = grad_middle.astype(jnp.bfloat16)
    grad_out = jnp.einsum("gw,gd->wd", context, grad_mid_all, preferred_element_type=jnp.float32)
    grad_context = jnp.einsum(
        "gd,wd->gw", grad_mid_all, txt_out, preferred_element_type=jnp.float32
    )
    grad_context = grad_context.astype(jnp.bfloat16).reshape(group_caps, L, head_count, HEAD)
    shares_again = jnp.exp(score_rows(queries, keys_all, keep) - log_totals)
    grad_shares = jnp.einsum(
        "nqhe,nkhe->nhqk", grad_context, values_all, preferred_element_type=jnp.float32
    )
    grad_values = jnp.einsum(
        "nhqk,nqhe->nkhe",
        shares_again.astype(jnp.bfloat16),
        grad_context,
        preferred_element_type=jnp.float32,
    ).astype(jnp.bfloat16)
    grad_scores = (
        shares_again * (grad_shares - jnp.sum(grad_shares * shares_again, -1, keepdims=True))
    ).astype(jnp.bfloat16)
    grad_queries = (
        jnp.einsum("nhqk,nkhe->nqhe", grad_scores, keys_all, preferred_element_type=jnp.float32)
        * 0.125
    ).astype(jnp.bfloat16)
    grad_keys = (
        jnp.einsum("nhqk,nqhe->nkhe", grad_scores, queries, preferred_element_type=jnp.float32)
        * 0.125
    ).astype(jnp.bfloat16)
    grad_triple = jnp.stack([grad_queries, grad_keys, grad_values], 0).reshape(3, group_rows, width)
    grad_qkv = jnp.einsum(
        "gd,jgw->jdw", normed1_all, grad_triple, preferred_element_type=jnp.float32
    )
    grad_qv_bias = jnp.stack(
        [
            jnp.sum(grad_triple[0].astype(jnp.float32), 0),
            jnp.sum(grad_triple[2].astype(jnp.float32), 0),
        ]
    )
    attn_sums = reduce_exchanged(jnp.concatenate([grad_qkv.reshape(-1, D), grad_out], 0), "dp")
    grad_normed1 = scatter_exchanged(
        jnp.einsum("jgw,jdw->gd", grad_triple, txt_qkv, preferred_element_type=jnp.float32), "mp"
    )

    def own(values):
        return lax.dynamic_slice_in_dim(values, mp_index * own_rows, own_rows, 0)

    unit1_own = own(unit1)
    grad_normed2_own = own(grad_normed2)
    unit2_own = own(unit2)
    grad_middle_own = own(grad_middle)
    grad_inputs = grad_middle_own + norm_back(grad_normed1, unit1_own, own(inverse1), txt_gains[0])
    small_parts = jnp.stack(
        [
            jnp.sum(grad_normed1 * unit1_own, 0),
            jnp.sum(grad_normed2_own * unit2_own, 0),
            jnp.sum(grad_normed1, 0),
            jnp.sum(grad_normed2_own, 0),
            jnp.sum(grad_middle_own, 0),
            jnp.sum(own(grad_result), 0),
        ]
    )
    bias_rows = jnp.stack(
        [jnp.concatenate([grad_qv_bias.reshape(-1), jnp.zeros_like(grad_qv_bias.reshape(-1))]), grad_fc1_bias]
    )
    shared = sum_exchanged(jnp.concatenate([sum_exchanged(small_parts, "mp"), bias_rows], 0), "dp")
    qv_count = grad_qv_bias.size
    fc1_rows = grad_fc1.shape[0]
    return (
        loss,
        grad_inputs,
        attn_sums[: grad_qkv.size // D].astype(jnp.float32).reshape(grad_qkv.shape),
        shared[6, :qv_count].reshape(grad_qv_bias.shape),
        attn_sums[grad_qkv.size // D :].astype(jnp.float32),
        fc_sums[:fc1_rows].astype(jnp.float32),
        shared[7],
        fc_sums[fc1_rows:].astype(jnp.float32),
        shared[0:2],
        shared[2:4],
        shared[4:6],
    )


def solution(mesh):
    placed = (
        P(("dp", "mp"), None),
        P("dp", None),
        P(),
        P(("dp", "mp"), None),
        P(("dp", "mp"), None),
        P(),
        P(None, None, "mp"),
        P("mp", None),
        P(None, "mp"),
        P("mp", None),
        P(None, None, "mp"),
        P(None, "mp"),
        P("mp", None),
        P(None, "mp"),
        P("mp"),
        P("mp", None),
        P(),
        P(),
        P(),
    )
    return jax.shard_map(
        local_body,
        mesh=mesh,
        in_specs=placed,
        out_specs=(
            P(),
            P(("dp", "mp"), None),
            P(None, None, "mp"),
            P(None, "mp"),
            P("mp", None),
            P(None, "mp"),
            P("mp"),
            P("mp", None),
            P(),
            P(),
            P(),
        ),
        check_vma=False,
    )
```

```python
import jax
import jax.numpy as jnp
from jax import lax
from jax.sharding import PartitionSpec as P

D = 768
HEAD = 64
L = 16
P_LOW = 50
P_HIGH = 145


EPS = 1e-06
SCALE = 40.0
LOSS_SCALE = 16.0
MASKED = -1e30


def layer_stats(values):
    center = values - jnp.mean(values, -1, keepdims=True)
    inverse = lax.rsqrt(jnp.mean(center * center, -1, keepdims=True) + EPS)
    return (center * inverse, inverse)


def norm_back(grad_out, unit, inverse, gain):
    scaled = grad_out * gain
    return inverse * (
        scaled
        - jnp.mean(scaled, -1, keepdims=True)
        - unit * jnp.mean(scaled * unit, -1, keepdims=True)
    )


def gelu_exact(values):
    return jax.nn.gelu(values, approximate=False)


def score_rows(queries, keys_all, keep):
    scores = (
        jnp.einsum("nqhe,nkhe->nhqk", queries, keys_all, preferred_element_type=jnp.float32) * 0.125
    )
    if keep is not None:
        scores = jnp.where(keep, scores, MASKED)
    return scores


def attention_shares(queries, keys_all, keep):
    scores = score_rows(queries, keys_all, keep)
    highest = jnp.max(scores, -1, keepdims=True)
    raised = jnp.exp(scores - highest)
    totals = jnp.sum(raised, -1, keepdims=True)
    return (raised / totals, highest + jnp.log(totals))


def axis_bits(axis):
    count = lax.axis_size(axis)
    bits = count.bit_length() - 1
    assert 1 << bits == count
    return count, list(reversed(range(bits)))


def exchange(values, axis, count, bit):
    return lax.ppermute(values, axis, [(i, i ^ (1 << bit)) for i in range(count)])


def gather_stacked(values, axis):
    count, bits = axis_bits(axis)
    data = values[None]
    for bit in bits:
        data = jnp.concatenate([data, exchange(data, axis, count, bit)], 0)
    return data


def gather_ordered(values, axis):
    count, bits = axis_bits(axis)
    index = lax.axis_index(axis)
    data = values
    done = []
    for bit in bits:
        other = exchange(data, axis, count, bit)
        upper = ((index >> bit) & 1) == 1
        data = jnp.stack([jnp.where(upper, other, data), jnp.where(upper, data, other)], 0)
        done.insert(0, bit)
    order = sorted(range(len(done)), key=lambda a: -done[a])
    data = data.transpose(order + list(range(len(done), data.ndim)))
    return data.reshape((count,) + values.shape)


def sum_exchanged(values, axis):
    count, bits = axis_bits(axis)
    for bit in reversed(bits):
        values = values + exchange(values, axis, count, bit)
    return values


def scatter_exchanged(values, axis):
    count, bits = axis_bits(axis)
    index = lax.axis_index(axis)
    data = values.reshape((2,) * len(bits) + (values.shape[0] // count,) + values.shape[1:])
    for bit in reversed(bits):
        place = len(bits) - 1 - bit
        mine = (index >> bit) & 1
        kept = lax.dynamic_index_in_dim(data, mine, place, keepdims=False)
        sent = lax.dynamic_index_in_dim(data, 1 - mine, place, keepdims=False)
        data = kept + exchange(sent.astype(jnp.bfloat16), axis, count, bit).astype(jnp.float32)
    return data


def reduce_exchanged(values, axis):
    part = scatter_exchanged(values, axis).astype(jnp.bfloat16)
    return gather_ordered(part, axis).reshape(values.shape)


def image_tower(tokens, count, length, gains, weights):
    w_qkv, w_out, w_fc1, w_fc2 = weights
    _, middle = image_attention(tokens, count, length, gains, w_qkv, w_out)
    return image_ffn(middle, count, length, gains, w_fc1, w_fc2)


def image_attention(tokens, count, length, gains, w_qkv, w_out):
    head_count = D // HEAD
    inputs = tokens.astype(jnp.float32)
    unit, _ = layer_stats(inputs)
    normed = (unit * gains[0]).astype(jnp.bfloat16)
    projected = jnp.einsum("rd,jdw->jrw", normed, w_qkv, preferred_element_type=jnp.float32).astype(
        jnp.bfloat16
    )
    shaped = projected.reshape(3, count, length, head_count, HEAD)
    shares, _ = attention_shares(shaped[0], shaped[1], None)
    context = jnp.einsum(
        "nhqk,nkhe->nqhe",
        shares.astype(jnp.bfloat16),
        shaped[2],
        preferred_element_type=jnp.float32,
    )
    context = context.astype(jnp.bfloat16).reshape(count * length, D)
    middle = inputs + jnp.dot(context, w_out, preferred_element_type=jnp.float32)
    return inputs, middle


def image_ffn(middle, count, length, gains, w_fc1, w_fc2):
    unit2, _ = layer_stats(middle)
    normed2 = (unit2 * gains[1]).astype(jnp.bfloat16)
    active = gelu_exact(jnp.dot(normed2, w_fc1, preferred_element_type=jnp.float32)).astype(
        jnp.bfloat16
    )
    result = middle + jnp.dot(active, w_fc2, preferred_element_type=jnp.float32)
    pooled = jnp.mean(result.reshape(count, length, D), 1)
    return (pooled * lax.rsqrt(jnp.sum(pooled * pooled, -1, keepdims=True) + EPS)).astype(
        jnp.bfloat16
    )


def local_body(
    text_in,
    caption_ids,
    pairing,
    image_low,
    image_high,
    img_gains,
    img_qkv,
    img_out,
    img_fc1,
    img_fc2,
    txt_qkv,
    txt_qv_bias,
    txt_out,
    txt_fc1,
    txt_fc1_bias,
    txt_fc2,
    txt_gains,
    txt_shifts,
    txt_biases,
):
    qkv_parts = gather_stacked(img_qkv, "mp")
    fc1_parts = gather_stacked(img_fc1, "mp")
    weights = (
        qkv_parts.transpose(1, 2, 0, 3).reshape(3, D, -1),
        gather_stacked(img_out, "mp").reshape(-1, D),
        fc1_parts.transpose(1, 0, 2).reshape(D, -1),
        gather_stacked(img_fc2, "mp").reshape(-1, D),
    )
    low_count = image_low.shape[0] // P_LOW
    high_count = image_high.shape[0] // P_HIGH
    images16 = jnp.concatenate(
        [
            image_tower(image_low, low_count, P_LOW, img_gains, weights),
            image_tower(image_high, high_count, P_HIGH, img_gains, weights),
        ],
        0,
    )
    width = txt_qkv.shape[2]
    head_count = width // HEAD
    own_rows = text_in.shape[0]
    own_caps = own_rows // L
    group_caps = caption_ids.shape[0]
    group_rows = group_caps * L
    mp_index = lax.axis_index("mp")
    present = (caption_ids > 0).astype(jnp.float32)
    keep = (caption_ids > 0)[:, None, None, :]
    counts = jnp.sum(present, 1, keepdims=True)
    inputs = lax.all_gather(text_in, "mp", axis=0, tiled=True).astype(jnp.float32)
    unit1, inverse1 = layer_stats(inputs)
    normed1_all = (unit1 * txt_gains[0] + txt_shifts[0]).astype(jnp.bfloat16)
    bias_rows = jnp.stack([txt_qv_bias[0], jnp.zeros_like(txt_qv_bias[0]), txt_qv_bias[1]])
    made = (
        jnp.einsum("rd,jdw->rjw", normed1_all, txt_qkv, preferred_element_type=jnp.float32)
        + bias_rows
    )
    triple = made.astype(jnp.bfloat16).reshape(group_caps, L, 3, head_count, HEAD)
    queries = triple[:, :, 0]
    keys_all = triple[:, :, 1]
    values_all = triple[:, :, 2]
    shares, log_totals = attention_shares(queries, keys_all, keep)
    context = jnp.einsum(
        "nhqk,nkhe->nqhe",
        shares.astype(jnp.bfloat16),
        values_all,
        preferred_element_type=jnp.float32,
    )
    context = context.astype(jnp.bfloat16).reshape(group_rows, width)
    middle = inputs + (
        lax.psum(
            jnp.dot(context, txt_out, preferred_element_type=jnp.float32).astype(jnp.bfloat16),
            "mp",
        ).astype(jnp.float32)
        + txt_biases[0]
    )
    unit2, inverse2 = layer_stats(middle)
    normed2_all = (unit2 * txt_gains[1] + txt_shifts[1]).astype(jnp.bfloat16)
    hidden = jnp.dot(normed2_all, txt_fc1, preferred_element_type=jnp.float32) + txt_fc1_bias
    active, gelu_pull = jax.vjp(gelu_exact, hidden)
    active16 = active.astype(jnp.bfloat16)
    ffn_part = jnp.dot(active16, txt_fc2, preferred_element_type=jnp.float32)
    ffn_pooled = jnp.sum(ffn_part.reshape(group_caps, L, D) * present[:, :, None], 1)
    image_slots = lax.dynamic_update_slice_in_dim(
        jnp.zeros((group_caps, D), jnp.float32),
        images16.astype(jnp.float32),
        mp_index * own_caps,
        0,
    )
    both = sum_exchanged(jnp.concatenate([ffn_pooled, image_slots], 0), "mp")
    mid_pooled = jnp.sum(middle.reshape(group_caps, L, D) * present[:, :, None], 1)
    pooled = (mid_pooled + both[:group_caps]) / counts + txt_biases[1]
    inverse_len = lax.rsqrt(jnp.sum(pooled * pooled, -1, keepdims=True) + EPS)
    captions_unit = pooled * inverse_len
    captions16 = captions_unit.astype(jnp.bfloat16)
    gathered = gather_ordered(
        jnp.concatenate([captions16, both[group_caps:].astype(jnp.bfloat16)], 0), "dp"
    )
    arrived = gathered[:, :group_caps].reshape(-1, D)
    images_all = gathered[:, group_caps:].reshape(-1, D)
    total_pairs = pairing.shape[0]
    first_pair = lax.axis_index("dp") * group_caps
    logits = SCALE * jnp.einsum("id,jd->ij", images_all, arrived, preferred_element_type=jnp.float32)
    matched = (pairing[:, None] == jnp.arange(total_pairs)[None, :]).astype(jnp.float32)
    raised = jnp.exp(logits - SCALE)
    row_lse = SCALE + jnp.log(jnp.sum(raised, 1))
    col_lse = SCALE + jnp.log(jnp.sum(raised, 0))
    total = 0.5 * jnp.sum(row_lse) + 0.5 * jnp.sum(col_lse) - jnp.sum(matched * logits)
    loss = total / total_pairs
    own_logits = lax.dynamic_slice_in_dim(logits, first_pair, group_caps, 1)
    own_col_lse = lax.dynamic_slice_in_dim(col_lse, first_pair, group_caps, 0)
    own_matched = lax.dynamic_slice_in_dim(matched, first_pair, group_caps, 1)
    grads16 = (
        LOSS_SCALE
        * (
            0.5 * jnp.exp(own_logits - row_lse[:, None])
            + 0.5 * jnp.exp(own_logits - own_col_lse[None, :])
            - own_matched
        )
    ).astype(jnp.bfloat16)
    grad_caps = SCALE * jnp.einsum(
        "ic,id->cd", grads16, images_all, preferred_element_type=jnp.float32
    )
    grad_pooled = inverse_len * (
        grad_caps - captions_unit * jnp.sum(captions_unit * grad_caps, -1, keepdims=True)
    )
    grad_result = (grad_pooled[:, None, :] * (present / counts)[:, :, None]).reshape(group_rows, D)
    grad_all = grad_result.astype(jnp.bfloat16)
    grad_fc2 = jnp.einsum("gf,gd->fd", active16, grad_all, preferred_element_type=jnp.float32)
    grad_active = jnp.einsum("gd,fd->gf", grad_all, txt_fc2, preferred_element_type=jnp.float32)
    grad_hidden16 = gelu_pull(grad_active)[0].astype(jnp.bfloat16)
    grad_fc1 = jnp.einsum(
        "gd,gf->df", normed2_all, grad_hidden16, preferred_element_type=jnp.float32
    )
    grad_fc1_bias = jnp.sum(grad_hidden16.astype(jnp.float32), 0)
    fc_sums = lax.psum(jnp.concatenate([grad_fc1, grad_fc2], 0).astype(jnp.bfloat16), "dp")
    grad_normed2 = reduce_exchanged(
        jnp.einsum("gf,df->gd", grad_hidden16, txt_fc1, preferred_element_type=jnp.float32), "mp"
    ).astype(jnp.float32)
    grad_middle = grad_result + norm_back(grad_normed2, unit2, inverse2, txt_gains[1])
    grad_mid_all = grad_middle.astype(jnp.bfloat16)
    grad_out = jnp.einsum("gw,gd->wd", context, grad_mid_all, preferred_element_type=jnp.float32)
    grad_context = jnp.einsum(
        "gd,wd->gw", grad_mid_all, txt_out, preferred_element_type=jnp.float32
    )
    grad_context = grad_context.astype(jnp.bfloat16).reshape(group_caps, L, head_count, HEAD)
    shares_again = jnp.exp(score_rows(queries, keys_all, keep) - log_totals)
    grad_shares = jnp.einsum(
        "nqhe,nkhe->nhqk", grad_context, values_all, preferred_element_type=jnp.float32
    )
    grad_values = jnp.einsum(
        "nhqk,nqhe->nkhe",
        shares_again.astype(jnp.bfloat16),
        grad_context,
        preferred_element_type=jnp.float32,
    ).astype(jnp.bfloat16)
    grad_scores = (
        shares_again * (grad_shares - jnp.sum(grad_shares * shares_again, -1, keepdims=True))
    ).astype(jnp.bfloat16)
    grad_queries = (
        jnp.einsum("nhqk,nkhe->nqhe", grad_scores, keys_all, preferred_element_type=jnp.float32)
        * 0.125
    ).astype(jnp.bfloat16)
    grad_keys = (
        jnp.einsum("nhqk,nqhe->nkhe", grad_scores, queries, preferred_element_type=jnp.float32)
        * 0.125
    ).astype(jnp.bfloat16)
    grad_triple = jnp.stack([grad_queries, grad_keys, grad_values], 0).reshape(3, group_rows, width)
    grad_qkv = jnp.einsum(
        "gd,jgw->jdw", normed1_all, grad_triple, preferred_element_type=jnp.float32
    )
    grad_qv_bias = jnp.stack(
        [
            jnp.sum(grad_triple[0].astype(jnp.float32), 0),
            jnp.sum(grad_triple[2].astype(jnp.float32), 0),
        ]
    )
    attn_sums = reduce_exchanged(jnp.concatenate([grad_qkv.reshape(-1, D), grad_out], 0), "dp")
    grad_normed1 = scatter_exchanged(
        jnp.einsum("jgw,jdw->gd", grad_triple, txt_qkv, preferred_element_type=jnp.float32), "mp"
    )

    def own(values):
        return lax.dynamic_slice_in_dim(values, mp_index * own_rows, own_rows, 0)

    unit1_own = own(unit1)
    grad_normed2_own = own(grad_normed2)
    unit2_own = own(unit2)
    grad_middle_own = own(grad_middle)
    grad_inputs = grad_middle_own + norm_back(grad_normed1, unit1_own, own(inverse1), txt_gains[0])
    small_parts = jnp.stack(
        [
            jnp.sum(grad_normed1 * unit1_own, 0),
            jnp.sum(grad_normed2_own * unit2_own, 0),
            jnp.sum(grad_normed1, 0),
            jnp.sum(grad_normed2_own, 0),
            jnp.sum(grad_middle_own, 0),
            jnp.sum(own(grad_result), 0),
        ]
    )
    bias_rows = jnp.stack(
        [jnp.concatenate([grad_qv_bias.reshape(-1), jnp.zeros_like(grad_qv_bias.reshape(-1))]), grad_fc1_bias]
    )
    shared = sum_exchanged(jnp.concatenate([sum_exchanged(small_parts, "mp"), bias_rows], 0), "dp")
    qv_count = grad_qv_bias.size
    fc1_rows = grad_fc1.shape[0]
    return (
        loss,
        grad_inputs,
        attn_sums[: grad_qkv.size // D].astype(jnp.float32).reshape(grad_qkv.shape),
        shared[6, :qv_count].reshape(grad_qv_bias.shape),
        attn_sums[grad_qkv.size // D :].astype(jnp.float32),
        fc_sums[:fc1_rows].astype(jnp.float32),
        shared[7],
        fc_sums[fc1_rows:].astype(jnp.float32),
        shared[0:2],
        shared[2:4],
        shared[4:6],
    )


def solution(mesh):
    placed = (
        P(("dp", "mp"), None),
        P("dp", None),
        P(),
        P(("dp", "mp"), None),
        P(("dp", "mp"), None),
        P(),
        P(None, None, "mp"),
        P("mp", None),
        P(None, "mp"),
        P("mp", None),
        P(None, None, "mp"),
        P(None, "mp"),
        P("mp", None),
        P(None, "mp"),
        P("mp"),
        P("mp", None),
        P(),
        P(),
        P(),
    )
    return jax.shard_map(
        local_body,
        mesh=mesh,
        in_specs=placed,
        out_specs=(
            P(),
            P(("dp", "mp"), None),
            P(None, None, "mp"),
            P(None, "mp"),
            P("mp", None),
            P(None, "mp"),
            P("mp"),
            P("mp", None),
            P(),
            P(),
            P(),
        ),
        check_vma=False,
    )
```

```python
import jax
import jax.numpy as jnp
from jax import lax
from jax.sharding import PartitionSpec as P

D = 768
HEAD = 64
L = 16
P_LOW = 50
P_HIGH = 145


EPS = 1e-06
SCALE = 40.0
LOSS_SCALE = 16.0
MASKED = -1e30


def layer_stats(values):
    center = values - jnp.mean(values, -1, keepdims=True)
    inverse = lax.rsqrt(jnp.mean(center * center, -1, keepdims=True) + EPS)
    return (center * inverse, inverse)


def norm_back(grad_out, unit, inverse, gain):
    scaled = grad_out * gain
    return inverse * (
        scaled
        - jnp.mean(scaled, -1, keepdims=True)
        - unit * jnp.mean(scaled * unit, -1, keepdims=True)
    )


def gelu_exact(values):
    return jax.nn.gelu(values, approximate=False)


def score_rows(queries, keys_all, keep):
    scores = (
        jnp.einsum("nqhe,nkhe->nhqk", queries, keys_all, preferred_element_type=jnp.float32) * 0.125
    )
    if keep is not None:
        scores = jnp.where(keep, scores, MASKED)
    return scores


def attention_shares(queries, keys_all, keep):
    scores = score_rows(queries, keys_all, keep)
    highest = jnp.max(scores, -1, keepdims=True)
    raised = jnp.exp(scores - highest)
    totals = jnp.sum(raised, -1, keepdims=True)
    return (raised / totals, highest + jnp.log(totals))


def axis_bits(axis):
    count = lax.axis_size(axis)
    bits = count.bit_length() - 1
    assert 1 << bits == count
    return count, list(reversed(range(bits)))


def exchange(values, axis, count, bit):
    return lax.ppermute(values, axis, [(i, i ^ (1 << bit)) for i in range(count)])


def gather_stacked(values, axis):
    count, bits = axis_bits(axis)
    data = values[None]
    for bit in bits:
        data = jnp.concatenate([data, exchange(data, axis, count, bit)], 0)
    return data


def gather_ordered(values, axis):
    count, bits = axis_bits(axis)
    index = lax.axis_index(axis)
    data = values
    done = []
    for bit in bits:
        other = exchange(data, axis, count, bit)
        upper = ((index >> bit) & 1) == 1
        data = jnp.stack([jnp.where(upper, other, data), jnp.where(upper, data, other)], 0)
        done.insert(0, bit)
    order = sorted(range(len(done)), key=lambda a: -done[a])
    data = data.transpose(order + list(range(len(done), data.ndim)))
    return data.reshape((count,) + values.shape)


def sum_exchanged(values, axis):
    count, bits = axis_bits(axis)
    for bit in reversed(bits):
        values = values + exchange(values, axis, count, bit)
    return values


def scatter_exchanged(values, axis):
    count, bits = axis_bits(axis)
    index = lax.axis_index(axis)
    data = values.reshape((2,) * len(bits) + (values.shape[0] // count,) + values.shape[1:])
    for bit in reversed(bits):
        place = len(bits) - 1 - bit
        mine = (index >> bit) & 1
        kept = lax.dynamic_index_in_dim(data, mine, place, keepdims=False)
        sent = lax.dynamic_index_in_dim(data, 1 - mine, place, keepdims=False)
        data = kept + exchange(sent.astype(jnp.bfloat16), axis, count, bit).astype(jnp.float32)
    return data


def reduce_exchanged(values, axis):
    part = scatter_exchanged(values, axis).astype(jnp.bfloat16)
    return gather_ordered(part, axis).reshape(values.shape)


def image_tower(tokens, count, length, gains, weights):
    w_qkv, w_out, w_fc1, w_fc2 = weights
    _, middle = image_attention(tokens, count, length, gains, w_qkv, w_out)
    return image_ffn(middle, count, length, gains, w_fc1, w_fc2)


def image_attention(tokens, count, length, gains, w_qkv, w_out):
    head_count = D // HEAD
    inputs = tokens.astype(jnp.float32)
    unit, _ = layer_stats(inputs)
    normed = (unit * gains[0]).astype(jnp.bfloat16)
    projected = jnp.einsum("rd,jdw->jrw", normed, w_qkv, preferred_element_type=jnp.float32).astype(
        jnp.bfloat16
    )
    shaped = projected.reshape(3, count, length, head_count, HEAD)
    shares, _ = attention_shares(shaped[0], shaped[1], None)
    context = jnp.einsum(
        "nhqk,nkhe->nqhe",
        shares.astype(jnp.bfloat16),
        shaped[2],
        preferred_element_type=jnp.float32,
    )
    context = context.astype(jnp.bfloat16).reshape(count * length, D)
    middle = inputs + jnp.dot(context, w_out, preferred_element_type=jnp.float32)
    return inputs, middle


def image_ffn(middle, count, length, gains, w_fc1, w_fc2):
    unit2, _ = layer_stats(middle)
    normed2 = (unit2 * gains[1]).astype(jnp.bfloat16)
    active = gelu_exact(jnp.dot(normed2, w_fc1, preferred_element_type=jnp.float32)).astype(
        jnp.bfloat16
    )
    pool = (
        lax.broadcasted_iota(jnp.int32, (count, count * length), 1) // length
        == lax.broadcasted_iota(jnp.int32, (count, count * length), 0)
    ).astype(jnp.bfloat16)
    mean_active = jnp.dot(pool, active, preferred_element_type=jnp.float32) / length
    pooled = jnp.mean(middle.reshape(count, length, D), 1) + jnp.dot(
        mean_active, w_fc2.astype(jnp.float32), precision=lax.Precision.HIGHEST
    )
    return (pooled * lax.rsqrt(jnp.sum(pooled * pooled, -1, keepdims=True) + EPS)).astype(
        jnp.bfloat16
    )


def local_body(
    text_in,
    caption_ids,
    pairing,
    image_low,
    image_high,
    img_gains,
    img_qkv,
    img_out,
    img_fc1,
    img_fc2,
    txt_qkv,
    txt_qv_bias,
    txt_out,
    txt_fc1,
    txt_fc1_bias,
    txt_fc2,
    txt_gains,
    txt_shifts,
    txt_biases,
):
    qkv_parts = gather_stacked(img_qkv, "mp")
    fc1_parts = gather_stacked(img_fc1, "mp")
    weights = (
        qkv_parts.transpose(1, 2, 0, 3).reshape(3, D, -1),
        gather_stacked(img_out, "mp").reshape(-1, D),
        fc1_parts.transpose(1, 0, 2).reshape(D, -1),
        gather_stacked(img_fc2, "mp").reshape(-1, D),
    )
    low_count = image_low.shape[0] // P_LOW
    high_count = image_high.shape[0] // P_HIGH
    images16 = jnp.concatenate(
        [
            image_tower(image_low, low_count, P_LOW, img_gains, weights),
            image_tower(image_high, high_count, P_HIGH, img_gains, weights),
        ],
        0,
    )
    width = txt_qkv.shape[2]
    head_count = width // HEAD
    own_rows = text_in.shape[0]
    own_caps = own_rows // L
    group_caps = caption_ids.shape[0]
    group_rows = group_caps * L
    mp_index = lax.axis_index("mp")
    present = (caption_ids > 0).astype(jnp.float32)
    keep = (caption_ids > 0)[:, None, None, :]
    counts = jnp.sum(present, 1, keepdims=True)
    inputs = lax.all_gather(text_in, "mp", axis=0, tiled=True).astype(jnp.float32)
    unit1, inverse1 = layer_stats(inputs)
    normed1_all = (unit1 * txt_gains[0] + txt_shifts[0]).astype(jnp.bfloat16)
    bias_rows = jnp.stack([txt_qv_bias[0], jnp.zeros_like(txt_qv_bias[0]), txt_qv_bias[1]])
    made = (
        jnp.einsum("rd,jdw->rjw", normed1_all, txt_qkv, preferred_element_type=jnp.float32)
        + bias_rows
    )
    triple = made.astype(jnp.bfloat16).reshape(group_caps, L, 3, head_count, HEAD)
    queries = triple[:, :, 0]
    keys_all = triple[:, :, 1]
    values_all = triple[:, :, 2]
    shares, log_totals = attention_shares(queries, keys_all, keep)
    context = jnp.einsum(
        "nhqk,nkhe->nqhe",
        shares.astype(jnp.bfloat16),
        values_all,
        preferred_element_type=jnp.float32,
    )
    context = context.astype(jnp.bfloat16).reshape(group_rows, width)
    middle = inputs + (
        lax.psum(
            jnp.dot(context, txt_out, preferred_element_type=jnp.float32).astype(jnp.bfloat16),
            "mp",
        ).astype(jnp.float32)
        + txt_biases[0]
    )
    unit2, inverse2 = layer_stats(middle)
    normed2_all = (unit2 * txt_gains[1] + txt_shifts[1]).astype(jnp.bfloat16)
    hidden = jnp.dot(normed2_all, txt_fc1, preferred_element_type=jnp.float32) + txt_fc1_bias
    active, gelu_pull = jax.vjp(gelu_exact, hidden)
    active16 = active.astype(jnp.bfloat16)
    ffn_part = jnp.dot(active16, txt_fc2, preferred_element_type=jnp.float32)
    ffn_pooled = jnp.sum(ffn_part.reshape(group_caps, L, D) * present[:, :, None], 1)
    image_slots = lax.dynamic_update_slice_in_dim(
        jnp.zeros((group_caps, D), jnp.float32),
        images16.astype(jnp.float32),
        mp_index * own_caps,
        0,
    )
    both = sum_exchanged(jnp.concatenate([ffn_pooled, image_slots], 0), "mp")
    mid_pooled = jnp.sum(middle.reshape(group_caps, L, D) * present[:, :, None], 1)
    pooled = (mid_pooled + both[:group_caps]) / counts + txt_biases[1]
    inverse_len = lax.rsqrt(jnp.sum(pooled * pooled, -1, keepdims=True) + EPS)
    captions_unit = pooled * inverse_len
    captions16 = captions_unit.astype(jnp.bfloat16)
    gathered = gather_ordered(
        jnp.concatenate([captions16, both[group_caps:].astype(jnp.bfloat16)], 0), "dp"
    )
    arrived = gathered[:, :group_caps].reshape(-1, D)
    images_all = gathered[:, group_caps:].reshape(-1, D)
    total_pairs = pairing.shape[0]
    first_pair = lax.axis_index("dp") * group_caps
    logits = SCALE * jnp.einsum("id,jd->ij", images_all, arrived, preferred_element_type=jnp.float32)
    matched = (pairing[:, None] == jnp.arange(total_pairs)[None, :]).astype(jnp.float32)
    raised = jnp.exp(logits - SCALE)
    row_lse = SCALE + jnp.log(jnp.sum(raised, 1))
    col_lse = SCALE + jnp.log(jnp.sum(raised, 0))
    total = 0.5 * jnp.sum(row_lse) + 0.5 * jnp.sum(col_lse) - jnp.sum(matched * logits)
    loss = total / total_pairs
    own_logits = lax.dynamic_slice_in_dim(logits, first_pair, group_caps, 1)
    own_col_lse = lax.dynamic_slice_in_dim(col_lse, first_pair, group_caps, 0)
    own_matched = lax.dynamic_slice_in_dim(matched, first_pair, group_caps, 1)
    grads16 = (
        LOSS_SCALE
        * (
            0.5 * jnp.exp(own_logits - row_lse[:, None])
            + 0.5 * jnp.exp(own_logits - own_col_lse[None, :])
            - own_matched
        )
    ).astype(jnp.bfloat16)
    grad_caps = SCALE * jnp.einsum(
        "ic,id->cd", grads16, images_all, preferred_element_type=jnp.float32
    )
    grad_pooled = inverse_len * (
        grad_caps - captions_unit * jnp.sum(captions_unit * grad_caps, -1, keepdims=True)
    )
    grad_result = (grad_pooled[:, None, :] * (present / counts)[:, :, None]).reshape(group_rows, D)
    grad_all = grad_result.astype(jnp.bfloat16)
    grad_fc2 = jnp.einsum("gf,gd->fd", active16, grad_all, preferred_element_type=jnp.float32)
    grad_active = jnp.einsum("gd,fd->gf", grad_all, txt_fc2, preferred_element_type=jnp.float32)
    grad_hidden16 = gelu_pull(grad_active)[0].astype(jnp.bfloat16)
    grad_fc1 = jnp.einsum(
        "gd,gf->df", normed2_all, grad_hidden16, preferred_element_type=jnp.float32
    )
    grad_fc1_bias = jnp.sum(grad_hidden16.astype(jnp.float32), 0)
    fc_sums = lax.psum(jnp.concatenate([grad_fc1, grad_fc2], 0).astype(jnp.bfloat16), "dp")
    grad_normed2 = reduce_exchanged(
        jnp.einsum("gf,df->gd", grad_hidden16, txt_fc1, preferred_element_type=jnp.float32), "mp"
    ).astype(jnp.float32)
    grad_middle = grad_result + norm_back(grad_normed2, unit2, inverse2, txt_gains[1])
    grad_mid_all = grad_middle.astype(jnp.bfloat16)
    grad_out = jnp.einsum("gw,gd->wd", context, grad_mid_all, preferred_element_type=jnp.float32)
    grad_context = jnp.einsum(
        "gd,wd->gw", grad_mid_all, txt_out, preferred_element_type=jnp.float32
    )
    grad_context = grad_context.astype(jnp.bfloat16).reshape(group_caps, L, head_count, HEAD)
    shares_again = jnp.exp(score_rows(queries, keys_all, keep) - log_totals)
    grad_shares = jnp.einsum(
        "nqhe,nkhe->nhqk", grad_context, values_all, preferred_element_type=jnp.float32
    )
    grad_values = jnp.einsum(
        "nhqk,nqhe->nkhe",
        shares_again.astype(jnp.bfloat16),
        grad_context,
        preferred_element_type=jnp.float32,
    ).astype(jnp.bfloat16)
    grad_scores = (
        shares_again * (grad_shares - jnp.sum(grad_shares * shares_again, -1, keepdims=True))
    ).astype(jnp.bfloat16)
    grad_queries = (
        jnp.einsum("nhqk,nkhe->nqhe", grad_scores, keys_all, preferred_element_type=jnp.float32)
        * 0.125
    ).astype(jnp.bfloat16)
    grad_keys = (
        jnp.einsum("nhqk,nqhe->nkhe", grad_scores, queries, preferred_element_type=jnp.float32)
        * 0.125
    ).astype(jnp.bfloat16)
    grad_triple = jnp.stack([grad_queries, grad_keys, grad_values], 0).reshape(3, group_rows, width)
    grad_qkv = jnp.einsum(
        "gd,jgw->jdw", normed1_all, grad_triple, preferred_element_type=jnp.float32
    )
    grad_qv_bias = jnp.stack(
        [
            jnp.sum(grad_triple[0].astype(jnp.float32), 0),
            jnp.sum(grad_triple[2].astype(jnp.float32), 0),
        ]
    )
    attn_sums = reduce_exchanged(jnp.concatenate([grad_qkv.reshape(-1, D), grad_out], 0), "dp")
    grad_normed1 = scatter_exchanged(
        jnp.einsum("jgw,jdw->gd", grad_triple, txt_qkv, preferred_element_type=jnp.float32), "mp"
    )

    def own(values):
        return lax.dynamic_slice_in_dim(values, mp_index * own_rows, own_rows, 0)

    unit1_own = own(unit1)
    grad_normed2_own = own(grad_normed2)
    unit2_own = own(unit2)
    grad_middle_own = own(grad_middle)
    grad_inputs = grad_middle_own + norm_back(grad_normed1, unit1_own, own(inverse1), txt_gains[0])
    small_parts = jnp.stack(
        [
            jnp.sum(grad_normed1 * unit1_own, 0),
            jnp.sum(grad_normed2_own * unit2_own, 0),
            jnp.sum(grad_normed1, 0),
            jnp.sum(grad_normed2_own, 0),
            jnp.sum(grad_middle_own, 0),
            jnp.sum(own(grad_result), 0),
        ]
    )
    bias_rows = jnp.stack(
        [jnp.concatenate([grad_qv_bias.reshape(-1), jnp.zeros_like(grad_qv_bias.reshape(-1))]), grad_fc1_bias]
    )
    shared = sum_exchanged(jnp.concatenate([sum_exchanged(small_parts, "mp"), bias_rows], 0), "dp")
    qv_count = grad_qv_bias.size
    fc1_rows = grad_fc1.shape[0]
    return (
        loss,
        grad_inputs,
        attn_sums[: grad_qkv.size // D].astype(jnp.float32).reshape(grad_qkv.shape),
        shared[6, :qv_count].reshape(grad_qv_bias.shape),
        attn_sums[grad_qkv.size // D :].astype(jnp.float32),
        fc_sums[:fc1_rows].astype(jnp.float32),
        shared[7],
        fc_sums[fc1_rows:].astype(jnp.float32),
        shared[0:2],
        shared[2:4],
        shared[4:6],
    )


def solution(mesh):
    placed = (
        P(("dp", "mp"), None),
        P("dp", None),
        P(),
        P(("dp", "mp"), None),
        P(("dp", "mp"), None),
        P(),
        P(None, None, "mp"),
        P("mp", None),
        P(None, "mp"),
        P("mp", None),
        P(None, None, "mp"),
        P(None, "mp"),
        P("mp", None),
        P(None, "mp"),
        P("mp"),
        P("mp", None),
        P(),
        P(),
        P(),
    )
    return jax.shard_map(
        local_body,
        mesh=mesh,
        in_specs=placed,
        out_specs=(
            P(),
            P(("dp", "mp"), None),
            P(None, None, "mp"),
            P(None, "mp"),
            P("mp", None),
            P(None, "mp"),
            P("mp"),
            P("mp", None),
            P(),
            P(),
            P(),
        ),
        check_vma=False,
    )
```

```python
import jax
import jax.numpy as jnp
from jax import lax
from jax.sharding import PartitionSpec as P

D = 768
HEAD = 64
L = 16
P_LOW = 50
P_HIGH = 145


EPS = 1e-06
SCALE = 40.0
LOSS_SCALE = 16.0
MASKED = -1e30


def layer_stats(values):
    center = values - jnp.mean(values, -1, keepdims=True)
    inverse = lax.rsqrt(jnp.mean(center * center, -1, keepdims=True) + EPS)
    return (center * inverse, inverse)


def norm_back(grad_out, unit, inverse, gain):
    scaled = grad_out * gain
    return inverse * (
        scaled
        - jnp.mean(scaled, -1, keepdims=True)
        - unit * jnp.mean(scaled * unit, -1, keepdims=True)
    )


def gelu_exact(values):
    return jax.nn.gelu(values, approximate=False)


def score_rows(queries, keys_all, keep):
    scores = (
        jnp.einsum("nqhe,nkhe->nhqk", queries, keys_all, preferred_element_type=jnp.float32) * 0.125
    )
    if keep is not None:
        scores = jnp.where(keep, scores, MASKED)
    return scores


def attention_shares(queries, keys_all, keep):
    scores = score_rows(queries, keys_all, keep)
    highest = jnp.max(scores, -1, keepdims=True)
    raised = jnp.exp(scores - highest)
    totals = jnp.sum(raised, -1, keepdims=True)
    return (raised / totals, highest + jnp.log(totals))


def axis_bits(axis):
    count = lax.axis_size(axis)
    bits = count.bit_length() - 1
    assert 1 << bits == count
    return count, list(reversed(range(bits)))


def exchange(values, axis, count, bit):
    return lax.ppermute(values, axis, [(i, i ^ (1 << bit)) for i in range(count)])


def gather_stacked(values, axis):
    count, bits = axis_bits(axis)
    data = values[None]
    for bit in bits:
        data = jnp.concatenate([data, exchange(data, axis, count, bit)], 0)
    return data


def gather_ordered(values, axis):
    count, bits = axis_bits(axis)
    index = lax.axis_index(axis)
    data = values
    done = []
    for bit in bits:
        other = exchange(data, axis, count, bit)
        upper = ((index >> bit) & 1) == 1
        data = jnp.stack([jnp.where(upper, other, data), jnp.where(upper, data, other)], 0)
        done.insert(0, bit)
    order = sorted(range(len(done)), key=lambda a: -done[a])
    data = data.transpose(order + list(range(len(done), data.ndim)))
    return data.reshape((count,) + values.shape)


def sum_exchanged(values, axis):
    count, bits = axis_bits(axis)
    for bit in reversed(bits):
        values = values + exchange(values, axis, count, bit)
    return values


def scatter_exchanged(values, axis):
    count, bits = axis_bits(axis)
    index = lax.axis_index(axis)
    data = values.reshape((2,) * len(bits) + (values.shape[0] // count,) + values.shape[1:])
    for bit in reversed(bits):
        place = len(bits) - 1 - bit
        mine = (index >> bit) & 1
        kept = lax.dynamic_index_in_dim(data, mine, place, keepdims=False)
        sent = lax.dynamic_index_in_dim(data, 1 - mine, place, keepdims=False)
        data = kept + exchange(sent.astype(jnp.bfloat16), axis, count, bit).astype(jnp.float32)
    return data


def reduce_exchanged(values, axis):
    part = scatter_exchanged(values, axis).astype(jnp.bfloat16)
    return gather_ordered(part, axis).reshape(values.shape)


def image_tower(tokens, count, length, gains, weights):
    w_qkv, w_out, w_fc1, w_fc2 = weights
    _, middle = image_attention(tokens, count, length, gains, w_qkv, w_out)
    return image_ffn(middle, count, length, gains, w_fc1, w_fc2)


def image_attention(tokens, count, length, gains, w_qkv, w_out):
    head_count = D // HEAD
    inputs = tokens.astype(jnp.float32)
    unit, _ = layer_stats(inputs)
    normed = (unit * gains[0]).astype(jnp.bfloat16)
    projected = jnp.einsum("rd,jdw->jrw", normed, w_qkv, preferred_element_type=jnp.float32).astype(
        jnp.bfloat16
    )
    shaped = projected.reshape(3, count, length, head_count, HEAD)
    shares, _ = attention_shares(shaped[0], shaped[1], None)
    context = jnp.einsum(
        "nhqk,nkhe->nqhe",
        shares.astype(jnp.bfloat16),
        shaped[2],
        preferred_element_type=jnp.float32,
    )
    context = context.astype(jnp.bfloat16).reshape(count * length, D)
    middle = inputs + jnp.dot(context, w_out, preferred_element_type=jnp.float32)
    return inputs, middle


def image_ffn(middle, count, length, gains, w_fc1, w_fc2):
    unit2, _ = layer_stats(middle)
    normed2 = (unit2 * gains[1]).astype(jnp.bfloat16)
    active = gelu_exact(jnp.dot(normed2, w_fc1, preferred_element_type=jnp.float32)).astype(
        jnp.bfloat16
    )
    pool = (
        lax.broadcasted_iota(jnp.int32, (count, count * length), 1) // length
        == lax.broadcasted_iota(jnp.int32, (count, count * length), 0)
    ).astype(jnp.bfloat16)
    mean_active = jnp.dot(pool, active, preferred_element_type=jnp.float32) / length
    pooled = jnp.mean(middle.reshape(count, length, D), 1) + jnp.dot(
        mean_active, w_fc2.astype(jnp.float32), precision=lax.Precision.HIGHEST
    )
    return (pooled * lax.rsqrt(jnp.sum(pooled * pooled, -1, keepdims=True) + EPS)).astype(
        jnp.bfloat16
    )


def local_body(
    text_in,
    caption_ids,
    pairing,
    image_low,
    image_high,
    img_gains,
    img_qkv,
    img_out,
    img_fc1,
    img_fc2,
    txt_qkv,
    txt_qv_bias,
    txt_out,
    txt_fc1,
    txt_fc1_bias,
    txt_fc2,
    txt_gains,
    txt_shifts,
    txt_biases,
):
    qkv_parts = gather_stacked(img_qkv, "mp")
    out_parts = gather_stacked(img_out, "mp")
    qkv_parts, out_parts, fc1_local, fc2_local = lax.optimization_barrier(
        (qkv_parts, out_parts, img_fc1, img_fc2)
    )
    fc1_parts = gather_stacked(fc1_local, "mp")
    weights = (
        qkv_parts.transpose(1, 2, 0, 3).reshape(3, D, -1),
        out_parts.reshape(-1, D),
        fc1_parts.transpose(1, 0, 2).reshape(D, -1),
        gather_stacked(fc2_local, "mp").reshape(-1, D),
    )
    low_count = image_low.shape[0] // P_LOW
    high_count = image_high.shape[0] // P_HIGH
    images16 = jnp.concatenate(
        [
            image_tower(image_low, low_count, P_LOW, img_gains, weights),
            image_tower(image_high, high_count, P_HIGH, img_gains, weights),
        ],
        0,
    )
    width = txt_qkv.shape[2]
    head_count = width // HEAD
    own_rows = text_in.shape[0]
    own_caps = own_rows // L
    group_caps = caption_ids.shape[0]
    group_rows = group_caps * L
    mp_index = lax.axis_index("mp")
    present = (caption_ids > 0).astype(jnp.float32)
    keep = (caption_ids > 0)[:, None, None, :]
    counts = jnp.sum(present, 1, keepdims=True)
    inputs = lax.all_gather(text_in, "mp", axis=0, tiled=True).astype(jnp.float32)
    unit1, inverse1 = layer_stats(inputs)
    normed1_all = (unit1 * txt_gains[0] + txt_shifts[0]).astype(jnp.bfloat16)
    bias_rows = jnp.stack([txt_qv_bias[0], jnp.zeros_like(txt_qv_bias[0]), txt_qv_bias[1]])
    made = (
        jnp.einsum("rd,jdw->rjw", normed1_all, txt_qkv, preferred_element_type=jnp.float32)
        + bias_rows
    )
    triple = made.astype(jnp.bfloat16).reshape(group_caps, L, 3, head_count, HEAD)
    queries = triple[:, :, 0]
    keys_all = triple[:, :, 1]
    values_all = triple[:, :, 2]
    shares, log_totals = attention_shares(queries, keys_all, keep)
    context = jnp.einsum(
        "nhqk,nkhe->nqhe",
        shares.astype(jnp.bfloat16),
        values_all,
        preferred_element_type=jnp.float32,
    )
    context = context.astype(jnp.bfloat16).reshape(group_rows, width)
    middle = inputs + (
        lax.psum(
            jnp.dot(context, txt_out, preferred_element_type=jnp.float32).astype(jnp.bfloat16),
            "mp",
        ).astype(jnp.float32)
        + txt_biases[0]
    )
    unit2, inverse2 = layer_stats(middle)
    normed2_all = (unit2 * txt_gains[1] + txt_shifts[1]).astype(jnp.bfloat16)
    hidden = jnp.dot(normed2_all, txt_fc1, preferred_element_type=jnp.float32) + txt_fc1_bias
    active, gelu_pull = jax.vjp(gelu_exact, hidden)
    active16 = active.astype(jnp.bfloat16)
    ffn_part = jnp.dot(active16, txt_fc2, preferred_element_type=jnp.float32)
    ffn_pooled = jnp.sum(ffn_part.reshape(group_caps, L, D) * present[:, :, None], 1)
    image_slots = lax.dynamic_update_slice_in_dim(
        jnp.zeros((group_caps, D), jnp.float32),
        images16.astype(jnp.float32),
        mp_index * own_caps,
        0,
    )
    both = sum_exchanged(jnp.concatenate([ffn_pooled, image_slots], 0), "mp")
    mid_pooled = jnp.sum(middle.reshape(group_caps, L, D) * present[:, :, None], 1)
    pooled = (mid_pooled + both[:group_caps]) / counts + txt_biases[1]
    inverse_len = lax.rsqrt(jnp.sum(pooled * pooled, -1, keepdims=True) + EPS)
    captions_unit = pooled * inverse_len
    captions16 = captions_unit.astype(jnp.bfloat16)
    gathered = gather_ordered(
        jnp.concatenate([captions16, both[group_caps:].astype(jnp.bfloat16)], 0), "dp"
    )
    arrived = gathered[:, :group_caps].reshape(-1, D)
    images_all = gathered[:, group_caps:].reshape(-1, D)
    total_pairs = pairing.shape[0]
    first_pair = lax.axis_index("dp") * group_caps
    logits = SCALE * jnp.einsum("id,jd->ij", images_all, arrived, preferred_element_type=jnp.float32)
    matched = (pairing[:, None] == jnp.arange(total_pairs)[None, :]).astype(jnp.float32)
    raised = jnp.exp(logits - SCALE)
    row_lse = SCALE + jnp.log(jnp.sum(raised, 1))
    col_lse = SCALE + jnp.log(jnp.sum(raised, 0))
    total = 0.5 * jnp.sum(row_lse) + 0.5 * jnp.sum(col_lse) - jnp.sum(matched * logits)
    loss = total / total_pairs
    own_logits = lax.dynamic_slice_in_dim(logits, first_pair, group_caps, 1)
    own_col_lse = lax.dynamic_slice_in_dim(col_lse, first_pair, group_caps, 0)
    own_matched = lax.dynamic_slice_in_dim(matched, first_pair, group_caps, 1)
    grads16 = (
        LOSS_SCALE
        * (
            0.5 * jnp.exp(own_logits - row_lse[:, None])
            + 0.5 * jnp.exp(own_logits - own_col_lse[None, :])
            - own_matched
        )
    ).astype(jnp.bfloat16)
    grad_caps = SCALE * jnp.einsum(
        "ic,id->cd", grads16, images_all, preferred_element_type=jnp.float32
    )
    grad_pooled = inverse_len * (
        grad_caps - captions_unit * jnp.sum(captions_unit * grad_caps, -1, keepdims=True)
    )
    grad_result = (grad_pooled[:, None, :] * (present / counts)[:, :, None]).reshape(group_rows, D)
    grad_all = grad_result.astype(jnp.bfloat16)
    grad_fc2 = jnp.einsum("gf,gd->fd", active16, grad_all, preferred_element_type=jnp.float32)
    grad_active = jnp.einsum("gd,fd->gf", grad_all, txt_fc2, preferred_element_type=jnp.float32)
    grad_hidden16 = gelu_pull(grad_active)[0].astype(jnp.bfloat16)
    grad_fc1 = jnp.einsum(
        "gd,gf->df", normed2_all, grad_hidden16, preferred_element_type=jnp.float32
    )
    grad_fc1_bias = jnp.sum(grad_hidden16.astype(jnp.float32), 0)
    fc_sums = lax.psum(jnp.concatenate([grad_fc1, grad_fc2], 0).astype(jnp.bfloat16), "dp")
    grad_normed2 = reduce_exchanged(
        jnp.einsum("gf,df->gd", grad_hidden16, txt_fc1, preferred_element_type=jnp.float32), "mp"
    ).astype(jnp.float32)
    grad_middle = grad_result + norm_back(grad_normed2, unit2, inverse2, txt_gains[1])
    grad_mid_all = grad_middle.astype(jnp.bfloat16)
    grad_out = jnp.einsum("gw,gd->wd", context, grad_mid_all, preferred_element_type=jnp.float32)
    grad_context = jnp.einsum(
        "gd,wd->gw", grad_mid_all, txt_out, preferred_element_type=jnp.float32
    )
    grad_context = grad_context.astype(jnp.bfloat16).reshape(group_caps, L, head_count, HEAD)
    shares_again = jnp.exp(score_rows(queries, keys_all, keep) - log_totals)
    grad_shares = jnp.einsum(
        "nqhe,nkhe->nhqk", grad_context, values_all, preferred_element_type=jnp.float32
    )
    grad_values = jnp.einsum(
        "nhqk,nqhe->nkhe",
        shares_again.astype(jnp.bfloat16),
        grad_context,
        preferred_element_type=jnp.float32,
    ).astype(jnp.bfloat16)
    grad_scores = (
        shares_again * (grad_shares - jnp.sum(grad_shares * shares_again, -1, keepdims=True))
    ).astype(jnp.bfloat16)
    grad_queries = (
        jnp.einsum("nhqk,nkhe->nqhe", grad_scores, keys_all, preferred_element_type=jnp.float32)
        * 0.125
    ).astype(jnp.bfloat16)
    grad_keys = (
        jnp.einsum("nhqk,nqhe->nkhe", grad_scores, queries, preferred_element_type=jnp.float32)
        * 0.125
    ).astype(jnp.bfloat16)
    grad_triple = jnp.stack([grad_queries, grad_keys, grad_values], 0).reshape(3, group_rows, width)
    grad_qkv = jnp.einsum(
        "gd,jgw->jdw", normed1_all, grad_triple, preferred_element_type=jnp.float32
    )
    grad_qv_bias = jnp.stack(
        [
            jnp.sum(grad_triple[0].astype(jnp.float32), 0),
            jnp.sum(grad_triple[2].astype(jnp.float32), 0),
        ]
    )
    attn_sums = reduce_exchanged(jnp.concatenate([grad_qkv.reshape(-1, D), grad_out], 0), "dp")
    grad_normed1 = scatter_exchanged(
        jnp.einsum("jgw,jdw->gd", grad_triple, txt_qkv, preferred_element_type=jnp.float32), "mp"
    )

    def own(values):
        return lax.dynamic_slice_in_dim(values, mp_index * own_rows, own_rows, 0)

    unit1_own = own(unit1)
    grad_normed2_own = own(grad_normed2)
    unit2_own = own(unit2)
    grad_middle_own = own(grad_middle)
    grad_inputs = grad_middle_own + norm_back(grad_normed1, unit1_own, own(inverse1), txt_gains[0])
    small_parts = jnp.stack(
        [
            jnp.sum(grad_normed1 * unit1_own, 0),
            jnp.sum(grad_normed2_own * unit2_own, 0),
            jnp.sum(grad_normed1, 0),
            jnp.sum(grad_normed2_own, 0),
            jnp.sum(grad_middle_own, 0),
            jnp.sum(own(grad_result), 0),
        ]
    )
    bias_rows = jnp.stack(
        [jnp.concatenate([grad_qv_bias.reshape(-1), jnp.zeros_like(grad_qv_bias.reshape(-1))]), grad_fc1_bias]
    )
    shared = sum_exchanged(jnp.concatenate([sum_exchanged(small_parts, "mp"), bias_rows], 0), "dp")
    qv_count = grad_qv_bias.size
    fc1_rows = grad_fc1.shape[0]
    return (
        loss,
        grad_inputs,
        attn_sums[: grad_qkv.size // D].astype(jnp.float32).reshape(grad_qkv.shape),
        shared[6, :qv_count].reshape(grad_qv_bias.shape),
        attn_sums[grad_qkv.size // D :].astype(jnp.float32),
        fc_sums[:fc1_rows].astype(jnp.float32),
        shared[7],
        fc_sums[fc1_rows:].astype(jnp.float32),
        shared[0:2],
        shared[2:4],
        shared[4:6],
    )


def solution(mesh):
    placed = (
        P(("dp", "mp"), None),
        P("dp", None),
        P(),
        P(("dp", "mp"), None),
        P(("dp", "mp"), None),
        P(),
        P(None, None, "mp"),
        P("mp", None),
        P(None, "mp"),
        P("mp", None),
        P(None, None, "mp"),
        P(None, "mp"),
        P("mp", None),
        P(None, "mp"),
        P("mp"),
        P("mp", None),
        P(),
        P(),
        P(),
    )
    return jax.shard_map(
        local_body,
        mesh=mesh,
        in_specs=placed,
        out_specs=(
            P(),
            P(("dp", "mp"), None),
            P(None, None, "mp"),
            P(None, "mp"),
            P("mp", None),
            P(None, "mp"),
            P("mp"),
            P("mp", None),
            P(),
            P(),
            P(),
        ),
        check_vma=False,
    )
```

```python
import jax
import jax.numpy as jnp
from jax import lax
from jax.sharding import PartitionSpec as P

D = 768
HEAD = 64
L = 16
P_LOW = 50
P_HIGH = 145


EPS = 1e-06
SCALE = 40.0
LOSS_SCALE = 16.0
MASKED = -1e30


def layer_stats(values):
    center = values - jnp.mean(values, -1, keepdims=True)
    inverse = lax.rsqrt(jnp.mean(center * center, -1, keepdims=True) + EPS)
    return (center * inverse, inverse)


def norm_back(grad_out, unit, inverse, gain):
    scaled = grad_out * gain
    return inverse * (
        scaled
        - jnp.mean(scaled, -1, keepdims=True)
        - unit * jnp.mean(scaled * unit, -1, keepdims=True)
    )


def gelu_exact(values):
    return jax.nn.gelu(values, approximate=False)


def score_rows(queries, keys_all, keep):
    scores = (
        jnp.einsum("nqhe,nkhe->nhqk", queries, keys_all, preferred_element_type=jnp.float32) * 0.125
    )
    if keep is not None:
        scores = jnp.where(keep, scores, MASKED)
    return scores


def attention_shares(queries, keys_all, keep):
    scores = score_rows(queries, keys_all, keep)
    highest = jnp.max(scores, -1, keepdims=True)
    raised = jnp.exp(scores - highest)
    totals = jnp.sum(raised, -1, keepdims=True)
    return (raised / totals, highest + jnp.log(totals))


def axis_bits(axis):
    count = lax.axis_size(axis)
    bits = count.bit_length() - 1
    assert 1 << bits == count
    return count, list(reversed(range(bits)))


def exchange(values, axis, count, bit):
    return lax.ppermute(values, axis, [(i, i ^ (1 << bit)) for i in range(count)])


def gather_stacked(values, axis):
    count, bits = axis_bits(axis)
    data = values[None]
    for bit in bits:
        data = jnp.concatenate([data, exchange(data, axis, count, bit)], 0)
    return data


def gather_ordered(values, axis):
    count, bits = axis_bits(axis)
    index = lax.axis_index(axis)
    data = values
    done = []
    for bit in bits:
        other = exchange(data, axis, count, bit)
        upper = ((index >> bit) & 1) == 1
        data = jnp.stack([jnp.where(upper, other, data), jnp.where(upper, data, other)], 0)
        done.insert(0, bit)
    order = sorted(range(len(done)), key=lambda a: -done[a])
    data = data.transpose(order + list(range(len(done), data.ndim)))
    return data.reshape((count,) + values.shape)


def sum_exchanged(values, axis):
    count, bits = axis_bits(axis)
    for bit in reversed(bits):
        values = values + exchange(values, axis, count, bit)
    return values


def scatter_exchanged(values, axis):
    count, bits = axis_bits(axis)
    index = lax.axis_index(axis)
    data = values.reshape((2,) * len(bits) + (values.shape[0] // count,) + values.shape[1:])
    for bit in reversed(bits):
        place = len(bits) - 1 - bit
        mine = (index >> bit) & 1
        kept = lax.dynamic_index_in_dim(data, mine, place, keepdims=False)
        sent = lax.dynamic_index_in_dim(data, 1 - mine, place, keepdims=False)
        data = kept + exchange(sent.astype(jnp.bfloat16), axis, count, bit).astype(jnp.float32)
    return data


def reduce_exchanged(values, axis):
    part = scatter_exchanged(values, axis).astype(jnp.bfloat16)
    return gather_ordered(part, axis).reshape(values.shape)


def image_tower(tokens, count, length, gains, weights):
    w_qkv, w_out, w_fc1, w_fc2 = weights
    _, middle = image_attention(tokens, count, length, gains, w_qkv, w_out)
    return image_ffn(middle, count, length, gains, w_fc1, w_fc2)


def image_attention(tokens, count, length, gains, w_qkv, w_out):
    head_count = D // HEAD
    inputs = tokens.astype(jnp.float32)
    unit, _ = layer_stats(inputs)
    normed = (unit * gains[0]).astype(jnp.bfloat16)
    projected = jnp.einsum("rd,jdw->jrw", normed, w_qkv, preferred_element_type=jnp.float32).astype(
        jnp.bfloat16
    )
    shaped = projected.reshape(3, count, length, head_count, HEAD)
    shares, _ = attention_shares(shaped[0], shaped[1], None)
    context = jnp.einsum(
        "nhqk,nkhe->nqhe",
        shares.astype(jnp.bfloat16),
        shaped[2],
        preferred_element_type=jnp.float32,
    )
    context = context.astype(jnp.bfloat16).reshape(count * length, D)
    middle = inputs + jnp.dot(context, w_out, preferred_element_type=jnp.float32)
    return inputs, middle


def image_ffn(middle, count, length, gains, w_fc1, w_fc2):
    unit2, _ = layer_stats(middle)
    normed2 = (unit2 * gains[1]).astype(jnp.bfloat16)
    active = gelu_exact(jnp.dot(normed2, w_fc1, preferred_element_type=jnp.float32)).astype(
        jnp.bfloat16
    )
    pool = (
        lax.broadcasted_iota(jnp.int32, (count, count * length), 1) // length
        == lax.broadcasted_iota(jnp.int32, (count, count * length), 0)
    ).astype(jnp.bfloat16)
    mean_active = jnp.dot(pool, active, preferred_element_type=jnp.float32) / length
    pooled = jnp.mean(middle.reshape(count, length, D), 1) + jnp.dot(
        mean_active, w_fc2.astype(jnp.float32), precision=lax.Precision.HIGHEST
    )
    return (pooled * lax.rsqrt(jnp.sum(pooled * pooled, -1, keepdims=True) + EPS)).astype(
        jnp.bfloat16
    )


def local_body(
    text_in,
    caption_ids,
    pairing,
    image_low,
    image_high,
    img_gains,
    img_qkv,
    img_out,
    img_fc1,
    img_fc2,
    txt_qkv,
    txt_qv_bias,
    txt_out,
    txt_fc1,
    txt_fc1_bias,
    txt_fc2,
    txt_gains,
    txt_shifts,
    txt_biases,
):
    qkv_parts = gather_stacked(img_qkv, "mp")
    out_parts = gather_stacked(img_out, "mp")
    qkv_parts, out_parts, fc1_local, fc2_local = lax.optimization_barrier(
        (qkv_parts, out_parts, img_fc1, img_fc2)
    )
    fc1_parts = gather_stacked(fc1_local, "mp")
    weights = (
        qkv_parts.transpose(1, 2, 0, 3).reshape(3, D, -1),
        out_parts.reshape(-1, D),
        fc1_parts.transpose(1, 0, 2).reshape(D, -1),
        gather_stacked(fc2_local, "mp").reshape(-1, D),
    )
    low_count = image_low.shape[0] // P_LOW
    high_count = image_high.shape[0] // P_HIGH
    images16 = jnp.concatenate(
        [
            image_tower(image_low, low_count, P_LOW, img_gains, weights),
            image_tower(image_high, high_count, P_HIGH, img_gains, weights),
        ],
        0,
    )
    width = txt_qkv.shape[2]
    head_count = width // HEAD
    own_rows = text_in.shape[0]
    own_caps = own_rows // L
    group_caps = caption_ids.shape[0]
    group_rows = group_caps * L
    mp_index = lax.axis_index("mp")
    present = (caption_ids > 0).astype(jnp.float32)
    keep = (caption_ids > 0)[:, None, None, :]
    counts = jnp.sum(present, 1, keepdims=True)
    inputs = lax.all_gather(text_in, "mp", axis=0, tiled=True).astype(jnp.float32)
    unit1, inverse1 = layer_stats(inputs)
    normed1_all = (unit1 * txt_gains[0] + txt_shifts[0]).astype(jnp.bfloat16)
    bias_rows = jnp.stack([txt_qv_bias[0], jnp.zeros_like(txt_qv_bias[0]), txt_qv_bias[1]])
    made = (
        jnp.einsum("rd,jdw->rjw", normed1_all, txt_qkv, preferred_element_type=jnp.float32)
        + bias_rows
    )
    triple = made.astype(jnp.bfloat16).reshape(group_caps, L, 3, head_count, HEAD)
    queries = triple[:, :, 0]
    keys_all = triple[:, :, 1]
    values_all = triple[:, :, 2]
    shares, log_totals = attention_shares(queries, keys_all, keep)
    context = jnp.einsum(
        "nhqk,nkhe->nqhe",
        shares.astype(jnp.bfloat16),
        values_all,
        preferred_element_type=jnp.float32,
    )
    context = context.astype(jnp.bfloat16).reshape(group_rows, width)
    attn_part = jnp.dot(context, txt_out, preferred_element_type=jnp.float32).astype(jnp.bfloat16)
    attn_full = lax.psum(attn_part, "mp")
    middle = inputs + (attn_full.astype(jnp.float32) + txt_biases[0])
    unit2, inverse2 = layer_stats(middle)
    normed2_all = (unit2 * txt_gains[1] + txt_shifts[1]).astype(jnp.bfloat16)
    hidden = jnp.dot(normed2_all, txt_fc1, preferred_element_type=jnp.float32) + txt_fc1_bias
    active, gelu_pull = jax.vjp(gelu_exact, hidden)
    active16 = active.astype(jnp.bfloat16)
    ffn_part = jnp.dot(active16, txt_fc2, preferred_element_type=jnp.float32)
    ffn_pooled = jnp.sum(ffn_part.reshape(group_caps, L, D) * present[:, :, None], 1)
    image_slots = lax.dynamic_update_slice_in_dim(
        jnp.zeros((group_caps, D), jnp.float32),
        images16.astype(jnp.float32),
        mp_index * own_caps,
        0,
    )
    both = sum_exchanged(jnp.concatenate([ffn_pooled, image_slots], 0), "mp")
    mid_pooled = jnp.sum(middle.reshape(group_caps, L, D) * present[:, :, None], 1)
    pooled = (mid_pooled + both[:group_caps]) / counts + txt_biases[1]
    inverse_len = lax.rsqrt(jnp.sum(pooled * pooled, -1, keepdims=True) + EPS)
    captions_unit = pooled * inverse_len
    captions16 = captions_unit.astype(jnp.bfloat16)
    gathered = gather_ordered(
        jnp.concatenate([captions16, both[group_caps:].astype(jnp.bfloat16)], 0), "dp"
    )
    arrived = gathered[:, :group_caps].reshape(-1, D)
    images_all = gathered[:, group_caps:].reshape(-1, D)
    total_pairs = pairing.shape[0]
    first_pair = lax.axis_index("dp") * group_caps
    logits = SCALE * jnp.einsum("id,jd->ij", images_all, arrived, preferred_element_type=jnp.float32)
    matched = (pairing[:, None] == jnp.arange(total_pairs)[None, :]).astype(jnp.float32)
    raised = jnp.exp(logits - SCALE)
    row_lse = SCALE + jnp.log(jnp.sum(raised, 1))
    col_lse = SCALE + jnp.log(jnp.sum(raised, 0))
    total = 0.5 * jnp.sum(row_lse) + 0.5 * jnp.sum(col_lse) - jnp.sum(matched * logits)
    loss = total / total_pairs
    own_logits = lax.dynamic_slice_in_dim(logits, first_pair, group_caps, 1)
    own_col_lse = lax.dynamic_slice_in_dim(col_lse, first_pair, group_caps, 0)
    own_matched = lax.dynamic_slice_in_dim(matched, first_pair, group_caps, 1)
    grads16 = (
        LOSS_SCALE
        * (
            0.5 * jnp.exp(own_logits - row_lse[:, None])
            + 0.5 * jnp.exp(own_logits - own_col_lse[None, :])
            - own_matched
        )
    ).astype(jnp.bfloat16)
    grad_caps = SCALE * jnp.einsum(
        "ic,id->cd", grads16, images_all, preferred_element_type=jnp.float32
    )
    grad_pooled = inverse_len * (
        grad_caps - captions_unit * jnp.sum(captions_unit * grad_caps, -1, keepdims=True)
    )
    grad_result = (grad_pooled[:, None, :] * (present / counts)[:, :, None]).reshape(group_rows, D)
    grad_all = grad_result.astype(jnp.bfloat16)
    grad_fc2 = jnp.einsum("gf,gd->fd", active16, grad_all, preferred_element_type=jnp.float32)
    grad_active = jnp.einsum("gd,fd->gf", grad_all, txt_fc2, preferred_element_type=jnp.float32)
    grad_hidden16 = gelu_pull(grad_active)[0].astype(jnp.bfloat16)
    grad_fc1 = jnp.einsum(
        "gd,gf->df", normed2_all, grad_hidden16, preferred_element_type=jnp.float32
    )
    grad_fc1_bias = jnp.sum(grad_hidden16.astype(jnp.float32), 0)
    fc_sums = lax.psum(jnp.concatenate([grad_fc1, grad_fc2], 0).astype(jnp.bfloat16), "dp")
    grad_normed2 = reduce_exchanged(
        jnp.einsum("gf,df->gd", grad_hidden16, txt_fc1, preferred_element_type=jnp.float32), "mp"
    ).astype(jnp.float32)
    grad_middle = grad_result + norm_back(grad_normed2, unit2, inverse2, txt_gains[1])
    grad_mid_all = grad_middle.astype(jnp.bfloat16)
    grad_out = jnp.einsum("gw,gd->wd", context, grad_mid_all, preferred_element_type=jnp.float32)
    grad_context = jnp.einsum(
        "gd,wd->gw", grad_mid_all, txt_out, preferred_element_type=jnp.float32
    )
    grad_context = grad_context.astype(jnp.bfloat16).reshape(group_caps, L, head_count, HEAD)
    shares_again = jnp.exp(score_rows(queries, keys_all, keep) - log_totals)
    grad_shares = jnp.einsum(
        "nqhe,nkhe->nhqk", grad_context, values_all, preferred_element_type=jnp.float32
    )
    grad_values = jnp.einsum(
        "nhqk,nqhe->nkhe",
        shares_again.astype(jnp.bfloat16),
        grad_context,
        preferred_element_type=jnp.float32,
    ).astype(jnp.bfloat16)
    grad_scores = (
        shares_again * (grad_shares - jnp.sum(grad_shares * shares_again, -1, keepdims=True))
    ).astype(jnp.bfloat16)
    grad_queries = (
        jnp.einsum("nhqk,nkhe->nqhe", grad_scores, keys_all, preferred_element_type=jnp.float32)
        * 0.125
    ).astype(jnp.bfloat16)
    grad_keys = (
        jnp.einsum("nhqk,nqhe->nkhe", grad_scores, queries, preferred_element_type=jnp.float32)
        * 0.125
    ).astype(jnp.bfloat16)
    grad_triple = jnp.stack([grad_queries, grad_keys, grad_values], 0).reshape(3, group_rows, width)
    grad_qkv = jnp.einsum(
        "gd,jgw->jdw", normed1_all, grad_triple, preferred_element_type=jnp.float32
    )
    grad_qv_bias = jnp.stack(
        [
            jnp.sum(grad_triple[0].astype(jnp.float32), 0),
            jnp.sum(grad_triple[2].astype(jnp.float32), 0),
        ]
    )
    attn_sums = reduce_exchanged(jnp.concatenate([grad_qkv.reshape(-1, D), grad_out], 0), "dp")
    grad_normed1 = scatter_exchanged(
        jnp.einsum("jgw,jdw->gd", grad_triple, txt_qkv, preferred_element_type=jnp.float32), "mp"
    )

    def own(values):
        return lax.dynamic_slice_in_dim(values, mp_index * own_rows, own_rows, 0)

    unit1_own = own(unit1)
    grad_normed2_own = own(grad_normed2)
    unit2_own = own(unit2)
    grad_middle_own = own(grad_middle)
    grad_inputs = grad_middle_own + norm_back(grad_normed1, unit1_own, own(inverse1), txt_gains[0])
    small_parts = jnp.stack(
        [
            jnp.sum(grad_normed1 * unit1_own, 0),
            jnp.sum(grad_normed2_own * unit2_own, 0),
            jnp.sum(grad_normed1, 0),
            jnp.sum(grad_normed2_own, 0),
            jnp.sum(grad_middle_own, 0),
            jnp.sum(own(grad_result), 0),
        ]
    )
    bias_rows = jnp.stack(
        [jnp.concatenate([grad_qv_bias.reshape(-1), jnp.zeros_like(grad_qv_bias.reshape(-1))]), grad_fc1_bias]
    )
    shared = sum_exchanged(jnp.concatenate([sum_exchanged(small_parts, "mp"), bias_rows], 0), "dp")
    qv_count = grad_qv_bias.size
    fc1_rows = grad_fc1.shape[0]
    return (
        loss,
        grad_inputs,
        attn_sums[: grad_qkv.size // D].astype(jnp.float32).reshape(grad_qkv.shape),
        shared[6, :qv_count].reshape(grad_qv_bias.shape),
        attn_sums[grad_qkv.size // D :].astype(jnp.float32),
        fc_sums[:fc1_rows].astype(jnp.float32),
        shared[7],
        fc_sums[fc1_rows:].astype(jnp.float32),
        shared[0:2],
        shared[2:4],
        shared[4:6],
    )


def solution(mesh):
    placed = (
        P(("dp", "mp"), None),
        P("dp", None),
        P(),
        P(("dp", "mp"), None),
        P(("dp", "mp"), None),
        P(),
        P(None, None, "mp"),
        P("mp", None),
        P(None, "mp"),
        P("mp", None),
        P(None, None, "mp"),
        P(None, "mp"),
        P("mp", None),
        P(None, "mp"),
        P("mp"),
        P("mp", None),
        P(),
        P(),
        P(),
    )
    return jax.shard_map(
        local_body,
        mesh=mesh,
        in_specs=placed,
        out_specs=(
            P(),
            P(("dp", "mp"), None),
            P(None, None, "mp"),
            P(None, "mp"),
            P("mp", None),
            P(None, "mp"),
            P("mp"),
            P("mp", None),
            P(),
            P(),
            P(),
        ),
        check_vma=False,
    )
```

```python
import jax
import jax.numpy as jnp
from jax import lax
from jax.sharding import PartitionSpec as P

D = 768
HEAD = 64
L = 16
P_LOW = 50
P_HIGH = 145


EPS = 1e-06
SCALE = 40.0
LOSS_SCALE = 16.0
MASKED = -1e30


def layer_stats(values):
    center = values - jnp.mean(values, -1, keepdims=True)
    inverse = lax.rsqrt(jnp.mean(center * center, -1, keepdims=True) + EPS)
    return (center * inverse, inverse)


def norm_back(grad_out, unit, inverse, gain):
    scaled = grad_out * gain
    return inverse * (
        scaled
        - jnp.mean(scaled, -1, keepdims=True)
        - unit * jnp.mean(scaled * unit, -1, keepdims=True)
    )


def gelu_exact(values):
    return jax.nn.gelu(values, approximate=False)


def score_rows(queries, keys_all, keep):
    scores = (
        jnp.einsum("nqhe,nkhe->nhqk", queries, keys_all, preferred_element_type=jnp.float32) * 0.125
    )
    if keep is not None:
        scores = jnp.where(keep, scores, MASKED)
    return scores


def attention_shares(queries, keys_all, keep):
    scores = score_rows(queries, keys_all, keep)
    highest = jnp.max(scores, -1, keepdims=True)
    raised = jnp.exp(scores - highest)
    totals = jnp.sum(raised, -1, keepdims=True)
    return (raised / totals, highest + jnp.log(totals))


def axis_bits(axis):
    count = lax.axis_size(axis)
    bits = count.bit_length() - 1
    assert 1 << bits == count
    return count, list(reversed(range(bits)))


def exchange(values, axis, count, bit):
    return lax.ppermute(values, axis, [(i, i ^ (1 << bit)) for i in range(count)])


def gather_chunks(values, axis):
    count, bits = axis_bits(axis)
    chunks = [values]
    for bit in bits:
        chunks = chunks + [exchange(chunk, axis, count, bit) for chunk in chunks]
    return chunks


def gather_ordered(values, axis):
    count, bits = axis_bits(axis)
    index = lax.axis_index(axis)
    data = values
    done = []
    for bit in bits:
        other = exchange(data, axis, count, bit)
        upper = ((index >> bit) & 1) == 1
        data = jnp.stack([jnp.where(upper, other, data), jnp.where(upper, data, other)], 0)
        done.insert(0, bit)
    order = sorted(range(len(done)), key=lambda a: -done[a])
    data = data.transpose(order + list(range(len(done), data.ndim)))
    return data.reshape((count,) + values.shape)


def sum_exchanged(values, axis):
    count, bits = axis_bits(axis)
    for bit in reversed(bits):
        values = values + exchange(values, axis, count, bit)
    return values


def scatter_exchanged(values, axis):
    count, bits = axis_bits(axis)
    index = lax.axis_index(axis)
    data = values.reshape((2,) * len(bits) + (values.shape[0] // count,) + values.shape[1:])
    for bit in reversed(bits):
        place = len(bits) - 1 - bit
        mine = (index >> bit) & 1
        kept = lax.dynamic_index_in_dim(data, mine, place, keepdims=False)
        sent = lax.dynamic_index_in_dim(data, 1 - mine, place, keepdims=False)
        data = kept + exchange(sent.astype(jnp.bfloat16), axis, count, bit).astype(jnp.float32)
    return data


def reduce_exchanged(values, axis):
    part = scatter_exchanged(values, axis).astype(jnp.bfloat16)
    return gather_ordered(part, axis).reshape(values.shape)


def image_tower(tokens, count, length, gains, weights):
    qkv_chunks, out_chunks, fc1_chunks, fc2_chunks = weights
    inputs = tokens.astype(jnp.float32)
    unit, _ = layer_stats(inputs)
    normed = (unit * gains[0]).astype(jnp.bfloat16)
    middle = inputs
    for w_qkv, w_out in zip(qkv_chunks, out_chunks):
        middle = middle + image_heads(normed, count, length, w_qkv, w_out)
    unit2, _ = layer_stats(middle)
    normed2 = (unit2 * gains[1]).astype(jnp.bfloat16)
    result = middle
    for w_fc1, w_fc2 in zip(fc1_chunks, fc2_chunks):
        active = gelu_exact(jnp.dot(normed2, w_fc1, preferred_element_type=jnp.float32)).astype(
            jnp.bfloat16
        )
        result = result + jnp.dot(active, w_fc2, preferred_element_type=jnp.float32)
    pooled = jnp.mean(result.reshape(count, length, D), 1)
    return (pooled * lax.rsqrt(jnp.sum(pooled * pooled, -1, keepdims=True) + EPS)).astype(
        jnp.bfloat16
    )


def image_heads(normed, count, length, w_qkv, w_out):
    head_count = w_qkv.shape[2] // HEAD
    projected = jnp.einsum("rd,jdw->jrw", normed, w_qkv, preferred_element_type=jnp.float32).astype(
        jnp.bfloat16
    )
    shaped = projected.reshape(3, count, length, head_count, HEAD)
    shares, _ = attention_shares(shaped[0], shaped[1], None)
    context = jnp.einsum(
        "nhqk,nkhe->nqhe",
        shares.astype(jnp.bfloat16),
        shaped[2],
        preferred_element_type=jnp.float32,
    )
    context = context.astype(jnp.bfloat16).reshape(count * length, head_count * HEAD)
    return jnp.dot(context, w_out, preferred_element_type=jnp.float32)


def local_body(
    text_in,
    caption_ids,
    pairing,
    image_low,
    image_high,
    img_gains,
    img_qkv,
    img_out,
    img_fc1,
    img_fc2,
    txt_qkv,
    txt_qv_bias,
    txt_out,
    txt_fc1,
    txt_fc1_bias,
    txt_fc2,
    txt_gains,
    txt_shifts,
    txt_biases,
):
    weights = (
        gather_chunks(img_qkv, "mp"),
        gather_chunks(img_out, "mp"),
        gather_chunks(img_fc1, "mp"),
        gather_chunks(img_fc2, "mp"),
    )
    low_count = image_low.shape[0] // P_LOW
    high_count = image_high.shape[0] // P_HIGH
    images16 = jnp.concatenate(
        [
            image_tower(image_low, low_count, P_LOW, img_gains, weights),
            image_tower(image_high, high_count, P_HIGH, img_gains, weights),
        ],
        0,
    )
    width = txt_qkv.shape[2]
    head_count = width // HEAD
    own_rows = text_in.shape[0]
    own_caps = own_rows // L
    group_caps = caption_ids.shape[0]
    group_rows = group_caps * L
    mp_index = lax.axis_index("mp")
    present = (caption_ids > 0).astype(jnp.float32)
    keep = (caption_ids > 0)[:, None, None, :]
    counts = jnp.sum(present, 1, keepdims=True)
    inputs = lax.all_gather(text_in, "mp", axis=0, tiled=True).astype(jnp.float32)
    unit1, inverse1 = layer_stats(inputs)
    normed1_all = (unit1 * txt_gains[0] + txt_shifts[0]).astype(jnp.bfloat16)
    bias_rows = jnp.stack([txt_qv_bias[0], jnp.zeros_like(txt_qv_bias[0]), txt_qv_bias[1]])
    made = (
        jnp.einsum("rd,jdw->rjw", normed1_all, txt_qkv, preferred_element_type=jnp.float32)
        + bias_rows
    )
    triple = made.astype(jnp.bfloat16).reshape(group_caps, L, 3, head_count, HEAD)
    queries = triple[:, :, 0]
    keys_all = triple[:, :, 1]
    values_all = triple[:, :, 2]
    shares, log_totals = attention_shares(queries, keys_all, keep)
    context = jnp.einsum(
        "nhqk,nkhe->nqhe",
        shares.astype(jnp.bfloat16),
        values_all,
        preferred_element_type=jnp.float32,
    )
    context = context.astype(jnp.bfloat16).reshape(group_rows, width)
    middle = inputs + (
        lax.psum(
            jnp.dot(context, txt_out, preferred_element_type=jnp.float32).astype(jnp.bfloat16),
            "mp",
        ).astype(jnp.float32)
        + txt_biases[0]
    )
    unit2, inverse2 = layer_stats(middle)
    normed2_all = (unit2 * txt_gains[1] + txt_shifts[1]).astype(jnp.bfloat16)
    hidden = jnp.dot(normed2_all, txt_fc1, preferred_element_type=jnp.float32) + txt_fc1_bias
    active, gelu_pull = jax.vjp(gelu_exact, hidden)
    active16 = active.astype(jnp.bfloat16)
    ffn_part = jnp.dot(active16, txt_fc2, preferred_element_type=jnp.float32)
    ffn_pooled = jnp.sum(ffn_part.reshape(group_caps, L, D) * present[:, :, None], 1)
    image_slots = lax.dynamic_update_slice_in_dim(
        jnp.zeros((group_caps, D), jnp.float32),
        images16.astype(jnp.float32),
        mp_index * own_caps,
        0,
    )
    both = sum_exchanged(jnp.concatenate([ffn_pooled, image_slots], 0), "mp")
    mid_pooled = jnp.sum(middle.reshape(group_caps, L, D) * present[:, :, None], 1)
    pooled = (mid_pooled + both[:group_caps]) / counts + txt_biases[1]
    inverse_len = lax.rsqrt(jnp.sum(pooled * pooled, -1, keepdims=True) + EPS)
    captions_unit = pooled * inverse_len
    captions16 = captions_unit.astype(jnp.bfloat16)
    gathered = gather_ordered(
        jnp.concatenate([captions16, both[group_caps:].astype(jnp.bfloat16)], 0), "dp"
    )
    arrived = gathered[:, :group_caps].reshape(-1, D)
    images_all = gathered[:, group_caps:].reshape(-1, D)
    total_pairs = pairing.shape[0]
    first_pair = lax.axis_index("dp") * group_caps
    logits = SCALE * jnp.einsum("id,jd->ij", images_all, arrived, preferred_element_type=jnp.float32)
    matched = (pairing[:, None] == jnp.arange(total_pairs)[None, :]).astype(jnp.float32)
    raised = jnp.exp(logits - SCALE)
    row_lse = SCALE + jnp.log(jnp.sum(raised, 1))
    col_lse = SCALE + jnp.log(jnp.sum(raised, 0))
    total = 0.5 * jnp.sum(row_lse) + 0.5 * jnp.sum(col_lse) - jnp.sum(matched * logits)
    loss = total / total_pairs
    own_logits = lax.dynamic_slice_in_dim(logits, first_pair, group_caps, 1)
    own_col_lse = lax.dynamic_slice_in_dim(col_lse, first_pair, group_caps, 0)
    own_matched = lax.dynamic_slice_in_dim(matched, first_pair, group_caps, 1)
    grads16 = (
        LOSS_SCALE
        * (
            0.5 * jnp.exp(own_logits - row_lse[:, None])
            + 0.5 * jnp.exp(own_logits - own_col_lse[None, :])
            - own_matched
        )
    ).astype(jnp.bfloat16)
    grad_caps = SCALE * jnp.einsum(
        "ic,id->cd", grads16, images_all, preferred_element_type=jnp.float32
    )
    grad_pooled = inverse_len * (
        grad_caps - captions_unit * jnp.sum(captions_unit * grad_caps, -1, keepdims=True)
    )
    grad_result = (grad_pooled[:, None, :] * (present / counts)[:, :, None]).reshape(group_rows, D)
    grad_all = grad_result.astype(jnp.bfloat16)
    grad_fc2 = jnp.einsum("gf,gd->fd", active16, grad_all, preferred_element_type=jnp.float32)
    grad_active = jnp.einsum("gd,fd->gf", grad_all, txt_fc2, preferred_element_type=jnp.float32)
    grad_hidden16 = gelu_pull(grad_active)[0].astype(jnp.bfloat16)
    grad_fc1 = jnp.einsum(
        "gd,gf->df", normed2_all, grad_hidden16, preferred_element_type=jnp.float32
    )
    grad_fc1_bias = jnp.sum(grad_hidden16.astype(jnp.float32), 0)
    fc_sums = lax.psum(jnp.concatenate([grad_fc1, grad_fc2], 0).astype(jnp.bfloat16), "dp")
    grad_normed2 = reduce_exchanged(
        jnp.einsum("gf,df->gd", grad_hidden16, txt_fc1, preferred_element_type=jnp.float32), "mp"
    ).astype(jnp.float32)
    grad_middle = grad_result + norm_back(grad_normed2, unit2, inverse2, txt_gains[1])
    grad_mid_all = grad_middle.astype(jnp.bfloat16)
    grad_out = jnp.einsum("gw,gd->wd", context, grad_mid_all, preferred_element_type=jnp.float32)
    grad_context = jnp.einsum(
        "gd,wd->gw", grad_mid_all, txt_out, preferred_element_type=jnp.float32
    )
    grad_context = grad_context.astype(jnp.bfloat16).reshape(group_caps, L, head_count, HEAD)
    shares_again = jnp.exp(score_rows(queries, keys_all, keep) - log_totals)
    grad_shares = jnp.einsum(
        "nqhe,nkhe->nhqk", grad_context, values_all, preferred_element_type=jnp.float32
    )
    grad_values = jnp.einsum(
        "nhqk,nqhe->nkhe",
        shares_again.astype(jnp.bfloat16),
        grad_context,
        preferred_element_type=jnp.float32,
    ).astype(jnp.bfloat16)
    grad_scores = (
        shares_again * (grad_shares - jnp.sum(grad_shares * shares_again, -1, keepdims=True))
    ).astype(jnp.bfloat16)
    grad_queries = (
        jnp.einsum("nhqk,nkhe->nqhe", grad_scores, keys_all, preferred_element_type=jnp.float32)
        * 0.125
    ).astype(jnp.bfloat16)
    grad_keys = (
        jnp.einsum("nhqk,nqhe->nkhe", grad_scores, queries, preferred_element_type=jnp.float32)
        * 0.125
    ).astype(jnp.bfloat16)
    grad_triple = jnp.stack([grad_queries, grad_keys, grad_values], 0).reshape(3, group_rows, width)
    grad_qkv = jnp.einsum(
        "gd,jgw->jdw", normed1_all, grad_triple, preferred_element_type=jnp.float32
    )
    grad_qv_bias = jnp.stack(
        [
            jnp.sum(grad_triple[0].astype(jnp.float32), 0),
            jnp.sum(grad_triple[2].astype(jnp.float32), 0),
        ]
    )
    attn_sums = reduce_exchanged(jnp.concatenate([grad_qkv.reshape(-1, D), grad_out], 0), "dp")
    grad_normed1 = scatter_exchanged(
        jnp.einsum("jgw,jdw->gd", grad_triple, txt_qkv, preferred_element_type=jnp.float32), "mp"
    )

    def own(values):
        return lax.dynamic_slice_in_dim(values, mp_index * own_rows, own_rows, 0)

    unit1_own = own(unit1)
    grad_normed2_own = own(grad_normed2)
    unit2_own = own(unit2)
    grad_middle_own = own(grad_middle)
    grad_inputs = grad_middle_own + norm_back(grad_normed1, unit1_own, own(inverse1), txt_gains[0])
    small_parts = jnp.stack(
        [
            jnp.sum(grad_normed1 * unit1_own, 0),
            jnp.sum(grad_normed2_own * unit2_own, 0),
            jnp.sum(grad_normed1, 0),
            jnp.sum(grad_normed2_own, 0),
            jnp.sum(grad_middle_own, 0),
            jnp.sum(own(grad_result), 0),
        ]
    )
    bias_rows = jnp.stack(
        [jnp.concatenate([grad_qv_bias.reshape(-1), jnp.zeros_like(grad_qv_bias.reshape(-1))]), grad_fc1_bias]
    )
    shared = sum_exchanged(jnp.concatenate([sum_exchanged(small_parts, "mp"), bias_rows], 0), "dp")
    qv_count = grad_qv_bias.size
    fc1_rows = grad_fc1.shape[0]
    return (
        loss,
        grad_inputs,
        attn_sums[: grad_qkv.size // D].astype(jnp.float32).reshape(grad_qkv.shape),
        shared[6, :qv_count].reshape(grad_qv_bias.shape),
        attn_sums[grad_qkv.size // D :].astype(jnp.float32),
        fc_sums[:fc1_rows].astype(jnp.float32),
        shared[7],
        fc_sums[fc1_rows:].astype(jnp.float32),
        shared[0:2],
        shared[2:4],
        shared[4:6],
    )


def solution(mesh):
    placed = (
        P(("dp", "mp"), None),
        P("dp", None),
        P(),
        P(("dp", "mp"), None),
        P(("dp", "mp"), None),
        P(),
        P(None, None, "mp"),
        P("mp", None),
        P(None, "mp"),
        P("mp", None),
        P(None, None, "mp"),
        P(None, "mp"),
        P("mp", None),
        P(None, "mp"),
        P("mp"),
        P("mp", None),
        P(),
        P(),
        P(),
    )
    return jax.shard_map(
        local_body,
        mesh=mesh,
        in_specs=placed,
        out_specs=(
            P(),
            P(("dp", "mp"), None),
            P(None, None, "mp"),
            P(None, "mp"),
            P("mp", None),
            P(None, "mp"),
            P("mp"),
            P("mp", None),
            P(),
            P(),
            P(),
        ),
        check_vma=False,
    )
```

```python
import jax
import jax.numpy as jnp
from jax import lax
from jax.sharding import PartitionSpec as P

D = 768
HEAD = 64
L = 16
P_LOW = 50
P_HIGH = 145


EPS = 1e-06
SCALE = 40.0
LOSS_SCALE = 16.0
MASKED = -1e30


def layer_stats(values):
    center = values - jnp.mean(values, -1, keepdims=True)
    inverse = lax.rsqrt(jnp.mean(center * center, -1, keepdims=True) + EPS)
    return (center * inverse, inverse)


def norm_back(grad_out, unit, inverse, gain):
    scaled = grad_out * gain
    return inverse * (
        scaled
        - jnp.mean(scaled, -1, keepdims=True)
        - unit * jnp.mean(scaled * unit, -1, keepdims=True)
    )


def gelu_exact(values):
    return jax.nn.gelu(values, approximate=False)


def score_rows(queries, keys_all, keep):
    scores = (
        jnp.einsum("nqhe,nkhe->nhqk", queries, keys_all, preferred_element_type=jnp.float32) * 0.125
    )
    if keep is not None:
        scores = jnp.where(keep, scores, MASKED)
    return scores


def attention_shares(queries, keys_all, keep):
    scores = score_rows(queries, keys_all, keep)
    highest = jnp.max(scores, -1, keepdims=True)
    raised = jnp.exp(scores - highest)
    totals = jnp.sum(raised, -1, keepdims=True)
    return (raised / totals, highest + jnp.log(totals))


def axis_bits(axis):
    count = lax.axis_size(axis)
    bits = count.bit_length() - 1
    assert 1 << bits == count
    return count, list(reversed(range(bits)))


def exchange(values, axis, count, bit):
    return lax.ppermute(values, axis, [(i, i ^ (1 << bit)) for i in range(count)])


def gather_stacked(values, axis):
    count, bits = axis_bits(axis)
    data = values[None]
    for bit in bits:
        data = jnp.concatenate([data, exchange(data, axis, count, bit)], 0)
    return data


def gather_ordered(values, axis):
    count, bits = axis_bits(axis)
    index = lax.axis_index(axis)
    data = values
    done = []
    for bit in bits:
        other = exchange(data, axis, count, bit)
        upper = ((index >> bit) & 1) == 1
        data = jnp.stack([jnp.where(upper, other, data), jnp.where(upper, data, other)], 0)
        done.insert(0, bit)
    order = sorted(range(len(done)), key=lambda a: -done[a])
    data = data.transpose(order + list(range(len(done), data.ndim)))
    return data.reshape((count,) + values.shape)


def sum_exchanged(values, axis):
    count, bits = axis_bits(axis)
    for bit in reversed(bits):
        values = values + exchange(values, axis, count, bit)
    return values


def scatter_exchanged(values, axis):
    count, bits = axis_bits(axis)
    index = lax.axis_index(axis)
    data = values.reshape((2,) * len(bits) + (values.shape[0] // count,) + values.shape[1:])
    for bit in reversed(bits):
        place = len(bits) - 1 - bit
        mine = (index >> bit) & 1
        kept = lax.dynamic_index_in_dim(data, mine, place, keepdims=False)
        sent = lax.dynamic_index_in_dim(data, 1 - mine, place, keepdims=False)
        data = kept + exchange(sent.astype(jnp.bfloat16), axis, count, bit).astype(jnp.float32)
    return data


def reduce_exchanged(values, axis):
    part = scatter_exchanged(values, axis).astype(jnp.bfloat16)
    return gather_ordered(part, axis).reshape(values.shape)


def image_tower(tokens, count, length, gains, weights):
    w_qkv, w_out, w_fc1, w_fc2 = weights
    _, middle = image_attention(tokens, count, length, gains, w_qkv, w_out)
    return image_ffn(middle, count, length, gains, w_fc1, w_fc2)


def image_attention(tokens, count, length, gains, w_qkv, w_out):
    head_count = D // HEAD
    inputs = tokens.astype(jnp.float32)
    unit, _ = layer_stats(inputs)
    normed = (unit * gains[0]).astype(jnp.bfloat16)
    projected = jnp.einsum("rd,jdw->jrw", normed, w_qkv, preferred_element_type=jnp.float32).astype(
        jnp.bfloat16
    )
    shaped = projected.reshape(3, count, length, head_count, HEAD)
    shares, _ = attention_shares(shaped[0], shaped[1], None)
    context = jnp.einsum(
        "nhqk,nkhe->nqhe",
        shares.astype(jnp.bfloat16),
        shaped[2],
        preferred_element_type=jnp.float32,
    )
    context = context.astype(jnp.bfloat16).reshape(count * length, D)
    middle = inputs + jnp.dot(context, w_out, preferred_element_type=jnp.float32)
    return inputs, middle


def image_ffn(middle, count, length, gains, w_fc1, w_fc2):
    unit2, _ = layer_stats(middle)
    normed2 = (unit2 * gains[1]).astype(jnp.bfloat16)
    active = gelu_exact(jnp.dot(normed2, w_fc1, preferred_element_type=jnp.float32)).astype(
        jnp.bfloat16
    )
    result = middle + jnp.dot(active, w_fc2, preferred_element_type=jnp.float32)
    pooled = jnp.mean(result.reshape(count, length, D), 1)
    return (pooled * lax.rsqrt(jnp.sum(pooled * pooled, -1, keepdims=True) + EPS)).astype(
        jnp.bfloat16
    )


def local_body(
    text_in,
    caption_ids,
    pairing,
    image_low,
    image_high,
    img_gains,
    img_qkv,
    img_out,
    img_fc1,
    img_fc2,
    txt_qkv,
    txt_qv_bias,
    txt_out,
    txt_fc1,
    txt_fc1_bias,
    txt_fc2,
    txt_gains,
    txt_shifts,
    txt_biases,
):
    qkv_parts = gather_stacked(img_qkv, "mp")
    out_parts = gather_stacked(img_out, "mp")
    qkv_parts, out_parts, fc1_local, fc2_local = lax.optimization_barrier(
        (qkv_parts, out_parts, img_fc1, img_fc2)
    )
    fc1_parts = gather_stacked(fc1_local, "mp")
    weights = (
        qkv_parts.transpose(1, 2, 0, 3).reshape(3, D, -1),
        out_parts.reshape(-1, D),
        fc1_parts.transpose(1, 0, 2).reshape(D, -1),
        gather_stacked(fc2_local, "mp").reshape(-1, D),
    )
    low_count = image_low.shape[0] // P_LOW
    high_count = image_high.shape[0] // P_HIGH
    images16 = jnp.concatenate(
        [
            image_tower(image_low, low_count, P_LOW, img_gains, weights),
            image_tower(image_high, high_count, P_HIGH, img_gains, weights),
        ],
        0,
    )
    width = txt_qkv.shape[2]
    head_count = width // HEAD
    own_rows = text_in.shape[0]
    own_caps = own_rows // L
    group_caps = caption_ids.shape[0]
    group_rows = group_caps * L
    mp_index = lax.axis_index("mp")
    present = (caption_ids > 0).astype(jnp.float32)
    keep = (caption_ids > 0)[:, None, None, :]
    counts = jnp.sum(present, 1, keepdims=True)
    inputs = lax.all_gather(text_in, "mp", axis=0, tiled=True).astype(jnp.float32)
    unit1, inverse1 = layer_stats(inputs)
    normed1_all = (unit1 * txt_gains[0] + txt_shifts[0]).astype(jnp.bfloat16)
    bias_rows = jnp.stack([txt_qv_bias[0], jnp.zeros_like(txt_qv_bias[0]), txt_qv_bias[1]])
    made = (
        jnp.einsum("rd,jdw->rjw", normed1_all, txt_qkv, preferred_element_type=jnp.float32)
        + bias_rows
    )
    triple = made.astype(jnp.bfloat16).reshape(group_caps, L, 3, head_count, HEAD)
    queries = triple[:, :, 0]
    keys_all = triple[:, :, 1]
    values_all = triple[:, :, 2]
    shares, log_totals = attention_shares(queries, keys_all, keep)
    context = jnp.einsum(
        "nhqk,nkhe->nqhe",
        shares.astype(jnp.bfloat16),
        values_all,
        preferred_element_type=jnp.float32,
    )
    context = context.astype(jnp.bfloat16).reshape(group_rows, width)
    middle = inputs + (
        lax.psum(
            jnp.dot(context, txt_out, preferred_element_type=jnp.float32).astype(jnp.bfloat16),
            "mp",
        ).astype(jnp.float32)
        + txt_biases[0]
    )
    unit2, inverse2 = layer_stats(middle)
    normed2_all = (unit2 * txt_gains[1] + txt_shifts[1]).astype(jnp.bfloat16)
    hidden = jnp.dot(normed2_all, txt_fc1, preferred_element_type=jnp.float32) + txt_fc1_bias
    active, gelu_pull = jax.vjp(gelu_exact, hidden)
    active16 = active.astype(jnp.bfloat16)
    ffn_part = jnp.dot(active16, txt_fc2, preferred_element_type=jnp.float32)
    ffn_pooled = jnp.sum(ffn_part.reshape(group_caps, L, D) * present[:, :, None], 1)
    image_slots = lax.dynamic_update_slice_in_dim(
        jnp.zeros((group_caps, D), jnp.float32),
        images16.astype(jnp.float32),
        mp_index * own_caps,
        0,
    )
    both = sum_exchanged(jnp.concatenate([ffn_pooled, image_slots], 0), "mp")
    mid_pooled = jnp.sum(middle.reshape(group_caps, L, D) * present[:, :, None], 1)
    pooled = (mid_pooled + both[:group_caps]) / counts + txt_biases[1]
    inverse_len = lax.rsqrt(jnp.sum(pooled * pooled, -1, keepdims=True) + EPS)
    captions_unit = pooled * inverse_len
    captions16 = captions_unit.astype(jnp.bfloat16)
    gathered = gather_ordered(
        jnp.concatenate([captions16, both[group_caps:].astype(jnp.bfloat16)], 0), "dp"
    )
    arrived = gathered[:, :group_caps].reshape(-1, D)
    images_all = gathered[:, group_caps:].reshape(-1, D)
    total_pairs = pairing.shape[0]
    first_pair = lax.axis_index("dp") * group_caps
    logits = SCALE * jnp.einsum("id,jd->ij", images_all, arrived, preferred_element_type=jnp.float32)
    matched = (pairing[:, None] == jnp.arange(total_pairs)[None, :]).astype(jnp.float32)
    raised = jnp.exp(logits - SCALE)
    row_lse = SCALE + jnp.log(jnp.sum(raised, 1))
    col_lse = SCALE + jnp.log(jnp.sum(raised, 0))
    total = 0.5 * jnp.sum(row_lse) + 0.5 * jnp.sum(col_lse) - jnp.sum(matched * logits)
    loss = total / total_pairs
    own_logits = lax.dynamic_slice_in_dim(logits, first_pair, group_caps, 1)
    own_col_lse = lax.dynamic_slice_in_dim(col_lse, first_pair, group_caps, 0)
    own_matched = lax.dynamic_slice_in_dim(matched, first_pair, group_caps, 1)
    grads16 = (
        LOSS_SCALE
        * (
            0.5 * jnp.exp(own_logits - row_lse[:, None])
            + 0.5 * jnp.exp(own_logits - own_col_lse[None, :])
            - own_matched
        )
    ).astype(jnp.bfloat16)
    grad_caps = SCALE * jnp.einsum(
        "ic,id->cd", grads16, images_all, preferred_element_type=jnp.float32
    )
    grad_pooled = inverse_len * (
        grad_caps - captions_unit * jnp.sum(captions_unit * grad_caps, -1, keepdims=True)
    )
    grad_result = (grad_pooled[:, None, :] * (present / counts)[:, :, None]).reshape(group_rows, D)
    grad_all = grad_result.astype(jnp.bfloat16)
    grad_fc2 = jnp.einsum("gf,gd->fd", active16, grad_all, preferred_element_type=jnp.float32)
    grad_active = jnp.einsum("gd,fd->gf", grad_all, txt_fc2, preferred_element_type=jnp.float32)
    grad_hidden16 = gelu_pull(grad_active)[0].astype(jnp.bfloat16)
    grad_fc1 = jnp.einsum(
        "gd,gf->df", normed2_all, grad_hidden16, preferred_element_type=jnp.float32
    )
    grad_fc1_bias = jnp.sum(grad_hidden16.astype(jnp.float32), 0)
    fc_sums = lax.psum(jnp.concatenate([grad_fc1, grad_fc2], 0).astype(jnp.bfloat16), "dp")
    grad_normed2 = reduce_exchanged(
        jnp.einsum("gf,df->gd", grad_hidden16, txt_fc1, preferred_element_type=jnp.float32), "mp"
    ).astype(jnp.float32)
    grad_middle = grad_result + norm_back(grad_normed2, unit2, inverse2, txt_gains[1])
    grad_mid_all = grad_middle.astype(jnp.bfloat16)
    grad_out = jnp.einsum("gw,gd->wd", context, grad_mid_all, preferred_element_type=jnp.float32)
    grad_context = jnp.einsum(
        "gd,wd->gw", grad_mid_all, txt_out, preferred_element_type=jnp.float32
    )
    grad_context = grad_context.astype(jnp.bfloat16).reshape(group_caps, L, head_count, HEAD)
    shares_again = jnp.exp(score_rows(queries, keys_all, keep) - log_totals)
    grad_shares = jnp.einsum(
        "nqhe,nkhe->nhqk", grad_context, values_all, preferred_element_type=jnp.float32
    )
    grad_values = jnp.einsum(
        "nhqk,nqhe->nkhe",
        shares_again.astype(jnp.bfloat16),
        grad_context,
        preferred_element_type=jnp.float32,
    ).astype(jnp.bfloat16)
    grad_scores = (
        shares_again * (grad_shares - jnp.sum(grad_shares * shares_again, -1, keepdims=True))
    ).astype(jnp.bfloat16)
    grad_queries = (
        jnp.einsum("nhqk,nkhe->nqhe", grad_scores, keys_all, preferred_element_type=jnp.float32)
        * 0.125
    ).astype(jnp.bfloat16)
    grad_keys = (
        jnp.einsum("nhqk,nqhe->nkhe", grad_scores, queries, preferred_element_type=jnp.float32)
        * 0.125
    ).astype(jnp.bfloat16)
    grad_triple = jnp.stack([grad_queries, grad_keys, grad_values], 0).reshape(3, group_rows, width)
    grad_qkv = jnp.einsum(
        "gd,jgw->jdw", normed1_all, grad_triple, preferred_element_type=jnp.float32
    )
    grad_qv_bias = jnp.stack(
        [
            jnp.sum(grad_triple[0].astype(jnp.float32), 0),
            jnp.sum(grad_triple[2].astype(jnp.float32), 0),
        ]
    )
    attn_sums = reduce_exchanged(jnp.concatenate([grad_qkv.reshape(-1, D), grad_out], 0), "dp")
    grad_normed1 = scatter_exchanged(
        jnp.einsum("jgw,jdw->gd", grad_triple, txt_qkv, preferred_element_type=jnp.float32), "mp"
    )

    def own(values):
        return lax.dynamic_slice_in_dim(values, mp_index * own_rows, own_rows, 0)

    unit1_own = own(unit1)
    grad_normed2_own = own(grad_normed2)
    unit2_own = own(unit2)
    grad_middle_own = own(grad_middle)
    grad_inputs = grad_middle_own + norm_back(grad_normed1, unit1_own, own(inverse1), txt_gains[0])
    small_parts = jnp.stack(
        [
            jnp.sum(grad_normed1 * unit1_own, 0),
            jnp.sum(grad_normed2_own * unit2_own, 0),
            jnp.sum(grad_normed1, 0),
            jnp.sum(grad_normed2_own, 0),
            jnp.sum(grad_middle_own, 0),
            jnp.sum(own(grad_result), 0),
        ]
    )
    bias_rows = jnp.stack(
        [jnp.concatenate([grad_qv_bias.reshape(-1), jnp.zeros_like(grad_qv_bias.reshape(-1))]), grad_fc1_bias]
    )
    shared = sum_exchanged(jnp.concatenate([sum_exchanged(small_parts, "mp"), bias_rows], 0), "dp")
    qv_count = grad_qv_bias.size
    fc1_rows = grad_fc1.shape[0]
    return (
        loss,
        grad_inputs,
        attn_sums[: grad_qkv.size // D].astype(jnp.float32).reshape(grad_qkv.shape),
        shared[6, :qv_count].reshape(grad_qv_bias.shape),
        attn_sums[grad_qkv.size // D :].astype(jnp.float32),
        fc_sums[:fc1_rows].astype(jnp.float32),
        shared[7],
        fc_sums[fc1_rows:].astype(jnp.float32),
        shared[0:2],
        shared[2:4],
        shared[4:6],
    )


def solution(mesh):
    placed = (
        P(("dp", "mp"), None),
        P("dp", None),
        P(),
        P(("dp", "mp"), None),
        P(("dp", "mp"), None),
        P(),
        P(None, None, "mp"),
        P("mp", None),
        P(None, "mp"),
        P("mp", None),
        P(None, None, "mp"),
        P(None, "mp"),
        P("mp", None),
        P(None, "mp"),
        P("mp"),
        P("mp", None),
        P(),
        P(),
        P(),
    )
    return jax.shard_map(
        local_body,
        mesh=mesh,
        in_specs=placed,
        out_specs=(
            P(),
            P(("dp", "mp"), None),
            P(None, None, "mp"),
            P(None, "mp"),
            P("mp", None),
            P(None, "mp"),
            P("mp"),
            P("mp", None),
            P(),
            P(),
            P(),
        ),
        check_vma=False,
    )
```

```python
import jax
import jax.numpy as jnp
from jax import lax
from jax.sharding import PartitionSpec as P

D = 768
HEAD = 64
L = 16
P_LOW = 50
P_HIGH = 145


EPS = 1e-06
SCALE = 40.0
LOSS_SCALE = 16.0
MASKED = -1e30


def layer_stats(values):
    center = values - jnp.mean(values, -1, keepdims=True)
    inverse = lax.rsqrt(jnp.mean(center * center, -1, keepdims=True) + EPS)
    return (center * inverse, inverse)


def norm_back(grad_out, unit, inverse, gain):
    scaled = grad_out * gain
    return inverse * (
        scaled
        - jnp.mean(scaled, -1, keepdims=True)
        - unit * jnp.mean(scaled * unit, -1, keepdims=True)
    )


def gelu_exact(values):
    return jax.nn.gelu(values, approximate=False)


def score_rows(queries, keys_all, keep):
    scores = (
        jnp.einsum("nqhe,nkhe->nhqk", queries, keys_all, preferred_element_type=jnp.float32) * 0.125
    )
    if keep is not None:
        scores = jnp.where(keep, scores, MASKED)
    return scores


def attention_shares(queries, keys_all, keep):
    scores = score_rows(queries, keys_all, keep)
    highest = jnp.max(scores, -1, keepdims=True)
    raised = jnp.exp(scores - highest)
    totals = jnp.sum(raised, -1, keepdims=True)
    return (raised / totals, highest + jnp.log(totals))


def axis_bits(axis):
    count = lax.axis_size(axis)
    bits = count.bit_length() - 1
    assert 1 << bits == count
    return count, list(reversed(range(bits)))


def exchange(values, axis, count, bit):
    return lax.ppermute(values, axis, [(i, i ^ (1 << bit)) for i in range(count)])


def gather_stacked(values, axis):
    count, bits = axis_bits(axis)
    data = values[None]
    for bit in bits:
        data = jnp.concatenate([data, exchange(data, axis, count, bit)], 0)
    return data


def gather_ordered(values, axis):
    count, bits = axis_bits(axis)
    index = lax.axis_index(axis)
    data = values
    done = []
    for bit in bits:
        other = exchange(data, axis, count, bit)
        upper = ((index >> bit) & 1) == 1
        data = jnp.stack([jnp.where(upper, other, data), jnp.where(upper, data, other)], 0)
        done.insert(0, bit)
    order = sorted(range(len(done)), key=lambda a: -done[a])
    data = data.transpose(order + list(range(len(done), data.ndim)))
    return data.reshape((count,) + values.shape)


def sum_exchanged(values, axis):
    count, bits = axis_bits(axis)
    for bit in reversed(bits):
        values = values + exchange(values, axis, count, bit)
    return values


def scatter_exchanged(values, axis):
    count, bits = axis_bits(axis)
    index = lax.axis_index(axis)
    data = values.reshape((2,) * len(bits) + (values.shape[0] // count,) + values.shape[1:])
    for bit in reversed(bits):
        place = len(bits) - 1 - bit
        mine = (index >> bit) & 1
        kept = lax.dynamic_index_in_dim(data, mine, place, keepdims=False)
        sent = lax.dynamic_index_in_dim(data, 1 - mine, place, keepdims=False)
        data = kept + exchange(sent.astype(jnp.bfloat16), axis, count, bit).astype(jnp.float32)
    return data


def reduce_exchanged(values, axis):
    part = scatter_exchanged(values, axis).astype(jnp.bfloat16)
    return gather_ordered(part, axis).reshape(values.shape)


def image_tower(tokens, count, length, gains, weights):
    w_qkv, w_out, w_fc1, w_fc2 = weights
    _, middle = image_attention(tokens, count, length, gains, w_qkv, w_out)
    return image_ffn(middle, count, length, gains, w_fc1, w_fc2)


def image_attention(tokens, count, length, gains, w_qkv, w_out):
    head_count = D // HEAD
    inputs = tokens.astype(jnp.float32)
    unit, _ = layer_stats(inputs)
    normed = (unit * gains[0]).astype(jnp.bfloat16)
    projected = jnp.einsum("rd,jdw->jrw", normed, w_qkv, preferred_element_type=jnp.float32).astype(
        jnp.bfloat16
    )
    shaped = projected.reshape(3, count, length, head_count, HEAD)
    shares, _ = attention_shares(shaped[0], shaped[1], None)
    context = jnp.einsum(
        "nhqk,nkhe->nqhe",
        shares.astype(jnp.bfloat16),
        shaped[2],
        preferred_element_type=jnp.float32,
    )
    context = context.astype(jnp.bfloat16).reshape(count * length, D)
    middle = inputs + jnp.dot(context, w_out, preferred_element_type=jnp.float32)
    return inputs, middle


def image_ffn(middle, count, length, gains, w_fc1, w_fc2):
    unit2, _ = layer_stats(middle)
    normed2 = (unit2 * gains[1]).astype(jnp.bfloat16)
    active = gelu_exact(jnp.dot(normed2, w_fc1, preferred_element_type=jnp.float32)).astype(
        jnp.bfloat16
    )
    result = middle + jnp.dot(active, w_fc2, preferred_element_type=jnp.float32)
    pooled = jnp.mean(result.reshape(count, length, D), 1)
    return (pooled * lax.rsqrt(jnp.sum(pooled * pooled, -1, keepdims=True) + EPS)).astype(
        jnp.bfloat16
    )


def local_body(
    text_in,
    caption_ids,
    pairing,
    image_low,
    image_high,
    img_gains,
    img_qkv,
    img_out,
    img_fc1,
    img_fc2,
    txt_qkv,
    txt_qv_bias,
    txt_out,
    txt_fc1,
    txt_fc1_bias,
    txt_fc2,
    txt_gains,
    txt_shifts,
    txt_biases,
):
    qkv_parts = gather_stacked(img_qkv, "mp")
    fc1_parts = gather_stacked(img_fc1, "mp")
    weights = (
        qkv_parts.transpose(1, 2, 0, 3).reshape(3, D, -1),
        gather_stacked(img_out, "mp").reshape(-1, D),
        fc1_parts.transpose(1, 0, 2).reshape(D, -1),
        gather_stacked(img_fc2, "mp").reshape(-1, D),
    )
    low_count = image_low.shape[0] // P_LOW
    high_count = image_high.shape[0] // P_HIGH
    images16 = jnp.concatenate(
        [
            image_tower(image_low, low_count, P_LOW, img_gains, weights),
            image_tower(image_high, high_count, P_HIGH, img_gains, weights),
        ],
        0,
    )
    width = txt_qkv.shape[2]
    head_count = width // HEAD
    own_rows = text_in.shape[0]
    own_caps = own_rows // L
    group_caps = caption_ids.shape[0]
    group_rows = group_caps * L
    mp_index = lax.axis_index("mp")
    present = (caption_ids > 0).astype(jnp.float32)
    keep = (caption_ids > 0)[:, None, None, :]
    counts = jnp.sum(present, 1, keepdims=True)
    inputs = gather_ordered(text_in, "mp").reshape(-1, D).astype(jnp.float32)
    unit1, inverse1 = layer_stats(inputs)
    normed1_all = (unit1 * txt_gains[0] + txt_shifts[0]).astype(jnp.bfloat16)
    bias_rows = jnp.stack([txt_qv_bias[0], jnp.zeros_like(txt_qv_bias[0]), txt_qv_bias[1]])
    made = (
        jnp.einsum("rd,jdw->rjw", normed1_all, txt_qkv, preferred_element_type=jnp.float32)
        + bias_rows
    )
    triple = made.astype(jnp.bfloat16).reshape(group_caps, L, 3, head_count, HEAD)
    queries = triple[:, :, 0]
    keys_all = triple[:, :, 1]
    values_all = triple[:, :, 2]
    shares, log_totals = attention_shares(queries, keys_all, keep)
    context = jnp.einsum(
        "nhqk,nkhe->nqhe",
        shares.astype(jnp.bfloat16),
        values_all,
        preferred_element_type=jnp.float32,
    )
    context = context.astype(jnp.bfloat16).reshape(group_rows, width)
    middle = inputs + (
        lax.psum(
            jnp.dot(context, txt_out, preferred_element_type=jnp.float32).astype(jnp.bfloat16),
            "mp",
        ).astype(jnp.float32)
        + txt_biases[0]
    )
    unit2, inverse2 = layer_stats(middle)
    normed2_all = (unit2 * txt_gains[1] + txt_shifts[1]).astype(jnp.bfloat16)
    hidden = jnp.dot(normed2_all, txt_fc1, preferred_element_type=jnp.float32) + txt_fc1_bias
    active, gelu_pull = jax.vjp(gelu_exact, hidden)
    active16 = active.astype(jnp.bfloat16)
    ffn_part = jnp.dot(active16, txt_fc2, preferred_element_type=jnp.float32)
    ffn_pooled = jnp.sum(ffn_part.reshape(group_caps, L, D) * present[:, :, None], 1)
    image_slots = lax.dynamic_update_slice_in_dim(
        jnp.zeros((group_caps, D), jnp.float32),
        images16.astype(jnp.float32),
        mp_index * own_caps,
        0,
    )
    images_all = gather_ordered(
        sum_exchanged(image_slots.astype(jnp.bfloat16), "mp"), "dp"
    ).reshape(-1, D)
    ffn_sum = sum_exchanged(ffn_pooled, "mp")
    mid_pooled = jnp.sum(middle.reshape(group_caps, L, D) * present[:, :, None], 1)
    pooled = (mid_pooled + ffn_sum) / counts + txt_biases[1]
    inverse_len = lax.rsqrt(jnp.sum(pooled * pooled, -1, keepdims=True) + EPS)
    captions_unit = pooled * inverse_len
    captions16 = captions_unit.astype(jnp.bfloat16)
    arrived = gather_ordered(captions16, "dp").reshape(-1, D)
    total_pairs = pairing.shape[0]
    first_pair = lax.axis_index("dp") * group_caps
    logits = SCALE * jnp.einsum("id,jd->ij", images_all, arrived, preferred_element_type=jnp.float32)
    matched = (pairing[:, None] == jnp.arange(total_pairs)[None, :]).astype(jnp.float32)
    raised = jnp.exp(logits - SCALE)
    row_lse = SCALE + jnp.log(jnp.sum(raised, 1))
    col_lse = SCALE + jnp.log(jnp.sum(raised, 0))
    total = 0.5 * jnp.sum(row_lse) + 0.5 * jnp.sum(col_lse) - jnp.sum(matched * logits)
    loss = total / total_pairs
    own_logits = lax.dynamic_slice_in_dim(logits, first_pair, group_caps, 1)
    own_col_lse = lax.dynamic_slice_in_dim(col_lse, first_pair, group_caps, 0)
    own_matched = lax.dynamic_slice_in_dim(matched, first_pair, group_caps, 1)
    grads16 = (
        LOSS_SCALE
        * (
            0.5 * jnp.exp(own_logits - row_lse[:, None])
            + 0.5 * jnp.exp(own_logits - own_col_lse[None, :])
            - own_matched
        )
    ).astype(jnp.bfloat16)
    grad_caps = SCALE * jnp.einsum(
        "ic,id->cd", grads16, images_all, preferred_element_type=jnp.float32
    )
    grad_pooled = inverse_len * (
        grad_caps - captions_unit * jnp.sum(captions_unit * grad_caps, -1, keepdims=True)
    )
    grad_result = (grad_pooled[:, None, :] * (present / counts)[:, :, None]).reshape(group_rows, D)
    grad_all = grad_result.astype(jnp.bfloat16)
    grad_fc2 = jnp.einsum("gf,gd->fd", active16, grad_all, preferred_element_type=jnp.float32)
    grad_active = jnp.einsum("gd,fd->gf", grad_all, txt_fc2, preferred_element_type=jnp.float32)
    grad_hidden16 = gelu_pull(grad_active)[0].astype(jnp.bfloat16)
    grad_fc1 = jnp.einsum(
        "gd,gf->df", normed2_all, grad_hidden16, preferred_element_type=jnp.float32
    )
    grad_fc1_bias = jnp.sum(grad_hidden16.astype(jnp.float32), 0)
    fc_sums = lax.psum(jnp.concatenate([grad_fc1, grad_fc2], 0).astype(jnp.bfloat16), "dp")
    grad_normed2 = reduce_exchanged(
        jnp.einsum("gf,df->gd", grad_hidden16, txt_fc1, preferred_element_type=jnp.float32), "mp"
    ).astype(jnp.float32)
    grad_middle = grad_result + norm_back(grad_normed2, unit2, inverse2, txt_gains[1])
    grad_mid_all = grad_middle.astype(jnp.bfloat16)
    grad_out = jnp.einsum("gw,gd->wd", context, grad_mid_all, preferred_element_type=jnp.float32)
    grad_context = jnp.einsum(
        "gd,wd->gw", grad_mid_all, txt_out, preferred_element_type=jnp.float32
    )
    grad_context = grad_context.astype(jnp.bfloat16).reshape(group_caps, L, head_count, HEAD)
    shares_again = jnp.exp(score_rows(queries, keys_all, keep) - log_totals)
    grad_shares = jnp.einsum(
        "nqhe,nkhe->nhqk", grad_context, values_all, preferred_element_type=jnp.float32
    )
    grad_values = jnp.einsum(
        "nhqk,nqhe->nkhe",
        shares_again.astype(jnp.bfloat16),
        grad_context,
        preferred_element_type=jnp.float32,
    ).astype(jnp.bfloat16)
    grad_scores = (
        shares_again * (grad_shares - jnp.sum(grad_shares * shares_again, -1, keepdims=True))
    ).astype(jnp.bfloat16)
    grad_queries = (
        jnp.einsum("nhqk,nkhe->nqhe", grad_scores, keys_all, preferred_element_type=jnp.float32)
        * 0.125
    ).astype(jnp.bfloat16)
    grad_keys = (
        jnp.einsum("nhqk,nqhe->nkhe", grad_scores, queries, preferred_element_type=jnp.float32)
        * 0.125
    ).astype(jnp.bfloat16)
    grad_triple = jnp.stack([grad_queries, grad_keys, grad_values], 0).reshape(3, group_rows, width)
    grad_qkv = jnp.einsum(
        "gd,jgw->jdw", normed1_all, grad_triple, preferred_element_type=jnp.float32
    )
    grad_qv_bias = jnp.stack(
        [
            jnp.sum(grad_triple[0].astype(jnp.float32), 0),
            jnp.sum(grad_triple[2].astype(jnp.float32), 0),
        ]
    )
    attn_sums = reduce_exchanged(jnp.concatenate([grad_qkv.reshape(-1, D), grad_out], 0), "dp")
    grad_normed1 = scatter_exchanged(
        jnp.einsum("jgw,jdw->gd", grad_triple, txt_qkv, preferred_element_type=jnp.float32), "mp"
    )

    def own(values):
        return lax.dynamic_slice_in_dim(values, mp_index * own_rows, own_rows, 0)

    unit1_own = own(unit1)
    grad_normed2_own = own(grad_normed2)
    unit2_own = own(unit2)
    grad_middle_own = own(grad_middle)
    grad_inputs = grad_middle_own + norm_back(grad_normed1, unit1_own, own(inverse1), txt_gains[0])
    small_parts = jnp.stack(
        [
            jnp.sum(grad_normed1 * unit1_own, 0),
            jnp.sum(grad_normed2_own * unit2_own, 0),
            jnp.sum(grad_normed1, 0),
            jnp.sum(grad_normed2_own, 0),
            jnp.sum(grad_middle_own, 0),
            jnp.sum(own(grad_result), 0),
        ]
    )
    bias_rows = jnp.stack(
        [jnp.concatenate([grad_qv_bias.reshape(-1), jnp.zeros_like(grad_qv_bias.reshape(-1))]), grad_fc1_bias]
    )
    shared = sum_exchanged(jnp.concatenate([sum_exchanged(small_parts, "mp"), bias_rows], 0), "dp")
    qv_count = grad_qv_bias.size
    fc1_rows = grad_fc1.shape[0]
    return (
        loss,
        grad_inputs,
        attn_sums[: grad_qkv.size // D].astype(jnp.float32).reshape(grad_qkv.shape),
        shared[6, :qv_count].reshape(grad_qv_bias.shape),
        attn_sums[grad_qkv.size // D :].astype(jnp.float32),
        fc_sums[:fc1_rows].astype(jnp.float32),
        shared[7],
        fc_sums[fc1_rows:].astype(jnp.float32),
        shared[0:2],
        shared[2:4],
        shared[4:6],
    )


def solution(mesh):
    placed = (
        P(("dp", "mp"), None),
        P("dp", None),
        P(),
        P(("dp", "mp"), None),
        P(("dp", "mp"), None),
        P(),
        P(None, None, "mp"),
        P("mp", None),
        P(None, "mp"),
        P("mp", None),
        P(None, None, "mp"),
        P(None, "mp"),
        P("mp", None),
        P(None, "mp"),
        P("mp"),
        P("mp", None),
        P(),
        P(),
        P(),
    )
    return jax.shard_map(
        local_body,
        mesh=mesh,
        in_specs=placed,
        out_specs=(
            P(),
            P(("dp", "mp"), None),
            P(None, None, "mp"),
            P(None, "mp"),
            P("mp", None),
            P(None, "mp"),
            P("mp"),
            P("mp", None),
            P(),
            P(),
            P(),
        ),
        check_vma=False,
    )
```

```python
import jax
import jax.numpy as jnp
from jax import lax
from jax.sharding import PartitionSpec as P

D = 768
HEAD = 64
L = 16
P_LOW = 50
P_HIGH = 145


EPS = 1e-06
SCALE = 40.0
LOSS_SCALE = 16.0
MASKED = -1e30


def layer_stats(values):
    center = values - jnp.mean(values, -1, keepdims=True)
    inverse = lax.rsqrt(jnp.mean(center * center, -1, keepdims=True) + EPS)
    return (center * inverse, inverse)


def norm_back(grad_out, unit, inverse, gain):
    scaled = grad_out * gain
    return inverse * (
        scaled
        - jnp.mean(scaled, -1, keepdims=True)
        - unit * jnp.mean(scaled * unit, -1, keepdims=True)
    )


def gelu_exact(values):
    return jax.nn.gelu(values, approximate=False)


def score_rows(queries, keys_all, keep):
    scores = (
        jnp.einsum("nqhe,nkhe->nhqk", queries, keys_all, preferred_element_type=jnp.float32) * 0.125
    )
    if keep is not None:
        scores = jnp.where(keep, scores, MASKED)
    return scores


def attention_shares(queries, keys_all, keep):
    scores = score_rows(queries, keys_all, keep)
    highest = jnp.max(scores, -1, keepdims=True)
    raised = jnp.exp(scores - highest)
    totals = jnp.sum(raised, -1, keepdims=True)
    return (raised / totals, highest + jnp.log(totals))


def axis_bits(axis):
    count = lax.axis_size(axis)
    bits = count.bit_length() - 1
    assert 1 << bits == count
    return count, list(reversed(range(bits)))


def exchange(values, axis, count, bit):
    return lax.ppermute(values, axis, [(i, i ^ (1 << bit)) for i in range(count)])


def gather_stacked(values, axis):
    count, bits = axis_bits(axis)
    data = values[None]
    for bit in bits:
        data = jnp.concatenate([data, exchange(data, axis, count, bit)], 0)
    return data


def gather_ordered(values, axis):
    count, bits = axis_bits(axis)
    index = lax.axis_index(axis)
    data = values
    done = []
    for bit in bits:
        other = exchange(data, axis, count, bit)
        upper = ((index >> bit) & 1) == 1
        data = jnp.stack([jnp.where(upper, other, data), jnp.where(upper, data, other)], 0)
        done.insert(0, bit)
    order = sorted(range(len(done)), key=lambda a: -done[a])
    data = data.transpose(order + list(range(len(done), data.ndim)))
    return data.reshape((count,) + values.shape)


def sum_exchanged(values, axis):
    count, bits = axis_bits(axis)
    for bit in reversed(bits):
        values = values + exchange(values, axis, count, bit)
    return values


def scatter_exchanged(values, axis):
    count, bits = axis_bits(axis)
    index = lax.axis_index(axis)
    data = values.reshape((2,) * len(bits) + (values.shape[0] // count,) + values.shape[1:])
    for bit in reversed(bits):
        place = len(bits) - 1 - bit
        mine = (index >> bit) & 1
        kept = lax.dynamic_index_in_dim(data, mine, place, keepdims=False)
        sent = lax.dynamic_index_in_dim(data, 1 - mine, place, keepdims=False)
        data = kept + exchange(sent.astype(jnp.bfloat16), axis, count, bit).astype(jnp.float32)
    return data


def reduce_exchanged(values, axis):
    part = scatter_exchanged(values, axis).astype(jnp.bfloat16)
    return gather_ordered(part, axis).reshape(values.shape)


def image_tower(tokens, count, length, gains, weights):
    w_qkv, w_out, w_fc1, w_fc2 = weights
    _, middle = image_attention(tokens, count, length, gains, w_qkv, w_out)
    return image_ffn(middle, count, length, gains, w_fc1, w_fc2)


def image_attention(tokens, count, length, gains, w_qkv, w_out):
    head_count = D // HEAD
    inputs = tokens.astype(jnp.float32)
    unit, _ = layer_stats(inputs)
    normed = (unit * gains[0]).astype(jnp.bfloat16)
    projected = jnp.einsum("rd,jdw->jrw", normed, w_qkv, preferred_element_type=jnp.float32).astype(
        jnp.bfloat16
    )
    shaped = projected.reshape(3, count, length, head_count, HEAD)
    shares, _ = attention_shares(shaped[0], shaped[1], None)
    context = jnp.einsum(
        "nhqk,nkhe->nqhe",
        shares.astype(jnp.bfloat16),
        shaped[2],
        preferred_element_type=jnp.float32,
    )
    context = context.astype(jnp.bfloat16).reshape(count * length, D)
    middle = inputs + jnp.dot(context, w_out, preferred_element_type=jnp.float32)
    return inputs, middle


def image_ffn(middle, count, length, gains, w_fc1, w_fc2):
    unit2, _ = layer_stats(middle)
    normed2 = (unit2 * gains[1]).astype(jnp.bfloat16)
    active = gelu_exact(jnp.dot(normed2, w_fc1, preferred_element_type=jnp.float32)).astype(
        jnp.bfloat16
    )
    result = middle + jnp.dot(active, w_fc2, preferred_element_type=jnp.float32)
    pooled = jnp.mean(result.reshape(count, length, D), 1)
    return (pooled * lax.rsqrt(jnp.sum(pooled * pooled, -1, keepdims=True) + EPS)).astype(
        jnp.bfloat16
    )


def local_body(
    text_in,
    caption_ids,
    pairing,
    image_low,
    image_high,
    img_gains,
    img_qkv,
    img_out,
    img_fc1,
    img_fc2,
    txt_qkv,
    txt_qv_bias,
    txt_out,
    txt_fc1,
    txt_fc1_bias,
    txt_fc2,
    txt_gains,
    txt_shifts,
    txt_biases,
):
    qkv_parts = gather_stacked(img_qkv, "mp")
    fc1_parts = gather_stacked(img_fc1, "mp")
    weights = (
        qkv_parts.transpose(1, 2, 0, 3).reshape(3, D, -1),
        gather_stacked(img_out, "mp").reshape(-1, D),
        fc1_parts.transpose(1, 0, 2).reshape(D, -1),
        gather_stacked(img_fc2, "mp").reshape(-1, D),
    )
    low_count = image_low.shape[0] // P_LOW
    high_count = image_high.shape[0] // P_HIGH
    images16 = jnp.concatenate(
        [
            image_tower(image_low, low_count, P_LOW, img_gains, weights),
            image_tower(image_high, high_count, P_HIGH, img_gains, weights),
        ],
        0,
    )
    width = txt_qkv.shape[2]
    head_count = width // HEAD
    own_rows = text_in.shape[0]
    own_caps = own_rows // L
    group_caps = caption_ids.shape[0]
    group_rows = group_caps * L
    mp_index = lax.axis_index("mp")
    present = (caption_ids > 0).astype(jnp.float32)
    keep = (caption_ids > 0)[:, None, None, :]
    counts = jnp.sum(present, 1, keepdims=True)
    inputs = lax.all_gather(text_in, "mp", axis=0, tiled=True).astype(jnp.float32)
    unit1, inverse1 = layer_stats(inputs)
    normed1_all = (unit1 * txt_gains[0] + txt_shifts[0]).astype(jnp.bfloat16)
    bias_rows = jnp.stack([txt_qv_bias[0], jnp.zeros_like(txt_qv_bias[0]), txt_qv_bias[1]])
    made = (
        jnp.einsum("rd,jdw->rjw", normed1_all, txt_qkv, preferred_element_type=jnp.float32)
        + bias_rows
    )
    triple = made.astype(jnp.bfloat16).reshape(group_caps, L, 3, head_count, HEAD)
    queries = triple[:, :, 0]
    keys_all = triple[:, :, 1]
    values_all = triple[:, :, 2]
    shares, log_totals = attention_shares(queries, keys_all, keep)
    context = jnp.einsum(
        "nhqk,nkhe->nqhe",
        shares.astype(jnp.bfloat16),
        values_all,
        preferred_element_type=jnp.float32,
    )
    context = context.astype(jnp.bfloat16).reshape(group_rows, width)
    middle = inputs + (
        lax.psum(
            jnp.dot(context, txt_out, preferred_element_type=jnp.float32).astype(jnp.bfloat16),
            "mp",
        ).astype(jnp.float32)
        + txt_biases[0]
    )
    unit2, inverse2 = layer_stats(middle)
    normed2_all = (unit2 * txt_gains[1] + txt_shifts[1]).astype(jnp.bfloat16)
    hidden = jnp.dot(normed2_all, txt_fc1, preferred_element_type=jnp.float32) + txt_fc1_bias
    active, gelu_pull = jax.vjp(gelu_exact, hidden)
    active16 = active.astype(jnp.bfloat16)
    ffn_part = jnp.dot(active16, txt_fc2, preferred_element_type=jnp.float32)
    ffn_pooled = jnp.sum(ffn_part.reshape(group_caps, L, D) * present[:, :, None], 1)
    image_slots = lax.dynamic_update_slice_in_dim(
        jnp.zeros((group_caps, D), jnp.float32),
        images16.astype(jnp.float32),
        mp_index * own_caps,
        0,
    )
    images_all = gather_ordered(
        sum_exchanged(image_slots.astype(jnp.bfloat16), "mp"), "dp"
    ).reshape(-1, D)
    ffn_sum = sum_exchanged(ffn_pooled, "mp")
    mid_pooled = jnp.sum(middle.reshape(group_caps, L, D) * present[:, :, None], 1)
    pooled = (mid_pooled + ffn_sum) / counts + txt_biases[1]
    inverse_len = lax.rsqrt(jnp.sum(pooled * pooled, -1, keepdims=True) + EPS)
    captions_unit = pooled * inverse_len
    captions16 = captions_unit.astype(jnp.bfloat16)
    arrived = gather_ordered(captions16, "dp").reshape(-1, D)
    total_pairs = pairing.shape[0]
    first_pair = lax.axis_index("dp") * group_caps
    logits = SCALE * jnp.einsum("id,jd->ij", images_all, arrived, preferred_element_type=jnp.float32)
    matched = (pairing[:, None] == jnp.arange(total_pairs)[None, :]).astype(jnp.float32)
    raised = jnp.exp(logits - SCALE)
    row_lse = SCALE + jnp.log(jnp.sum(raised, 1))
    col_lse = SCALE + jnp.log(jnp.sum(raised, 0))
    total = 0.5 * jnp.sum(row_lse) + 0.5 * jnp.sum(col_lse) - jnp.sum(matched * logits)
    loss = total / total_pairs
    own_logits = lax.dynamic_slice_in_dim(logits, first_pair, group_caps, 1)
    own_col_lse = lax.dynamic_slice_in_dim(col_lse, first_pair, group_caps, 0)
    own_matched = lax.dynamic_slice_in_dim(matched, first_pair, group_caps, 1)
    grads16 = (
        LOSS_SCALE
        * (
            0.5 * jnp.exp(own_logits - row_lse[:, None])
            + 0.5 * jnp.exp(own_logits - own_col_lse[None, :])
            - own_matched
        )
    ).astype(jnp.bfloat16)
    grad_caps = SCALE * jnp.einsum(
        "ic,id->cd", grads16, images_all, preferred_element_type=jnp.float32
    )
    grad_pooled = inverse_len * (
        grad_caps - captions_unit * jnp.sum(captions_unit * grad_caps, -1, keepdims=True)
    )
    grad_result = (grad_pooled[:, None, :] * (present / counts)[:, :, None]).reshape(group_rows, D)
    grad_all = grad_result.astype(jnp.bfloat16)
    grad_fc2 = jnp.einsum("gf,gd->fd", active16, grad_all, preferred_element_type=jnp.float32)
    grad_active = jnp.einsum("gd,fd->gf", grad_all, txt_fc2, preferred_element_type=jnp.float32)
    grad_hidden16 = gelu_pull(grad_active)[0].astype(jnp.bfloat16)
    grad_fc1 = jnp.einsum(
        "gd,gf->df", normed2_all, grad_hidden16, preferred_element_type=jnp.float32
    )
    grad_fc1_bias = jnp.sum(grad_hidden16.astype(jnp.float32), 0)
    fc_sums = lax.psum(jnp.concatenate([grad_fc1, grad_fc2], 0).astype(jnp.bfloat16), "dp")
    grad_normed2 = reduce_exchanged(
        jnp.einsum("gf,df->gd", grad_hidden16, txt_fc1, preferred_element_type=jnp.float32), "mp"
    ).astype(jnp.float32)
    grad_middle = grad_result + norm_back(grad_normed2, unit2, inverse2, txt_gains[1])
    grad_mid_all = grad_middle.astype(jnp.bfloat16)
    grad_out = jnp.einsum("gw,gd->wd", context, grad_mid_all, preferred_element_type=jnp.float32)
    out_sums = reduce_exchanged(grad_out, "dp")
    grad_context = jnp.einsum(
        "gd,wd->gw", grad_mid_all, txt_out, preferred_element_type=jnp.float32
    )
    grad_context = grad_context.astype(jnp.bfloat16).reshape(group_caps, L, head_count, HEAD)
    shares_again = jnp.exp(score_rows(queries, keys_all, keep) - log_totals)
    grad_shares = jnp.einsum(
        "nqhe,nkhe->nhqk", grad_context, values_all, preferred_element_type=jnp.float32
    )
    grad_values = jnp.einsum(
        "nhqk,nqhe->nkhe",
        shares_again.astype(jnp.bfloat16),
        grad_context,
        preferred_element_type=jnp.float32,
    ).astype(jnp.bfloat16)
    grad_scores = (
        shares_again * (grad_shares - jnp.sum(grad_shares * shares_again, -1, keepdims=True))
    ).astype(jnp.bfloat16)
    grad_queries = (
        jnp.einsum("nhqk,nkhe->nqhe", grad_scores, keys_all, preferred_element_type=jnp.float32)
        * 0.125
    ).astype(jnp.bfloat16)
    grad_keys = (
        jnp.einsum("nhqk,nqhe->nkhe", grad_scores, queries, preferred_element_type=jnp.float32)
        * 0.125
    ).astype(jnp.bfloat16)
    grad_triple = jnp.stack([grad_queries, grad_keys, grad_values], 0).reshape(3, group_rows, width)
    grad_qkv = jnp.einsum(
        "gd,jgw->jdw", normed1_all, grad_triple, preferred_element_type=jnp.float32
    )
    grad_qv_bias = jnp.stack(
        [
            jnp.sum(grad_triple[0].astype(jnp.float32), 0),
            jnp.sum(grad_triple[2].astype(jnp.float32), 0),
        ]
    )
    qkv_sums = reduce_exchanged(grad_qkv.reshape(-1, D), "dp")
    grad_normed1 = scatter_exchanged(
        jnp.einsum("jgw,jdw->gd", grad_triple, txt_qkv, preferred_element_type=jnp.float32), "mp"
    )

    def own(values):
        return lax.dynamic_slice_in_dim(values, mp_index * own_rows, own_rows, 0)

    unit1_own = own(unit1)
    grad_normed2_own = own(grad_normed2)
    unit2_own = own(unit2)
    grad_middle_own = own(grad_middle)
    grad_inputs = grad_middle_own + norm_back(grad_normed1, unit1_own, own(inverse1), txt_gains[0])
    small_parts = jnp.stack(
        [
            jnp.sum(grad_normed1 * unit1_own, 0),
            jnp.sum(grad_normed2_own * unit2_own, 0),
            jnp.sum(grad_normed1, 0),
            jnp.sum(grad_normed2_own, 0),
            jnp.sum(grad_middle_own, 0),
            jnp.sum(own(grad_result), 0),
        ]
    )
    bias_rows = jnp.stack(
        [jnp.concatenate([grad_qv_bias.reshape(-1), jnp.zeros_like(grad_qv_bias.reshape(-1))]), grad_fc1_bias]
    )
    shared = sum_exchanged(jnp.concatenate([sum_exchanged(small_parts, "mp"), bias_rows], 0), "dp")
    qv_count = grad_qv_bias.size
    fc1_rows = grad_fc1.shape[0]
    return (
        loss,
        grad_inputs,
        qkv_sums.astype(jnp.float32).reshape(grad_qkv.shape),
        shared[6, :qv_count].reshape(grad_qv_bias.shape),
        out_sums.astype(jnp.float32),
        fc_sums[:fc1_rows].astype(jnp.float32),
        shared[7],
        fc_sums[fc1_rows:].astype(jnp.float32),
        shared[0:2],
        shared[2:4],
        shared[4:6],
    )


def solution(mesh):
    placed = (
        P(("dp", "mp"), None),
        P("dp", None),
        P(),
        P(("dp", "mp"), None),
        P(("dp", "mp"), None),
        P(),
        P(None, None, "mp"),
        P("mp", None),
        P(None, "mp"),
        P("mp", None),
        P(None, None, "mp"),
        P(None, "mp"),
        P("mp", None),
        P(None, "mp"),
        P("mp"),
        P("mp", None),
        P(),
        P(),
        P(),
    )
    return jax.shard_map(
        local_body,
        mesh=mesh,
        in_specs=placed,
        out_specs=(
            P(),
            P(("dp", "mp"), None),
            P(None, None, "mp"),
            P(None, "mp"),
            P("mp", None),
            P(None, "mp"),
            P("mp"),
            P("mp", None),
            P(),
            P(),
            P(),
        ),
        check_vma=False,
    )
```

```python
import jax
import jax.numpy as jnp
from jax import lax
from jax.sharding import PartitionSpec as P

D = 768
HEAD = 64
L = 16
P_LOW = 50
P_HIGH = 145


EPS = 1e-06
SCALE = 40.0
LOSS_SCALE = 16.0
MASKED = -1e30


def layer_stats(values):
    center = values - jnp.mean(values, -1, keepdims=True)
    inverse = lax.rsqrt(jnp.mean(center * center, -1, keepdims=True) + EPS)
    return (center * inverse, inverse)


def norm_back(grad_out, unit, inverse, gain):
    scaled = grad_out * gain
    return inverse * (
        scaled
        - jnp.mean(scaled, -1, keepdims=True)
        - unit * jnp.mean(scaled * unit, -1, keepdims=True)
    )


def gelu_exact(values):
    return jax.nn.gelu(values, approximate=False)


def score_rows(queries, keys_all, keep):
    scores = (
        jnp.einsum("nqhe,nkhe->nhqk", queries, keys_all, preferred_element_type=jnp.float32) * 0.125
    )
    if keep is not None:
        scores = jnp.where(keep, scores, MASKED)
    return scores


def attention_shares(queries, keys_all, keep):
    scores = score_rows(queries, keys_all, keep)
    highest = jnp.max(scores, -1, keepdims=True)
    raised = jnp.exp(scores - highest)
    totals = jnp.sum(raised, -1, keepdims=True)
    return (raised / totals, highest + jnp.log(totals))


def axis_bits(axis):
    count = lax.axis_size(axis)
    bits = count.bit_length() - 1
    assert 1 << bits == count
    return count, list(reversed(range(bits)))


def exchange(values, axis, count, bit):
    return lax.ppermute(values, axis, [(i, i ^ (1 << bit)) for i in range(count)])


def gather_stacked(values, axis):
    count, bits = axis_bits(axis)
    data = values[None]
    for bit in bits:
        data = jnp.concatenate([data, exchange(data, axis, count, bit)], 0)
    return data


def gather_ordered(values, axis):
    count, bits = axis_bits(axis)
    index = lax.axis_index(axis)
    data = values
    done = []
    for bit in bits:
        other = exchange(data, axis, count, bit)
        upper = ((index >> bit) & 1) == 1
        data = jnp.stack([jnp.where(upper, other, data), jnp.where(upper, data, other)], 0)
        done.insert(0, bit)
    order = sorted(range(len(done)), key=lambda a: -done[a])
    data = data.transpose(order + list(range(len(done), data.ndim)))
    return data.reshape((count,) + values.shape)


def sum_exchanged(values, axis):
    count, bits = axis_bits(axis)
    for bit in reversed(bits):
        values = values + exchange(values, axis, count, bit)
    return values


def scatter_exchanged(values, axis):
    count, bits = axis_bits(axis)
    index = lax.axis_index(axis)
    data = values.reshape((2,) * len(bits) + (values.shape[0] // count,) + values.shape[1:])
    for bit in reversed(bits):
        place = len(bits) - 1 - bit
        mine = (index >> bit) & 1
        kept = lax.dynamic_index_in_dim(data, mine, place, keepdims=False)
        sent = lax.dynamic_index_in_dim(data, 1 - mine, place, keepdims=False)
        data = kept + exchange(sent.astype(jnp.bfloat16), axis, count, bit).astype(jnp.float32)
    return data


def reduce_exchanged(values, axis):
    part = scatter_exchanged(values, axis).astype(jnp.bfloat16)
    return gather_ordered(part, axis).reshape(values.shape)


def image_tower(tokens, count, length, gains, weights):
    w_qkv, w_out, w_fc1, w_fc2 = weights
    _, middle = image_attention(tokens, count, length, gains, w_qkv, w_out)
    return image_ffn(middle, count, length, gains, w_fc1, w_fc2)


def image_attention(tokens, count, length, gains, w_qkv, w_out):
    head_count = D // HEAD
    inputs = tokens.astype(jnp.float32)
    unit, _ = layer_stats(inputs)
    normed = (unit * gains[0]).astype(jnp.bfloat16)
    projected = jnp.einsum("rd,jdw->jrw", normed, w_qkv, preferred_element_type=jnp.float32).astype(
        jnp.bfloat16
    )
    shaped = projected.reshape(3, count, length, head_count, HEAD)
    shares, _ = attention_shares(shaped[0], shaped[1], None)
    context = jnp.einsum(
        "nhqk,nkhe->nqhe",
        shares.astype(jnp.bfloat16),
        shaped[2],
        preferred_element_type=jnp.float32,
    )
    context = context.astype(jnp.bfloat16).reshape(count * length, D)
    middle = inputs + jnp.dot(context, w_out, preferred_element_type=jnp.float32)
    return inputs, middle


def image_ffn(middle, count, length, gains, w_fc1, w_fc2):
    unit2, _ = layer_stats(middle)
    normed2 = (unit2 * gains[1]).astype(jnp.bfloat16)
    active = gelu_exact(jnp.dot(normed2, w_fc1, preferred_element_type=jnp.float32)).astype(
        jnp.bfloat16
    )
    result = middle + jnp.dot(active, w_fc2, preferred_element_type=jnp.float32)
    pooled = jnp.mean(result.reshape(count, length, D), 1)
    return (pooled * lax.rsqrt(jnp.sum(pooled * pooled, -1, keepdims=True) + EPS)).astype(
        jnp.bfloat16
    )


def local_body(
    text_in,
    caption_ids,
    pairing,
    image_low,
    image_high,
    img_gains,
    img_qkv,
    img_out,
    img_fc1,
    img_fc2,
    txt_qkv,
    txt_qv_bias,
    txt_out,
    txt_fc1,
    txt_fc1_bias,
    txt_fc2,
    txt_gains,
    txt_shifts,
    txt_biases,
):
    qkv_parts = gather_stacked(img_qkv, "mp")
    fc1_parts = gather_stacked(img_fc1, "mp")
    weights = (
        qkv_parts.transpose(1, 2, 0, 3).reshape(3, D, -1),
        gather_stacked(img_out, "mp").reshape(-1, D),
        fc1_parts.transpose(1, 0, 2).reshape(D, -1),
        gather_stacked(img_fc2, "mp").reshape(-1, D),
    )
    low_count = image_low.shape[0] // P_LOW
    high_count = image_high.shape[0] // P_HIGH
    images16 = jnp.concatenate(
        [
            image_tower(image_low, low_count, P_LOW, img_gains, weights),
            image_tower(image_high, high_count, P_HIGH, img_gains, weights),
        ],
        0,
    )
    width = txt_qkv.shape[2]
    head_count = width // HEAD
    own_rows = text_in.shape[0]
    own_caps = own_rows // L
    group_caps = caption_ids.shape[0]
    group_rows = group_caps * L
    mp_index = lax.axis_index("mp")
    present = (caption_ids > 0).astype(jnp.float32)
    keep = (caption_ids > 0)[:, None, None, :]
    counts = jnp.sum(present, 1, keepdims=True)
    inputs = lax.all_gather(text_in, "mp", axis=0, tiled=True).astype(jnp.float32)
    unit1, inverse1 = layer_stats(inputs)
    normed1_all = (unit1 * txt_gains[0] + txt_shifts[0]).astype(jnp.bfloat16)
    bias_rows = jnp.stack([txt_qv_bias[0], jnp.zeros_like(txt_qv_bias[0]), txt_qv_bias[1]])
    made = (
        jnp.einsum("rd,jdw->rjw", normed1_all, txt_qkv, preferred_element_type=jnp.float32)
        + bias_rows
    )
    triple = made.astype(jnp.bfloat16).reshape(group_caps, L, 3, head_count, HEAD)
    queries = triple[:, :, 0]
    keys_all = triple[:, :, 1]
    values_all = triple[:, :, 2]
    shares, log_totals = attention_shares(queries, keys_all, keep)
    context = jnp.einsum(
        "nhqk,nkhe->nqhe",
        shares.astype(jnp.bfloat16),
        values_all,
        preferred_element_type=jnp.float32,
    )
    context = context.astype(jnp.bfloat16).reshape(group_rows, width)
    middle = inputs + (
        lax.psum(
            jnp.dot(context, txt_out, preferred_element_type=jnp.float32).astype(jnp.bfloat16),
            "mp",
        ).astype(jnp.float32)
        + txt_biases[0]
    )
    unit2, inverse2 = layer_stats(middle)
    normed2_all = (unit2 * txt_gains[1] + txt_shifts[1]).astype(jnp.bfloat16)
    hidden = jnp.dot(normed2_all, txt_fc1, preferred_element_type=jnp.float32) + txt_fc1_bias
    active, gelu_pull = jax.vjp(gelu_exact, hidden)
    active16 = active.astype(jnp.bfloat16)
    ffn_part = jnp.dot(active16, txt_fc2, preferred_element_type=jnp.float32)
    ffn_pooled = jnp.sum(ffn_part.reshape(group_caps, L, D) * present[:, :, None], 1)
    image_slots = lax.dynamic_update_slice_in_dim(
        jnp.zeros((group_caps, D), jnp.float32),
        images16.astype(jnp.float32),
        mp_index * own_caps,
        0,
    )
    images_all = gather_ordered(
        sum_exchanged(image_slots.astype(jnp.bfloat16), "mp"), "dp"
    ).reshape(-1, D)
    ffn_sum = sum_exchanged(ffn_pooled, "mp")
    mid_pooled = jnp.sum(middle.reshape(group_caps, L, D) * present[:, :, None], 1)
    pooled = (mid_pooled + ffn_sum) / counts + txt_biases[1]
    inverse_len = lax.rsqrt(jnp.sum(pooled * pooled, -1, keepdims=True) + EPS)
    captions_unit = pooled * inverse_len
    captions16 = captions_unit.astype(jnp.bfloat16)
    arrived = gather_ordered(captions16, "dp").reshape(-1, D)
    total_pairs = pairing.shape[0]
    first_pair = lax.axis_index("dp") * group_caps
    logits = SCALE * jnp.einsum("id,jd->ij", images_all, arrived, preferred_element_type=jnp.float32)
    matched = (pairing[:, None] == jnp.arange(total_pairs)[None, :]).astype(jnp.float32)
    raised = jnp.exp(logits - SCALE)
    row_lse = SCALE + jnp.log(jnp.sum(raised, 1))
    col_lse = SCALE + jnp.log(jnp.sum(raised, 0))
    total = 0.5 * jnp.sum(row_lse) + 0.5 * jnp.sum(col_lse) - jnp.sum(matched * logits)
    loss = total / total_pairs
    own_logits = lax.dynamic_slice_in_dim(logits, first_pair, group_caps, 1)
    own_col_lse = lax.dynamic_slice_in_dim(col_lse, first_pair, group_caps, 0)
    own_matched = lax.dynamic_slice_in_dim(matched, first_pair, group_caps, 1)
    grads16 = (
        LOSS_SCALE
        * (
            0.5 * jnp.exp(own_logits - row_lse[:, None])
            + 0.5 * jnp.exp(own_logits - own_col_lse[None, :])
            - own_matched
        )
    ).astype(jnp.bfloat16)
    grad_caps = SCALE * jnp.einsum(
        "ic,id->cd", grads16, images_all, preferred_element_type=jnp.float32
    )
    grad_pooled = inverse_len * (
        grad_caps - captions_unit * jnp.sum(captions_unit * grad_caps, -1, keepdims=True)
    )
    grad_result = (grad_pooled[:, None, :] * (present / counts)[:, :, None]).reshape(group_rows, D)
    grad_all = grad_result.astype(jnp.bfloat16)
    grad_fc2 = jnp.einsum("gf,gd->fd", active16, grad_all, preferred_element_type=jnp.float32)
    grad_active = jnp.einsum("gd,fd->gf", grad_all, txt_fc2, preferred_element_type=jnp.float32)
    grad_hidden16 = gelu_pull(grad_active)[0].astype(jnp.bfloat16)
    grad_fc1 = jnp.einsum(
        "gd,gf->df", normed2_all, grad_hidden16, preferred_element_type=jnp.float32
    )
    grad_fc1_bias = jnp.sum(grad_hidden16.astype(jnp.float32), 0)
    fc_sums = lax.psum(jnp.concatenate([grad_fc1, grad_fc2], 0).astype(jnp.bfloat16), "dp")
    grad_normed2 = reduce_exchanged(
        jnp.einsum("gf,df->gd", grad_hidden16, txt_fc1, preferred_element_type=jnp.float32), "mp"
    ).astype(jnp.float32)
    grad_middle = grad_result + norm_back(grad_normed2, unit2, inverse2, txt_gains[1])
    grad_mid_all = grad_middle.astype(jnp.bfloat16)
    grad_out = jnp.einsum("gw,gd->wd", context, grad_mid_all, preferred_element_type=jnp.float32)
    out_sums = reduce_exchanged(grad_out, "dp")
    grad_context = jnp.einsum(
        "gd,wd->gw", grad_mid_all, txt_out, preferred_element_type=jnp.float32
    )
    grad_context = grad_context.astype(jnp.bfloat16).reshape(group_caps, L, head_count, HEAD)
    shares_again = jnp.exp(score_rows(queries, keys_all, keep) - log_totals)
    grad_shares = jnp.einsum(
        "nqhe,nkhe->nhqk", grad_context, values_all, preferred_element_type=jnp.float32
    )
    grad_values = jnp.einsum(
        "nhqk,nqhe->nkhe",
        shares_again.astype(jnp.bfloat16),
        grad_context,
        preferred_element_type=jnp.float32,
    ).astype(jnp.bfloat16)
    grad_scores = (
        shares_again * (grad_shares - jnp.sum(grad_shares * shares_again, -1, keepdims=True))
    ).astype(jnp.bfloat16)
    grad_queries = (
        jnp.einsum("nhqk,nkhe->nqhe", grad_scores, keys_all, preferred_element_type=jnp.float32)
        * 0.125
    ).astype(jnp.bfloat16)
    grad_keys = (
        jnp.einsum("nhqk,nqhe->nkhe", grad_scores, queries, preferred_element_type=jnp.float32)
        * 0.125
    ).astype(jnp.bfloat16)
    grad_triple = jnp.stack([grad_queries, grad_keys, grad_values], 0).reshape(3, group_rows, width)
    grad_qkv = jnp.einsum(
        "gd,jgw->jdw", normed1_all, grad_triple, preferred_element_type=jnp.float32
    )
    grad_qv_bias = jnp.stack(
        [
            jnp.sum(grad_triple[0].astype(jnp.float32), 0),
            jnp.sum(grad_triple[2].astype(jnp.float32), 0),
        ]
    )
    qkv_sums = reduce_exchanged(grad_qkv.reshape(-1, D), "dp")
    normed1_part = jnp.einsum("jgw,jdw->gd", grad_triple, txt_qkv, preferred_element_type=jnp.float32)
    grad_normed1 = scatter_exchanged(normed1_part, "mp")

    def own(values):
        return lax.dynamic_slice_in_dim(values, mp_index * own_rows, own_rows, 0)

    unit1_own = own(unit1)
    grad_normed2_own = own(grad_normed2)
    unit2_own = own(unit2)
    grad_middle_own = own(grad_middle)
    grad_inputs = grad_middle_own + norm_back(grad_normed1, unit1_own, own(inverse1), txt_gains[0])
    small_parts = jnp.stack(
        [
            jnp.sum(normed1_part * unit1, 0),
            jnp.sum(grad_normed2_own * unit2_own, 0),
            jnp.sum(normed1_part, 0),
            jnp.sum(grad_normed2_own, 0),
            jnp.sum(grad_middle_own, 0),
            jnp.sum(own(grad_result), 0),
        ]
    )
    bias_rows = jnp.stack(
        [jnp.concatenate([grad_qv_bias.reshape(-1), jnp.zeros_like(grad_qv_bias.reshape(-1))]), grad_fc1_bias]
    )
    shared = sum_exchanged(jnp.concatenate([sum_exchanged(small_parts, "mp"), bias_rows], 0), "dp")
    qv_count = grad_qv_bias.size
    fc1_rows = grad_fc1.shape[0]
    return (
        loss,
        grad_inputs,
        qkv_sums.astype(jnp.float32).reshape(grad_qkv.shape),
        shared[6, :qv_count].reshape(grad_qv_bias.shape),
        out_sums.astype(jnp.float32),
        fc_sums[:fc1_rows].astype(jnp.float32),
        shared[7],
        fc_sums[fc1_rows:].astype(jnp.float32),
        shared[0:2],
        shared[2:4],
        shared[4:6],
    )


def solution(mesh):
    placed = (
        P(("dp", "mp"), None),
        P("dp", None),
        P(),
        P(("dp", "mp"), None),
        P(("dp", "mp"), None),
        P(),
        P(None, None, "mp"),
        P("mp", None),
        P(None, "mp"),
        P("mp", None),
        P(None, None, "mp"),
        P(None, "mp"),
        P("mp", None),
        P(None, "mp"),
        P("mp"),
        P("mp", None),
        P(),
        P(),
        P(),
    )
    return jax.shard_map(
        local_body,
        mesh=mesh,
        in_specs=placed,
        out_specs=(
            P(),
            P(("dp", "mp"), None),
            P(None, None, "mp"),
            P(None, "mp"),
            P("mp", None),
            P(None, "mp"),
            P("mp"),
            P("mp", None),
            P(),
            P(),
            P(),
        ),
        check_vma=False,
    )
```

```python
import jax
import jax.numpy as jnp
from jax import lax
from jax.sharding import PartitionSpec as P

D = 768
HEAD = 64
L = 16
P_LOW = 50
P_HIGH = 145


EPS = 1e-06
SCALE = 40.0
LOSS_SCALE = 16.0
MASKED = -1e30


def layer_stats(values):
    center = values - jnp.mean(values, -1, keepdims=True)
    inverse = lax.rsqrt(jnp.mean(center * center, -1, keepdims=True) + EPS)
    return (center * inverse, inverse)


def norm_back(grad_out, unit, inverse, gain):
    scaled = grad_out * gain
    return inverse * (
        scaled
        - jnp.mean(scaled, -1, keepdims=True)
        - unit * jnp.mean(scaled * unit, -1, keepdims=True)
    )


def gelu_exact(values):
    return jax.nn.gelu(values, approximate=False)


def score_rows(queries, keys_all, keep):
    scores = (
        jnp.einsum("nqhe,nkhe->nhqk", queries, keys_all, preferred_element_type=jnp.float32) * 0.125
    )
    if keep is not None:
        scores = jnp.where(keep, scores, MASKED)
    return scores


def attention_shares(queries, keys_all, keep):
    scores = score_rows(queries, keys_all, keep)
    highest = jnp.max(scores, -1, keepdims=True)
    raised = jnp.exp(scores - highest)
    totals = jnp.sum(raised, -1, keepdims=True)
    return (raised / totals, highest + jnp.log(totals))


def axis_bits(axis):
    count = lax.axis_size(axis)
    bits = count.bit_length() - 1
    assert 1 << bits == count
    return count, list(reversed(range(bits)))


def exchange(values, axis, count, bit):
    return lax.ppermute(values, axis, [(i, i ^ (1 << bit)) for i in range(count)])


def gather_stacked(values, axis):
    count, bits = axis_bits(axis)
    data = values[None]
    for bit in bits:
        data = jnp.concatenate([data, exchange(data, axis, count, bit)], 0)
    return data


def gather_ordered(values, axis):
    count, bits = axis_bits(axis)
    index = lax.axis_index(axis)
    data = values
    done = []
    for bit in bits:
        other = exchange(data, axis, count, bit)
        upper = ((index >> bit) & 1) == 1
        data = jnp.stack([jnp.where(upper, other, data), jnp.where(upper, data, other)], 0)
        done.insert(0, bit)
    order = sorted(range(len(done)), key=lambda a: -done[a])
    data = data.transpose(order + list(range(len(done), data.ndim)))
    return data.reshape((count,) + values.shape)


def sum_exchanged(values, axis):
    count, bits = axis_bits(axis)
    for bit in reversed(bits):
        values = values + exchange(values, axis, count, bit)
    return values


def scatter_exchanged(values, axis, swap_first=False):
    count, bits = axis_bits(axis)
    index = lax.axis_index(axis)
    data = values.reshape((2,) * len(bits) + (values.shape[0] // count,) + values.shape[1:])
    order = list(reversed(bits))
    if swap_first and len(order) > 1:
        order[0], order[1] = order[1], order[0]
    left = list(bits)
    for bit in order:
        place = left.index(bit)
        left.remove(bit)
        mine = (index >> bit) & 1
        kept = lax.dynamic_index_in_dim(data, mine, place, keepdims=False)
        sent = lax.dynamic_index_in_dim(data, 1 - mine, place, keepdims=False)
        data = kept + exchange(sent.astype(jnp.bfloat16), axis, count, bit).astype(jnp.float32)
    return data


def reduce_exchanged(values, axis, swap_first=False):
    part = scatter_exchanged(values, axis, swap_first).astype(jnp.bfloat16)
    return gather_ordered(part, axis).reshape(values.shape)


def image_tower(tokens, count, length, gains, weights):
    w_qkv, w_out, w_fc1, w_fc2 = weights
    _, middle = image_attention(tokens, count, length, gains, w_qkv, w_out)
    return image_ffn(middle, count, length, gains, w_fc1, w_fc2)


def image_attention(tokens, count, length, gains, w_qkv, w_out):
    head_count = D // HEAD
    inputs = tokens.astype(jnp.float32)
    unit, _ = layer_stats(inputs)
    normed = (unit * gains[0]).astype(jnp.bfloat16)
    projected = jnp.einsum("rd,jdw->jrw", normed, w_qkv, preferred_element_type=jnp.float32).astype(
        jnp.bfloat16
    )
    shaped = projected.reshape(3, count, length, head_count, HEAD)
    shares, _ = attention_shares(shaped[0], shaped[1], None)
    context = jnp.einsum(
        "nhqk,nkhe->nqhe",
        shares.astype(jnp.bfloat16),
        shaped[2],
        preferred_element_type=jnp.float32,
    )
    context = context.astype(jnp.bfloat16).reshape(count * length, D)
    middle = inputs + jnp.dot(context, w_out, preferred_element_type=jnp.float32)
    return inputs, middle


def image_ffn(middle, count, length, gains, w_fc1, w_fc2):
    unit2, _ = layer_stats(middle)
    normed2 = (unit2 * gains[1]).astype(jnp.bfloat16)
    active = gelu_exact(jnp.dot(normed2, w_fc1, preferred_element_type=jnp.float32)).astype(
        jnp.bfloat16
    )
    result = middle + jnp.dot(active, w_fc2, preferred_element_type=jnp.float32)
    pooled = jnp.mean(result.reshape(count, length, D), 1)
    return (pooled * lax.rsqrt(jnp.sum(pooled * pooled, -1, keepdims=True) + EPS)).astype(
        jnp.bfloat16
    )


def local_body(
    text_in,
    caption_ids,
    pairing,
    image_low,
    image_high,
    img_gains,
    img_qkv,
    img_out,
    img_fc1,
    img_fc2,
    txt_qkv,
    txt_qv_bias,
    txt_out,
    txt_fc1,
    txt_fc1_bias,
    txt_fc2,
    txt_gains,
    txt_shifts,
    txt_biases,
):
    qkv_parts = gather_stacked(img_qkv, "mp")
    fc1_parts = gather_stacked(img_fc1, "mp")
    weights = (
        qkv_parts.transpose(1, 2, 0, 3).reshape(3, D, -1),
        gather_stacked(img_out, "mp").reshape(-1, D),
        fc1_parts.transpose(1, 0, 2).reshape(D, -1),
        gather_stacked(img_fc2, "mp").reshape(-1, D),
    )
    low_count = image_low.shape[0] // P_LOW
    high_count = image_high.shape[0] // P_HIGH
    images16 = jnp.concatenate(
        [
            image_tower(image_low, low_count, P_LOW, img_gains, weights),
            image_tower(image_high, high_count, P_HIGH, img_gains, weights),
        ],
        0,
    )
    width = txt_qkv.shape[2]
    head_count = width // HEAD
    own_rows = text_in.shape[0]
    own_caps = own_rows // L
    group_caps = caption_ids.shape[0]
    group_rows = group_caps * L
    mp_index = lax.axis_index("mp")
    present = (caption_ids > 0).astype(jnp.float32)
    keep = (caption_ids > 0)[:, None, None, :]
    counts = jnp.sum(present, 1, keepdims=True)
    inputs = lax.all_gather(text_in, "mp", axis=0, tiled=True).astype(jnp.float32)
    unit1, inverse1 = layer_stats(inputs)
    normed1_all = (unit1 * txt_gains[0] + txt_shifts[0]).astype(jnp.bfloat16)
    bias_rows = jnp.stack([txt_qv_bias[0], jnp.zeros_like(txt_qv_bias[0]), txt_qv_bias[1]])
    made = (
        jnp.einsum("rd,jdw->rjw", normed1_all, txt_qkv, preferred_element_type=jnp.float32)
        + bias_rows
    )
    triple = made.astype(jnp.bfloat16).reshape(group_caps, L, 3, head_count, HEAD)
    queries = triple[:, :, 0]
    keys_all = triple[:, :, 1]
    values_all = triple[:, :, 2]
    shares, log_totals = attention_shares(queries, keys_all, keep)
    context = jnp.einsum(
        "nhqk,nkhe->nqhe",
        shares.astype(jnp.bfloat16),
        values_all,
        preferred_element_type=jnp.float32,
    )
    context = context.astype(jnp.bfloat16).reshape(group_rows, width)
    middle = inputs + (
        lax.psum(
            jnp.dot(context, txt_out, preferred_element_type=jnp.float32).astype(jnp.bfloat16),
            "mp",
        ).astype(jnp.float32)
        + txt_biases[0]
    )
    unit2, inverse2 = layer_stats(middle)
    normed2_all = (unit2 * txt_gains[1] + txt_shifts[1]).astype(jnp.bfloat16)
    hidden = jnp.dot(normed2_all, txt_fc1, preferred_element_type=jnp.float32) + txt_fc1_bias
    active, gelu_pull = jax.vjp(gelu_exact, hidden)
    active16 = active.astype(jnp.bfloat16)
    ffn_part = jnp.dot(active16, txt_fc2, preferred_element_type=jnp.float32)
    ffn_pooled = jnp.sum(ffn_part.reshape(group_caps, L, D) * present[:, :, None], 1)
    image_slots = lax.dynamic_update_slice_in_dim(
        jnp.zeros((group_caps, D), jnp.float32),
        images16.astype(jnp.float32),
        mp_index * own_caps,
        0,
    )
    images_all = gather_ordered(
        sum_exchanged(image_slots.astype(jnp.bfloat16), "mp"), "dp"
    ).reshape(-1, D)
    ffn_sum = sum_exchanged(ffn_pooled, "mp")
    mid_pooled = jnp.sum(middle.reshape(group_caps, L, D) * present[:, :, None], 1)
    pooled = (mid_pooled + ffn_sum) / counts + txt_biases[1]
    inverse_len = lax.rsqrt(jnp.sum(pooled * pooled, -1, keepdims=True) + EPS)
    captions_unit = pooled * inverse_len
    captions16 = captions_unit.astype(jnp.bfloat16)
    arrived = gather_ordered(captions16, "dp").reshape(-1, D)
    total_pairs = pairing.shape[0]
    first_pair = lax.axis_index("dp") * group_caps
    logits = SCALE * jnp.einsum("id,jd->ij", images_all, arrived, preferred_element_type=jnp.float32)
    matched = (pairing[:, None] == jnp.arange(total_pairs)[None, :]).astype(jnp.float32)
    raised = jnp.exp(logits - SCALE)
    row_lse = SCALE + jnp.log(jnp.sum(raised, 1))
    col_lse = SCALE + jnp.log(jnp.sum(raised, 0))
    total = 0.5 * jnp.sum(row_lse) + 0.5 * jnp.sum(col_lse) - jnp.sum(matched * logits)
    loss = total / total_pairs
    own_logits = lax.dynamic_slice_in_dim(logits, first_pair, group_caps, 1)
    own_col_lse = lax.dynamic_slice_in_dim(col_lse, first_pair, group_caps, 0)
    own_matched = lax.dynamic_slice_in_dim(matched, first_pair, group_caps, 1)
    grads16 = (
        LOSS_SCALE
        * (
            0.5 * jnp.exp(own_logits - row_lse[:, None])
            + 0.5 * jnp.exp(own_logits - own_col_lse[None, :])
            - own_matched
        )
    ).astype(jnp.bfloat16)
    grad_caps = SCALE * jnp.einsum(
        "ic,id->cd", grads16, images_all, preferred_element_type=jnp.float32
    )
    grad_pooled = inverse_len * (
        grad_caps - captions_unit * jnp.sum(captions_unit * grad_caps, -1, keepdims=True)
    )
    grad_result = (grad_pooled[:, None, :] * (present / counts)[:, :, None]).reshape(group_rows, D)
    grad_all = grad_result.astype(jnp.bfloat16)
    grad_fc2 = jnp.einsum("gf,gd->fd", active16, grad_all, preferred_element_type=jnp.float32)
    grad_active = jnp.einsum("gd,fd->gf", grad_all, txt_fc2, preferred_element_type=jnp.float32)
    grad_hidden16 = gelu_pull(grad_active)[0].astype(jnp.bfloat16)
    grad_fc1 = jnp.einsum(
        "gd,gf->df", normed2_all, grad_hidden16, preferred_element_type=jnp.float32
    )
    grad_fc1_bias = jnp.sum(grad_hidden16.astype(jnp.float32), 0)
    fc_sums = lax.psum(jnp.concatenate([grad_fc1, grad_fc2], 0).astype(jnp.bfloat16), "dp")
    grad_normed2 = reduce_exchanged(
        jnp.einsum("gf,df->gd", grad_hidden16, txt_fc1, preferred_element_type=jnp.float32), "mp"
    ).astype(jnp.float32)
    grad_middle = grad_result + norm_back(grad_normed2, unit2, inverse2, txt_gains[1])
    grad_mid_all = grad_middle.astype(jnp.bfloat16)
    grad_out = jnp.einsum("gw,gd->wd", context, grad_mid_all, preferred_element_type=jnp.float32)
    out_sums = reduce_exchanged(grad_out, "dp")
    grad_context = jnp.einsum(
        "gd,wd->gw", grad_mid_all, txt_out, preferred_element_type=jnp.float32
    )
    grad_context = grad_context.astype(jnp.bfloat16).reshape(group_caps, L, head_count, HEAD)
    shares_again = jnp.exp(score_rows(queries, keys_all, keep) - log_totals)
    grad_shares = jnp.einsum(
        "nqhe,nkhe->nhqk", grad_context, values_all, preferred_element_type=jnp.float32
    )
    grad_values = jnp.einsum(
        "nhqk,nqhe->nkhe",
        shares_again.astype(jnp.bfloat16),
        grad_context,
        preferred_element_type=jnp.float32,
    ).astype(jnp.bfloat16)
    grad_scores = (
        shares_again * (grad_shares - jnp.sum(grad_shares * shares_again, -1, keepdims=True))
    ).astype(jnp.bfloat16)
    grad_queries = (
        jnp.einsum("nhqk,nkhe->nqhe", grad_scores, keys_all, preferred_element_type=jnp.float32)
        * 0.125
    ).astype(jnp.bfloat16)
    grad_keys = (
        jnp.einsum("nhqk,nqhe->nkhe", grad_scores, queries, preferred_element_type=jnp.float32)
        * 0.125
    ).astype(jnp.bfloat16)
    grad_triple = jnp.stack([grad_queries, grad_keys, grad_values], 0).reshape(3, group_rows, width)
    grad_qkv = jnp.einsum(
        "gd,jgw->jdw", normed1_all, grad_triple, preferred_element_type=jnp.float32
    )
    grad_qv_bias = jnp.stack(
        [
            jnp.sum(grad_triple[0].astype(jnp.float32), 0),
            jnp.sum(grad_triple[2].astype(jnp.float32), 0),
        ]
    )
    qkv_sums = reduce_exchanged(grad_qkv.reshape(-1, D), "dp", swap_first=True)
    normed1_part = jnp.einsum("jgw,jdw->gd", grad_triple, txt_qkv, preferred_element_type=jnp.float32)
    grad_normed1 = scatter_exchanged(normed1_part, "mp")

    def own(values):
        return lax.dynamic_slice_in_dim(values, mp_index * own_rows, own_rows, 0)

    unit1_own = own(unit1)
    grad_normed2_own = own(grad_normed2)
    unit2_own = own(unit2)
    grad_middle_own = own(grad_middle)
    grad_inputs = grad_middle_own + norm_back(grad_normed1, unit1_own, own(inverse1), txt_gains[0])
    small_parts = jnp.stack(
        [
            jnp.sum(normed1_part * unit1, 0),
            jnp.sum(grad_normed2_own * unit2_own, 0),
            jnp.sum(normed1_part, 0),
            jnp.sum(grad_normed2_own, 0),
            jnp.sum(grad_middle_own, 0),
            jnp.sum(own(grad_result), 0),
        ]
    )
    bias_rows = jnp.stack(
        [jnp.concatenate([grad_qv_bias.reshape(-1), jnp.zeros_like(grad_qv_bias.reshape(-1))]), grad_fc1_bias]
    )
    shared = sum_exchanged(jnp.concatenate([sum_exchanged(small_parts, "mp"), bias_rows], 0), "dp")
    qv_count = grad_qv_bias.size
    fc1_rows = grad_fc1.shape[0]
    return (
        loss,
        grad_inputs,
        qkv_sums.astype(jnp.float32).reshape(grad_qkv.shape),
        shared[6, :qv_count].reshape(grad_qv_bias.shape),
        out_sums.astype(jnp.float32),
        fc_sums[:fc1_rows].astype(jnp.float32),
        shared[7],
        fc_sums[fc1_rows:].astype(jnp.float32),
        shared[0:2],
        shared[2:4],
        shared[4:6],
    )


def solution(mesh):
    placed = (
        P(("dp", "mp"), None),
        P("dp", None),
        P(),
        P(("dp", "mp"), None),
        P(("dp", "mp"), None),
        P(),
        P(None, None, "mp"),
        P("mp", None),
        P(None, "mp"),
        P("mp", None),
        P(None, None, "mp"),
        P(None, "mp"),
        P("mp", None),
        P(None, "mp"),
        P("mp"),
        P("mp", None),
        P(),
        P(),
        P(),
    )
    return jax.shard_map(
        local_body,
        mesh=mesh,
        in_specs=placed,
        out_specs=(
            P(),
            P(("dp", "mp"), None),
            P(None, None, "mp"),
            P(None, "mp"),
            P("mp", None),
            P(None, "mp"),
            P("mp"),
            P("mp", None),
            P(),
            P(),
            P(),
        ),
        check_vma=False,
    )
```
